128 devices in a mesh: replica: 16 (over z, y), data: 8 (over x, core).
Axes of the slice: x: 4, y: 4, z: 4, core: 2. Of those that a mesh axis runs over, the one named last changes fastest.
Arguments:
- img_x: bfloat16 [32768, 2048], P(('replica', 'data'))
- txt_x: bfloat16 [32768, 512], P(('replica', 'data'))
- w_img: bfloat16 [2048, 1024], replicated
- w_txt: bfloat16 [512, 1024], replicated
- log_temp: float32 [1], replicated
- logit_bias: float32 [1], replicated
Outputs:
- output 1: float32 [1], replicated
- output 2: float32 [1], replicated
- output 3: float32 [1], replicated
- output 4: float32 [2048, 1024], replicated
- output 5: float32 [512, 1024], replicated
All inputs are finite; a program needn't handle non-finite values.
Results may differ from the reference program's by a relative error of at most 0.001.
Values are sent between devices in bfloat16 or wider.
A program may use at most 1 GiB of HBM per device.

```python
import math
import jax
import jax.numpy as jnp
from jax import lax

LOCAL_BATCH = 256
NUM_DEVICES = 128
IMG_FEAT = 2048
TXT_FEAT = 512
EMBED_DIM = 1024
LATENT_RANK = 8

GLOBAL_BATCH = LOCAL_BATCH * NUM_DEVICES


def setup_inputs(seed: int = 0) -> dict:
    key_list = jax.random.split(jax.random.key(seed), 12)
    latent = jax.random.normal(key_list[0], (NUM_DEVICES, LOCAL_BATCH, LATENT_RANK), jnp.float32)
    dev_mean = jax.random.normal(key_list[1], (NUM_DEVICES, 1, LATENT_RANK), jnp.float32)
    latent = (latent + 0.8 * dev_mean).reshape(GLOBAL_BATCH, LATENT_RANK)
    mix_img = jax.random.normal(key_list[2], (LATENT_RANK, IMG_FEAT), jnp.float32) * LATENT_RANK ** -0.5
    mix_txt = jax.random.normal(key_list[3], (LATENT_RANK, TXT_FEAT), jnp.float32) * LATENT_RANK ** -0.5
    shared = jax.random.normal(key_list[4], (LATENT_RANK, EMBED_DIM), jnp.float32)
    img_x = 0.7 * (jnp.dot(latent, mix_img) + jax.random.normal(key_list[5], (GLOBAL_BATCH, IMG_FEAT), jnp.float32))
    txt_x = 0.7 * (jnp.dot(latent, mix_txt) + jax.random.normal(key_list[6], (GLOBAL_BATCH, TXT_FEAT), jnp.float32))
    w_img = jnp.dot(mix_img.T, shared) * (LATENT_RANK ** 0.5 / IMG_FEAT) + jax.random.normal(key_list[7], (IMG_FEAT, EMBED_DIM), jnp.float32) * IMG_FEAT ** -0.5
    w_txt = jnp.dot(mix_txt.T, shared) * (LATENT_RANK ** 0.5 / TXT_FEAT) + jax.random.normal(key_list[8], (TXT_FEAT, EMBED_DIM), jnp.float32) * TXT_FEAT ** -0.5
    log_temp = math.log(4.0) + jax.random.uniform(key_list[9], (1,), jnp.float32, -0.3, 0.3)
    logit_bias = -math.log(GLOBAL_BATCH) + jax.random.uniform(key_list[10], (1,), jnp.float32, -0.5, 0.5)
    return {"img_x": img_x.astype(jnp.bfloat16), "txt_x": txt_x.astype(jnp.bfloat16), "w_img": w_img.astype(jnp.bfloat16), "w_txt": w_txt.astype(jnp.bfloat16), "log_temp": log_temp.astype(jnp.float32), "logit_bias": logit_bias.astype(jnp.float32)}


def normalize(raw):
    return raw * lax.rsqrt(jnp.sum(raw * raw, axis=-1, keepdims=True))


def reference(img_x, txt_x, w_img, w_txt, log_temp, logit_bias):
    img_raw = jnp.dot(img_x, w_img, preferred_element_type=jnp.float32)
    txt_raw = jnp.dot(txt_x, w_txt, preferred_element_type=jnp.float32)
    img_unit, img_pull = jax.vjp(normalize, img_raw)
    txt_unit, txt_pull = jax.vjp(normalize, txt_raw)
    img_emb = img_unit.astype(jnp.bfloat16)
    txt_emb = txt_unit.astype(jnp.bfloat16)
    temp_scale = jnp.exp(log_temp[0])
    bias_val = logit_bias[0]
    col_ids = jnp.arange(GLOBAL_BATCH)[None, :]
    row_ids = jnp.arange(LOCAL_BATCH)[:, None]

    def block_step(state_in, block_in):
        d_txt_acc, loss_acc, temp_acc, bias_acc = state_in
        img_blk, blk_idx = block_in
        sim_tile = jnp.dot(img_blk, txt_emb.T, preferred_element_type=jnp.float32)
        logits = temp_scale * sim_tile + bias_val
        labels = jnp.where(col_ids == row_ids + blk_idx * LOCAL_BATCH, 1.0, -1.0)
        loss_part = -jnp.sum(jax.nn.log_sigmoid(labels * logits))
        grad_tile = -labels * jax.nn.sigmoid(-labels * logits) / GLOBAL_BATCH
        grad_b = grad_tile.astype(jnp.bfloat16)
        d_img_blk = temp_scale * jnp.dot(grad_b, txt_emb, preferred_element_type=jnp.float32)
        d_txt_acc = d_txt_acc + jnp.dot(grad_b.T, img_blk, preferred_element_type=jnp.float32)
        new_state = (d_txt_acc, loss_acc + loss_part, temp_acc + jnp.sum(grad_tile * sim_tile), bias_acc + jnp.sum(grad_tile))
        return new_state, d_img_blk

    init_state = (jnp.zeros((GLOBAL_BATCH, EMBED_DIM), jnp.float32), jnp.zeros((), jnp.float32), jnp.zeros((), jnp.float32), jnp.zeros((), jnp.float32))
    img_blocks = img_emb.reshape(NUM_DEVICES, LOCAL_BATCH, EMBED_DIM)
    final_state, d_img_blocks = lax.scan(block_step, init_state, (img_blocks, jnp.arange(NUM_DEVICES)))
    d_txt_acc, loss_sum, temp_sum, bias_sum = final_state
    d_img = d_img_blocks.reshape(GLOBAL_BATCH, EMBED_DIM)
    d_txt = temp_scale * d_txt_acc
    d_img_raw = img_pull(d_img)[0].astype(jnp.bfloat16)
    d_txt_raw = txt_pull(d_txt)[0].astype(jnp.bfloat16)
    d_w_img = jnp.dot(img_x.T, d_img_raw, preferred_element_type=jnp.float32)
    d_w_txt = jnp.dot(txt_x.T, d_txt_raw, preferred_element_type=jnp.float32)
    loss_out = jnp.reshape(loss_sum / GLOBAL_BATCH, (1,))
    d_log_temp = jnp.reshape(temp_scale * temp_sum, (1,))
    d_logit_bias = jnp.reshape(bias_sum, (1,))
    return (loss_out, d_log_temp, d_logit_bias, d_w_img, d_w_txt)
```

```python
import functools

import jax
import jax.numpy as jnp
from jax import lax
from jax.experimental import pallas as pl
from jax.experimental.pallas import tpu as pltpu
from jax.sharding import PartitionSpec as P

TILE = 512
F32 = jnp.float32
BF16 = jnp.bfloat16


def normalize(raw):
    return raw * lax.rsqrt(jnp.sum(raw * raw, axis=-1, keepdims=True))


def embed_rows(feat_x, w_proj):
    raw_emb = jnp.dot(feat_x, w_proj, preferred_element_type=F32)
    unit_emb, pull_back = jax.vjp(normalize, raw_emb)
    return unit_emb.astype(BF16), pull_back


def score_terms(sim, scale, bias, diag):
    z = scale * sim + bias
    if diag is not None:
        z = jnp.where(diag, -z, z)
    e = jnp.exp(-jnp.abs(z))
    r = 1.0 / (1.0 + e)
    g = jnp.where(z >= 0.0, r, e * r)
    loss = jnp.maximum(z, 0.0) + jnp.log1p(e)
    if diag is not None:
        g = jnp.where(diag, -g, g)
    return loss, g


def fold(x):
    return jnp.sum(x.reshape(x.shape[0] // 8, 8, x.shape[1]), axis=0)


def tile_kernel(block, scal, img, img_t, txt, d_img, d_txt, sums):
    j = pl.program_id(0)
    rows = img.shape[0]
    scale, bias = scal[0], scal[1]
    rep, dat = lax.axis_index("replica"), lax.axis_index("data")

    @pl.when(j == 0)
    def _():
        d_img[...] = jnp.zeros_like(d_img)
        sums[...] = jnp.zeros_like(sums)

    def tile(i, masked):
        at = pl.ds(pl.multiple_of(i * TILE, TILE), TILE)
        sim = lax.dot_general(img[at, :], txt[...], (((1,), (1,)), ((), ())), preferred_element_type=F32)
        diag = None
        if masked:
            row = lax.broadcasted_iota(jnp.int32, sim.shape, 0) + (i * TILE - dat * block)
            col = lax.broadcasted_iota(jnp.int32, sim.shape, 1) + (j * TILE - rep * block)
            diag = (row == col) & (row >= 0) & (row < block)
        loss, g = score_terms(sim, scale, bias, diag)
        sums[0] += fold(loss)
        sums[1] += fold(g * sim)
        sums[2] += fold(g)
        gb = g.astype(BF16)
        d_img[at, :] += jnp.dot(gb, txt[...], preferred_element_type=F32)
        part = jnp.dot(img_t[:, at], gb, preferred_element_type=F32)

        @pl.when(i == 0)
        def _():
            d_txt[...] = part

        @pl.when(i > 0)
        def _():
            d_txt[...] += part

    per = TILE // block
    own_j = lax.div(rep, per) == j

    def step(i, carry):
        hit = own_j & (lax.div(dat, per) == i)

        @pl.when(hit)
        def _():
            tile(i, True)

        @pl.when(jnp.logical_not(hit))
        def _():
            tile(i, False)

        return carry

    lax.fori_loop(0, rows // TILE, step, 0)


def tile_call(block, scal, img, img_t, txt):
    rows, dim = img.shape
    cols = txt.shape[0]
    whole = pl.BlockSpec(memory_space=pltpu.VMEM)
    return pl.pallas_call(
        functools.partial(tile_kernel, block),
        grid=(cols // TILE,),
        in_specs=[pl.BlockSpec(memory_space=pltpu.SMEM), whole, whole, pl.BlockSpec((TILE, dim), lambda j: (j, 0))],
        out_specs=[whole, pl.BlockSpec((dim, TILE), lambda j: (0, j)), whole],
        out_shape=[
            jax.ShapeDtypeStruct((rows, dim), F32),
            jax.ShapeDtypeStruct((dim, cols), F32),
            jax.ShapeDtypeStruct((3, 8, TILE), F32),
        ],
        compiler_params=pltpu.CompilerParams(vmem_limit_bytes=60 * 2**20),
        cost_estimate=pl.CostEstimate(flops=6 * rows * cols * dim, bytes_accessed=4 * rows * dim + 8 * cols * dim, transcendentals=3 * rows * cols),
        name="tile",
    )(scal, img, img_t, txt)


def solution(mesh):
    rep_count = mesh.shape["replica"]
    data_count = mesh.shape["data"]
    batch_axes = ("replica", "data")

    def local_fn(img_x, txt_x, w_img, w_txt, log_temp, logit_bias):
        block = img_x.shape[0]
        dim = w_img.shape[1]
        total_rows = block * rep_count * data_count
        txt_emb, txt_pull = embed_rows(txt_x, w_txt)
        txt_all = lax.all_gather(txt_emb, "replica", axis=0, tiled=True)
        img_emb, img_pull = embed_rows(img_x, w_img)
        img_all = lax.all_gather(img_emb, "data", axis=0, tiled=True)
        temp_scale = jnp.exp(log_temp[0])
        scal = jnp.stack([temp_scale, logit_bias[0]])
        d_img, d_txt, sums = tile_call(block, scal, img_all, img_all.T, txt_all)
        d_txt = d_txt.reshape(dim, rep_count, block).transpose(1, 0, 2)
        d_txt = lax.psum_scatter(d_txt, "replica", scatter_dimension=0, tiled=False).T
        d_img = lax.psum_scatter(d_img, "data", scatter_dimension=0, tiled=True)
        post = temp_scale / total_rows
        d_img_raw = img_pull(post * d_img)[0].astype(BF16)
        d_txt_raw = txt_pull(post * d_txt)[0].astype(BF16)
        d_w_img = jnp.einsum("nf,nd->fd", img_x, d_img_raw, preferred_element_type=F32)
        d_w_txt = jnp.einsum("nf,nd->fd", txt_x, d_txt_raw, preferred_element_type=F32)
        parts = jnp.sum(sums, axis=(1, 2))
        parts, d_w_img, d_w_txt = lax.psum((parts, d_w_img, d_w_txt), batch_axes)
        parts = parts / total_rows
        return parts[0:1], temp_scale * parts[1:2], parts[2:3], d_w_img, d_w_txt

    batch_spec = P(batch_axes, None)
    return jax.shard_map(local_fn, mesh=mesh, in_specs=(batch_spec, batch_spec, P(), P(), P(), P()), out_specs=(P(), P(), P(), P(), P()), check_vma=False)
```

```python
import functools

import jax
import jax.numpy as jnp
from jax import lax
from jax.experimental import pallas as pl
from jax.experimental.pallas import tpu as pltpu
from jax.sharding import PartitionSpec as P

F32 = jnp.float32
BF16 = jnp.bfloat16
TILE = 512
MESH = pl.DeviceIdType.MESH
VMEM_LIMIT = 67043328


def normalize(raw):
    return raw * lax.rsqrt(jnp.sum(raw * raw, axis=-1, keepdims=True))


def embed_rows(feat_x, w_proj):
    raw_emb = jnp.dot(feat_x, w_proj, preferred_element_type=F32)
    unit_emb, pull_back = jax.vjp(normalize, raw_emb)
    return unit_emb.astype(BF16), pull_back


class Place:
    def __init__(self):
        rep, dat = lax.axis_index("replica"), lax.axis_index("data")
        self.z, self.y = lax.div(rep, 4), lax.rem(rep, 4)
        self.x, self.c = lax.div(dat, 2), lax.rem(dat, 2)

    def at(self, x=None, y=None, z=None, c=None):
        x = self.x if x is None else lax.rem(x + 8, 4)
        y = self.y if y is None else lax.rem(y + 8, 4)
        z = self.z if z is None else lax.rem(z + 8, 4)
        c = self.c if c is None else c
        return (z * 4 + y, x * 2 + c)

    def partner(self):
        return self.at(c=1 - self.c)

    def near(self, v):
        return v + 1 - 2 * lax.rem(v, 2)

    def far(self, v):
        return v - 1 + 2 * lax.rem(v, 2)

    def image_group(self):
        return Group(self.x, lax.rem(lax.div(self.y + 1, 2), 2), self.at(x=self.x + 1), self.at(x=self.x - 1), self.at(y=self.near(self.y)))

    def text_group(self):
        return Group(self.z, lax.div(self.y, 2), self.at(z=self.z + 1), self.at(z=self.z - 1), self.at(y=self.far(self.y)))

    def peers(self):
        out = [self.partner()]
        for g in (self.image_group(), self.text_group()):
            out += [g.right, g.left, g.pair]
        return out


class Group:
    def __init__(self, pos, side, right, left, pair):
        self.pos, self.side, self.right, self.left, self.pair = pos, side, right, left, pair

    def slot(self, twin, step):
        side = 1 - self.side if twin else self.side
        return side * 4 + lax.rem(self.pos + step + 4, 4)


def greet(place):
    barrier = pltpu.get_barrier_semaphore()
    peers = place.peers()
    for dev in peers:
        pl.semaphore_signal(barrier, inc=1, device_id=dev, device_id_type=MESH)
    pl.semaphore_wait(barrier, len(peers))


class Wire:
    def __init__(self, send, recv):
        self.send, self.recv, self.open = send, recv, []

    def go(self, k, src, dst, dev):
        copy = pltpu.make_async_remote_copy(src_ref=src, dst_ref=dst, send_sem=self.send.at[k], recv_sem=self.recv.at[k], device_id=dev, device_id_type=MESH)
        copy.start()
        self.open.append(copy)

    def got(self, k, dst, dev):
        pltpu.make_async_remote_copy(src_ref=dst, dst_ref=dst, send_sem=self.send.at[k], recv_sem=self.recv.at[k], device_id=dev, device_id_type=MESH).wait_recv()

    def drain(self):
        for copy in self.open:
            copy.wait_send()
        self.open = []


GATHER_COPIES = 8
SCATTER_COPIES = 10


def gather_stages(g, wire, own, blk, half, seen=None):
    seen = seen or (lambda slot: None)
    s = g.slot

    def start():
        me = s(False, 0)
        wire.go(0, own, blk(me), g.right)
        wire.go(1, own, blk(me), g.left)
        wire.go(2, own, blk(me), g.pair)

    def ring():
        wire.got(0, blk(s(False, -1)), g.left)
        wire.go(3, half(s(False, -1), 0), half(s(False, -1), 0), g.right)
        wire.got(1, blk(s(False, 1)), g.right)
        wire.go(4, half(s(False, 1), 1), half(s(False, 1), 1), g.left)
        seen(s(False, -1))
        seen(s(False, 1))

    def twin():
        wire.got(2, blk(s(True, 0)), g.pair)
        wire.go(5, blk(s(True, 0)), blk(s(True, 0)), g.right)
        wire.go(6, blk(s(True, 0)), blk(s(True, 0)), g.left)
        seen(s(True, 0))

    def across():
        wire.got(3, half(s(False, 2), 0), g.left)
        wire.got(4, half(s(False, 2), 1), g.right)
        wire.go(7, blk(s(False, 2)), blk(s(False, 2)), g.pair)
        seen(s(False, 2))

    def last():
        wire.got(5, blk(s(True, -1)), g.left)
        wire.got(6, blk(s(True, 1)), g.right)
        seen(s(True, -1))
        seen(s(True, 1))
        wire.got(7, blk(s(True, 2)), g.pair)
        seen(s(True, 2))

    return [start, ring, twin, across, last]


def scatter_stages(g, wire, blk, half, bufs, done):
    whole, part = bufs
    s = g.slot
    rp, rr0, rr1, rf0, rf1, rf2 = (whole.at[k] for k in range(6))
    rh0, rh1 = part.at[0], part.at[1]
    rows = part.shape[1]
    lo, hi = pl.ds(0, rows), pl.ds(rows, rows)

    def start():
        wire.go(0, blk(s(True, 2)), rp, g.pair)
        wire.go(1, blk(s(True, 1)), rr0, g.right)
        wire.go(2, blk(s(True, -1)), rr1, g.left)
        wire.go(3, half(s(False, 1), 1), rf0.at[hi], g.right)
        wire.go(4, half(s(False, -1), 0), rf1.at[lo], g.left)

    def across():
        wire.got(0, rp, g.pair)
        for h, sl in ((0, lo), (1, hi)):
            v = half(s(False, 2), h)
            v[...] += rp[sl]
        wire.go(5, half(s(False, 2), 0), rh0, g.right)
        wire.go(6, half(s(False, 2), 1), rh1, g.left)

    def twin():
        wire.got(1, rr0, g.left)
        wire.got(2, rr1, g.right)
        v = blk(s(True, 0))
        v[...] += rr0[...] + rr1[...]
        wire.go(7, v, rf2, g.pair)

    def ring():
        wire.got(5, rh0, g.left)
        v = half(s(False, 1), 0)
        v[...] += rh0[...]
        wire.go(8, v, rf0.at[lo], g.right)
        wire.got(6, rh1, g.right)
        v = half(s(False, -1), 1)
        v[...] += rh1[...]
        wire.go(9, v, rf1.at[hi], g.left)

    def last():
        wire.got(3, rf0.at[hi], g.left)
        wire.got(4, rf1.at[lo], g.right)
        wire.got(7, rf2, g.pair)
        wire.got(8, rf0.at[lo], g.left)
        wire.got(9, rf1.at[hi], g.right)
        done(rf0, rf1, rf2)

    return [start, across, twin, ring, last]


def run_both(a, b):
    for fa, fb in zip(a, b):
        fa()
        fb()


def rows_of(ref, size):
    def blk(slot):
        return ref.at[pl.ds(pl.multiple_of(slot * size, size), size)]

    def half(slot, h):
        return ref.at[pl.ds(pl.multiple_of(slot * size + h * (size // 2), size // 2), size // 2)]

    return blk, half


def score_terms(sim, scale, bias, diag):
    z = scale * sim + bias
    if diag is not None:
        z = jnp.where(diag, -z, z)
    e = jnp.exp(-jnp.abs(z))
    r = 1.0 / (1.0 + e)
    g = jnp.where(z >= 0.0, r, e * r)
    loss = jnp.maximum(z, 0.0) + jnp.log1p(e)
    if diag is not None:
        g = jnp.where(diag, -g, g)
    return loss, g


def fold(x):
    x = jnp.sum(x.reshape(x.shape[0] // 8, 8, x.shape[1]), axis=0)
    return sum(x[:, k * 128 : (k + 1) * 128] for k in range(x.shape[1] // 128))


def main_kernel(
    block, scal, img_own, txt_own, x_give, d_img_out, d_txt_out, sums, x_got,
    img, txt, d_img, d_txt, give, sbuf, gbuf,
    ibuf, ihalf, tbuf, thalf,
    ig_s, ig_r, tg_s, tg_r, is_s, is_r, ts_s, ts_r, core_s, core_r, local,
):
    place = Place()
    gi, gt = place.image_group(), place.text_group()
    c = place.c
    partner = place.partner()
    greet(place)

    half_rows = 8 * block
    img_blk, img_half = rows_of(img, block)
    core = Wire(core_s, core_r)
    core.go(0, x_give, x_got, partner)

    def txt_view(cc):
        def blk(slot):
            return txt.at[pl.ds(pl.multiple_of(cc * half_rows + slot * block, block), block)]

        def half(slot, h):
            return txt.at[pl.ds(pl.multiple_of(cc * half_rows + slot * block + h * (block // 2), block // 2), block // 2)]

        return blk, half

    txt_blk, txt_half = txt_view(c)
    other_blk, _ = txt_view(1 - c)
    wi, wt = Wire(ig_s, ig_r), Wire(tg_s, tg_r)

    counter = [1]

    def share(slot):
        core.go(counter[0], txt_blk(slot), txt_blk(slot), partner)
        counter[0] += 1

    core.go(counter[0], txt_own, txt_blk(gt.slot(False, 0)), partner)
    counter[0] += 1
    own_i = pltpu.make_async_copy(img_own, img_blk(gi.slot(False, 0)), local.at[0])
    own_t = pltpu.make_async_copy(txt_own, txt_blk(gt.slot(False, 0)), local.at[1])
    own_i.start()
    own_t.start()
    a = gather_stages(gi, wi, img_own, img_blk, img_half)
    b = gather_stages(gt, wt, txt_own, txt_blk, txt_half, share)
    a[0]()
    b[0]()
    d_img[...] = jnp.zeros_like(d_img)
    sums[...] = jnp.zeros_like(sums)
    run_both(a[1:], b[1:])
    own_i.wait()
    own_t.wait()
    order = [(False, 0), (False, -1), (False, 1), (True, 0), (False, 2), (True, -1), (True, 1), (True, 2)]
    for k, (twin, step) in enumerate(order):
        core.got(1 + k, other_blk(gt.slot(twin, step)), partner)
    core.got(0, x_got, partner)
    wi.drain()
    wt.drain()
    core.drain()

    scale, bias = scal[0], scal[1]
    chunks = half_rows // TILE
    per = TILE // block
    own_ci = lax.div(gi.slot(False, 0), per)
    own_ct = lax.div(gt.slot(False, 0), per)

    def img_rows(i):
        return pl.ds(pl.multiple_of(lax.rem(own_ci + i, chunks) * TILE, TILE), TILE)

    def chunk_of(k):
        return 2 * lax.rem(gt.side + lax.div(k + 1, 2), 2) + lax.rem(lax.rem(own_ct, 2) + lax.div(k, 2), 2)

    def txt_rows(cc, k):
        return pl.ds(pl.multiple_of(cc * half_rows + chunk_of(k) * TILE, TILE), TILE)

    count = chunks * chunks

    def sweep(cc, target, masked, enter, leave):
        def where(n):
            return lax.rem(n, chunks), lax.div(n, chunks)

        def score(n, slot):
            i, k = where(n)
            sbuf[slot] = lax.dot_general(img[img_rows(i), :], txt[txt_rows(cc, k), :], (((1,), (1,)), ((), ())), preferred_element_type=F32)

        def point(slot, diag=None):
            sim = sbuf[slot]
            loss, g = score_terms(sim, scale, bias, diag)
            sums[0] += fold(loss)
            sums[1] += fold(g * sim)
            sums[2] += fold(g)
            gbuf[slot] = g.astype(BF16)

        def products(n, slot):
            i, k = where(n)
            gb = gbuf[slot]
            rows = img_rows(i)
            d_img[rows, :] += jnp.dot(gb, txt[txt_rows(cc, k), :], preferred_element_type=F32)
            ref, at = target(k)
            ref[at, :] += lax.dot_general(gb, img[rows, :], (((0,), (0,)), ((), ())), preferred_element_type=F32)

        diag = None
        if masked:
            row = lax.broadcasted_iota(jnp.int32, (TILE, TILE), 0) - lax.rem(gi.slot(False, 0), per) * block
            col = lax.broadcasted_iota(jnp.int32, (TILE, TILE), 1) - lax.rem(gt.slot(False, 0), per) * block
            diag = (row == col) & (row >= 0) & (row < block)
        score(0, 0)
        score(1, 1)
        point(0, diag)
        per_k = chunks // 2

        def step(m, carry):
            n = 2 * m
            k = lax.div(m, per_k)

            @pl.when(lax.rem(m, per_k) == 0)
            def _():
                enter(k)

            score(n + 2, 0)
            point(1)
            products(n, 0)
            score(n + 3, 1)
            point(0)
            products(n + 1, 1)

            @pl.when(lax.rem(m, per_k) == per_k - 1)
            def _():
                leave(k)

            return carry

        lax.fori_loop(0, count // 2 - 1, step, 0)
        point(1)
        products(count - 2, 0)
        products(count - 1, 1)
        leave(chunks - 1)

    def give_rows(k):
        return pl.ds(pl.multiple_of(lax.rem(k, 2) * TILE, TILE), TILE)

    def d_rows(k):
        return pl.ds(pl.multiple_of(chunk_of(k) * TILE, TILE), TILE)

    base = 9

    def hand(k):
        return pltpu.make_async_remote_copy(
            src_ref=give.at[give_rows(k)], dst_ref=d_txt.at[d_rows(k)], send_sem=core_s.at[base + k], recv_sem=core_r.at[base + k], device_id=partner, device_id_type=MESH
        )

    def enter_give(k):
        @pl.when(k >= 2)
        def _():
            hand(k - 2).wait_send()

        give[give_rows(k), :] = jnp.zeros((TILE, give.shape[1]), F32)

    sweep(1 - c, lambda k: (give, give_rows(k)), False, enter_give, lambda k: hand(k).start())
    sweep(c, lambda k: (d_txt, d_rows(k)), True, lambda k: hand(k).wait_recv(), lambda k: None)
    hand(2).wait_send()
    hand(3).wait_send()

    wi, wt = Wire(is_s, is_r), Wire(ts_s, ts_r)
    di_blk, di_half = rows_of(d_img, block)
    dt_blk, dt_half = rows_of(d_txt, block)

    def finish(out, mine):
        def done(p, q, r):
            out[...] = (mine[...] + p[...]) + (q[...] + r[...])

        return done

    run_both(
        scatter_stages(gi, wi, di_blk, di_half, (ibuf, ihalf), finish(d_img_out, di_blk(gi.slot(False, 0)))),
        scatter_stages(gt, wt, dt_blk, dt_half, (tbuf, thalf), finish(d_txt_out, dt_blk(gt.slot(False, 0)))),
    )
    wi.drain()
    wt.drain()


def main_call(scal, img_emb, txt_emb, x_give):
    block, dim = img_emb.shape
    vmem = pl.BlockSpec(memory_space=pltpu.VMEM)
    hbm = pl.BlockSpec(memory_space=pl.ANY)
    sem = pltpu.SemaphoreType.DMA
    f = lambda *s: pltpu.VMEM(s, F32)
    return pl.pallas_call(
        functools.partial(main_kernel, block),
        in_specs=[pl.BlockSpec(memory_space=pltpu.SMEM), vmem, vmem, hbm],
        out_specs=[vmem, vmem, vmem, hbm],
        out_shape=[
            jax.ShapeDtypeStruct((block, dim), F32),
            jax.ShapeDtypeStruct((block, dim), F32),
            jax.ShapeDtypeStruct((3, 8, 128), F32),
            jax.ShapeDtypeStruct(x_give.shape, x_give.dtype),
        ],
        scratch_shapes=[
            pltpu.VMEM((8 * block, dim), BF16),
            pltpu.VMEM((16 * block, dim), BF16),
            f(8 * block, dim),
            f(8 * block, dim),
            f(2 * TILE, dim),
            f(2, TILE, TILE),
            pltpu.VMEM((2, TILE, TILE), BF16),
            f(6, block, dim),
            f(2, block // 2, dim),
            f(6, block, dim),
            f(2, block // 2, dim),
            sem((GATHER_COPIES,)), sem((GATHER_COPIES,)), sem((GATHER_COPIES,)), sem((GATHER_COPIES,)),
            sem((SCATTER_COPIES,)), sem((SCATTER_COPIES,)), sem((SCATTER_COPIES,)), sem((SCATTER_COPIES,)),
            sem((13,)), sem((13,)), sem((2,)),
        ],
        compiler_params=pltpu.CompilerParams(collective_id=0, has_side_effects=True, vmem_limit_bytes=VMEM_LIMIT),
        name="scores",
    )(scal, img_emb, txt_emb, x_give)


def sum_kernel(
    x_own, x_got, du_own, sums_in, out, sums,
    w, du, abuf, ahalf, bbuf, bhalf, abuf2, ahalf2, bbuf2, bhalf2, small,
    du_s, du_r, a1s, a1r, b1s, b1r, a2s, a2r, b2s, b2r, a3s, a3r, b3s, b3r, a4s, a4r, b4s, b4r, d_s, d_r, q_s, q_r,
):
    place = Place()
    gi, gt = place.image_group(), place.text_group()
    c = place.c
    partner = place.partner()
    greet(place)
    block = du_own.shape[1]
    img_f = (w.shape[0] // 5) * 4
    pre = Wire(du_s, du_r)
    pre.go(0, du_own, du, partner)

    def outer(lhs, rhs):
        return lax.dot_general(lhs, rhs, (((0,), (0,)), ((), ())), preferred_element_type=F32)

    w[:img_f] = outer(x_own[:, :img_f], du_own[0])
    w[img_f:] = outer(x_own[:, img_f:], du_own[1])
    pre.got(0, du, partner)
    w[:img_f] += outer(x_got[:, :img_f], du[0])
    w[img_f:] += outer(x_got[:, img_f:], du[1])
    pre.drain()

    small_wire = Wire(q_s, q_r)
    hops = [
        place.at(x=place.near(place.x)), place.at(x=place.far(place.x)), place.at(y=place.near(place.y)), place.at(y=place.far(place.y)),
        place.at(z=place.near(place.z)), place.at(z=place.far(place.z)), partner,
    ]
    small[0] = sums_in[...]

    def small_send(k):
        small_wire.go(k, small.at[2 * k], small.at[2 * k + 1], hops[k])

    def small_take(k):
        small_wire.got(k, small.at[2 * k + 1], hops[k])
        small[2 * k + 2] = small[2 * k] + small[2 * k + 1]

    rows = w.shape[0] // 16
    lanes = w.shape[1] // 8

    def colour(n, g1, g2, s1, s2, s3, s4, buf1, half1, buf2, half2):
        base = n * 8 * rows
        mine = base + g1.slot(False, 0) * rows

        def view(ref):
            def blk(slot):
                return ref.at[pl.ds(pl.multiple_of(base + slot * rows, rows), rows)]

            def half(slot, h):
                return ref.at[pl.ds(pl.multiple_of(base + slot * rows + h * (rows // 2), rows // 2), rows // 2)]

            return blk, half

        def strip(ref):
            def blk(slot):
                return ref.at[pl.ds(pl.multiple_of(mine, rows), rows), pl.ds(pl.multiple_of(slot * lanes, lanes), lanes)]

            def half(slot, h):
                return ref.at[pl.ds(pl.multiple_of(mine + h * (rows // 2), rows // 2), rows // 2), pl.ds(pl.multiple_of(slot * lanes, lanes), lanes)]

            return blk, half

        wires = [Wire(*s) for s in (s1, s2, s3, s4)]
        w_blk, w_half = view(w)
        ws_blk, ws_half = strip(w)
        o_blk, o_half = view(out.at[c])
        os_blk, os_half = strip(out.at[c])

        def done1(p, q, r):
            v = w_blk(g1.slot(False, 0))
            v[...] += p[...] + q[...] + r[...]

        def done2(p, q, r):
            me = g2.slot(False, 0)
            v = os_blk(me)
            v[...] = ws_blk(me)[...] + p[...] + q[...] + r[...]

        me2 = g2.slot(False, 0)
        count = [n * 8]

        def share(slot):
            dwire.go(count[0], o_blk(slot), o_blk(slot), partner)
            count[0] += 1

        def share_own():
            share(g1.slot(False, 0))

        stages = scatter_stages(g1, wires[0], w_blk, w_half, (buf1, half1), done1)
        stages += scatter_stages(g2, wires[1], ws_blk, ws_half, (buf2, half2), done2)
        stages += gather_stages(g2, wires[2], os_blk(me2), os_blk, os_half)
        tail = gather_stages(g1, wires[3], o_blk(g1.slot(False, 0)), o_blk, o_half, share)
        stages += [tail[0], share_own] + tail[1:]
        return stages, wires

    dwire = Wire(d_s, d_r)
    sa, wa = colour(0, gi, gt, (a1s, a1r), (a2s, a2r), (a3s, a3r), (a4s, a4r), abuf, ahalf, abuf2, ahalf2)
    sb, wb = colour(1, gt, gi, (b1s, b1r), (b2s, b2r), (b3s, b3r), (b4s, b4r), bbuf, bhalf, bbuf2, bhalf2)
    for n, (fa, fb) in enumerate(zip(sa, sb)):
        fa()
        fb()
        if n < 8:
            if n > 0:
                small_take(n - 1)
            if n < 7:
                small_send(n)
    sums[...] = small[14]
    order = [(False, 0), (False, -1), (False, 1), (True, 0), (False, 2), (True, -1), (True, 1), (True, 2)]
    for n, g1 in ((0, gi), (1, gt)):
        for k, (twin, step) in enumerate(order):
            v = out.at[1 - c].at[pl.ds(pl.multiple_of(n * 8 * rows + g1.slot(twin, step) * rows, rows), rows)]
            dwire.got(n * 8 + k, v, partner)
    for wire in wa + wb + [dwire, small_wire]:
        wire.drain()


def sum_call(x_own, x_got, du, sums):
    block, feats = x_own.shape
    dim = du.shape[2]
    vmem = pl.BlockSpec(memory_space=pltpu.VMEM)
    sem = pltpu.SemaphoreType.DMA
    f = lambda *s: pltpu.VMEM(s, F32)
    rows, lanes = feats // 16, dim // 8
    sc, ga = sem((SCATTER_COPIES,)), sem((GATHER_COPIES,))
    return pl.pallas_call(
        sum_kernel,
        in_specs=[vmem] * 4,
        out_specs=[vmem, vmem],
        out_shape=[jax.ShapeDtypeStruct((2, feats, dim), F32), jax.ShapeDtypeStruct(sums.shape, F32)],
        scratch_shapes=[
            f(feats, dim),
            pltpu.VMEM(du.shape, BF16),
            f(6, rows, dim), f(2, rows // 2, dim), f(6, rows, dim), f(2, rows // 2, dim),
            f(6, rows, lanes), f(2, rows // 2, lanes), f(6, rows, lanes), f(2, rows // 2, lanes),
            f(15, *sums.shape),
            sem((1,)), sem((1,)),
            sc, sc, sc, sc, sc, sc, sc, sc,
            ga, ga, ga, ga, ga, ga, ga, ga,
            sem((16,)), sem((16,)), sem((7,)), sem((7,)),
        ],
        compiler_params=pltpu.CompilerParams(collective_id=1, has_side_effects=True, vmem_limit_bytes=VMEM_LIMIT),
        name="weights",
    )(x_own, x_got, du, sums)


def solution(mesh):
    dev_count = mesh.shape["replica"] * mesh.shape["data"]
    batch_axes = ("replica", "data")

    def local_fn(img_x, txt_x, w_img, w_txt, log_temp, logit_bias):
        block = img_x.shape[0]
        total_rows = block * dev_count
        img_f, txt_f = img_x.shape[1] // 2, txt_x.shape[1] // 2
        core = lax.rem(lax.axis_index("data"), 2)

        def halves(which):
            a = lax.dynamic_slice_in_dim(img_x, which * img_f, img_f, axis=1)
            b = lax.dynamic_slice_in_dim(txt_x, which * txt_f, txt_f, axis=1)
            return jnp.concatenate([a, b], axis=1)

        txt_emb, txt_pull = embed_rows(txt_x, w_txt)
        img_emb, img_pull = embed_rows(img_x, w_img)
        temp_scale = jnp.exp(log_temp[0])
        scal = jnp.stack([temp_scale, logit_bias[0]])
        d_img, d_txt, sums, x_got = main_call(scal, img_emb, txt_emb, halves(1 - core))
        post = temp_scale / total_rows
        d_img_raw = img_pull(post * d_img)[0].astype(BF16)
        d_txt_raw = txt_pull(post * d_txt)[0].astype(BF16)
        grads, sums = sum_call(halves(core), x_got, jnp.stack([d_img_raw, d_txt_raw]), sums)
        d_w_img = grads[:, :img_f].reshape(2 * img_f, -1)
        d_w_txt = grads[:, img_f:].reshape(2 * txt_f, -1)
        parts = jnp.sum(sums, axis=(1, 2)) / total_rows
        return parts[0:1], temp_scale * parts[1:2], parts[2:3], d_w_img, d_w_txt

    batch_spec = P(batch_axes, None)
    return jax.shard_map(local_fn, mesh=mesh, in_specs=(batch_spec, batch_spec, P(), P(), P(), P()), out_specs=(P(), P(), P(), P(), P()), check_vma=False)
```

```python
import functools

import jax
import jax.numpy as jnp
from jax import lax
from jax.experimental import pallas as pl
from jax.experimental.pallas import tpu as pltpu
from jax.sharding import PartitionSpec as P

F32 = jnp.float32
BF16 = jnp.bfloat16
TILE = 512
MESH = pl.DeviceIdType.MESH
VMEM_LIMIT = 67043328


def normalize(raw):
    return raw * lax.rsqrt(jnp.sum(raw * raw, axis=-1, keepdims=True))


def embed_rows(feat_x, w_proj):
    raw_emb = jnp.dot(feat_x, w_proj, preferred_element_type=F32)
    unit_emb, pull_back = jax.vjp(normalize, raw_emb)
    return unit_emb.astype(BF16), pull_back


class Place:
    def __init__(self):
        rep, dat = lax.axis_index("replica"), lax.axis_index("data")
        self.z, self.y = lax.div(rep, 4), lax.rem(rep, 4)
        self.x, self.c = lax.div(dat, 2), lax.rem(dat, 2)

    def at(self, x=None, y=None, z=None, c=None):
        x = self.x if x is None else lax.rem(x + 8, 4)
        y = self.y if y is None else lax.rem(y + 8, 4)
        z = self.z if z is None else lax.rem(z + 8, 4)
        c = self.c if c is None else c
        return (z * 4 + y, x * 2 + c)

    def partner(self):
        return self.at(c=1 - self.c)

    def near(self, v):
        return v + 1 - 2 * lax.rem(v, 2)

    def far(self, v):
        return v - 1 + 2 * lax.rem(v, 2)

    def image_group(self):
        return Group(self.x, lax.rem(lax.div(self.y + 1, 2), 2), self.at(x=self.x + 1), self.at(x=self.x - 1), self.at(y=self.near(self.y)))

    def text_group(self):
        return Group(self.z, lax.div(self.y, 2), self.at(z=self.z + 1), self.at(z=self.z - 1), self.at(y=self.far(self.y)))

    def peers(self):
        out = [self.partner()]
        for g in (self.image_group(), self.text_group()):
            out += [g.right, g.left, g.pair]
        return out


class Group:
    def __init__(self, pos, side, right, left, pair):
        self.pos, self.side, self.right, self.left, self.pair = pos, side, right, left, pair

    def slot(self, key):
        side = 1 - self.side if key[0] else self.side
        return side * 4 + lax.rem(self.pos + key[1] + 4, 4)


def greet(place):
    barrier = pltpu.get_barrier_semaphore()
    peers = place.peers()
    for dev in peers:
        pl.semaphore_signal(barrier, inc=1, device_id=dev, device_id_type=MESH)
    pl.semaphore_wait(barrier, len(peers))


class Wire:
    def __init__(self, send, recv):
        self.send, self.recv, self.open = send, recv, []

    def copy(self, k, src, dst, dev):
        return pltpu.make_async_remote_copy(src_ref=src, dst_ref=dst, send_sem=self.send.at[k], recv_sem=self.recv.at[k], device_id=dev, device_id_type=MESH)

    def go(self, *what):
        self.copy(*what).start()
        self.open.append(what)

    def got(self, k, dst, dev):
        self.copy(k, dst, dst, dev).wait_recv()

    def drain(self):
        for what in self.open:
            self.copy(*what).wait_send()
        self.open = []


class Pieces:
    def __init__(self, send, recv):
        self.wire = Wire(send, recv)

    def go(self, k, src, dst, dev):
        for p in range(2):
            self.wire.go(2 * k + p, src[p], dst[p], dev)

    def got(self, k, dst, dev):
        for p in range(2):
            self.wire.got(2 * k + p, dst[p], dev)

    def drain(self):
        self.wire.drain()


GATHER_COPIES = 8
SCATTER_COPIES = 10


def gather_stages(wire, g, own, blk, half, relative, seen=None):
    seen = seen or (lambda key: None)

    def moved(key, way):
        twin, step = key
        if not relative:
            return key
        return {"right": (twin, step - 1), "left": (twin, step + 1), "pair": (not twin, step)}[way]

    def send(k, key, way, h=None):
        dev = getattr(g, way)
        view = blk if h is None else functools.partial(half, h=h)
        wire.go(k, view(key), view(moved(key, way)), dev)

    def start():
        for k, way in enumerate(("right", "left", "pair")):
            wire.go(k, own, blk(moved((False, 0), way)), getattr(g, way))

    def ring():
        wire.got(0, blk((False, -1)), g.left)
        send(3, (False, -1), "right", 0)
        wire.got(1, blk((False, 1)), g.right)
        send(4, (False, 1), "left", 1)
        seen((False, -1))
        seen((False, 1))

    def twin():
        wire.got(2, blk((True, 0)), g.pair)
        send(5, (True, 0), "right")
        send(6, (True, 0), "left")
        seen((True, 0))

    def across():
        wire.got(3, half((False, 2), 0), g.left)
        wire.got(4, half((False, 2), 1), g.right)
        send(7, (False, 2), "pair")
        seen((False, 2))

    def last():
        wire.got(5, blk((True, -1)), g.left)
        wire.got(6, blk((True, 1)), g.right)
        seen((True, -1))
        seen((True, 1))
        wire.got(7, blk((True, 2)), g.pair)
        seen((True, 2))

    return [start, ring, twin, across, last]


SEEN = [(False, 0), (False, -1), (False, 1), (True, 0), (False, 2), (True, -1), (True, 1), (True, 2)]


class Scatter:
    def __init__(self, wire, g, blk, half, bufs, finish):
        self.wire, self.g, self.blk, self.half, self.finish = wire, g, blk, half, finish
        whole, part = bufs
        self.rp, self.rr0, self.rr1, self.rf0, self.rf1, self.rf2 = (whole.at[k] for k in range(6))
        self.rh0, self.rh1 = part.at[0], part.at[1]
        rows = part.shape[1]
        self.lo, self.hi = pl.ds(0, rows), pl.ds(rows, rows)

    def twins(self):
        self.wire.go(1, self.blk((True, 1)), self.rr0, self.g.right)
        self.wire.go(2, self.blk((True, -1)), self.rr1, self.g.left)

    def opposite(self):
        self.wire.go(0, self.blk((True, 2)), self.rp, self.g.pair)

    def early(self):
        self.wire.go(3, self.half((False, 1), 1), self.rf0.at[self.hi], self.g.right)
        self.wire.go(4, self.half((False, -1), 0), self.rf1.at[self.lo], self.g.left)

    def across(self):
        self.wire.got(0, self.rp, self.g.pair)
        for h, sl in ((0, self.lo), (1, self.hi)):
            v = self.half((False, 2), h)
            v[...] += self.rp[sl]
        self.wire.go(5, self.half((False, 2), 0), self.rh0, self.g.right)
        self.wire.go(6, self.half((False, 2), 1), self.rh1, self.g.left)

    def twin(self):
        self.wire.got(1, self.rr0, self.g.left)
        self.wire.got(2, self.rr1, self.g.right)
        v = self.blk((True, 0))
        v[...] += self.rr0[...] + self.rr1[...]
        self.wire.go(7, v, self.rf2, self.g.pair)

    def ring(self):
        self.wire.got(5, self.rh0, self.g.left)
        v = self.half((False, 1), 0)
        v[...] += self.rh0[...]
        self.wire.go(8, v, self.rf0.at[self.lo], self.g.right)
        self.wire.got(6, self.rh1, self.g.right)
        v = self.half((False, -1), 1)
        v[...] += self.rh1[...]
        self.wire.go(9, v, self.rf1.at[self.hi], self.g.left)

    def last(self):
        self.wire.got(3, self.rf0.at[self.hi], self.g.left)
        self.wire.got(4, self.rf1.at[self.lo], self.g.right)
        self.wire.got(7, self.rf2, self.g.pair)
        self.wire.got(8, self.rf0.at[self.lo], self.g.left)
        self.wire.got(9, self.rf1.at[self.hi], self.g.right)
        self.finish(self.rf0, self.rf1, self.rf2)

    def stages(self):
        def start():
            self.opposite()
            self.twins()
            self.early()

        return [start, self.across, self.twin, self.ring, self.last]


def run_both(a, b):
    for fa, fb in zip(a, b):
        fa()
        fb()


PLACE = {(False, 0): 0, (True, 0): 1, (False, 1): 2, (False, 3): 3, (True, 2): 4, (False, 2): 5, (True, 1): 6, (True, 3): 7}


def rows_of(ref, size, base=0):
    def at(key):
        return base + PLACE[key[0], key[1] % 4] * size

    def blk(key):
        return ref.at[pl.ds(at(key), size)]

    def half(key, h):
        return ref.at[pl.ds(at(key) + h * (size // 2), size // 2)]

    return blk, half


def score_terms(sim, scale, bias, diag):
    z = scale * sim + bias
    if diag is not None:
        z = jnp.where(diag, -z, z)
    e = jnp.exp(-jnp.abs(z))
    r = 1.0 / (1.0 + e)
    g = jnp.where(z >= 0.0, r, e * r)
    loss = jnp.maximum(z, 0.0) + jnp.log1p(e)
    if diag is not None:
        g = jnp.where(diag, -g, g)
    return loss, g


def fold(x):
    x = jnp.sum(x.reshape(x.shape[0] // 8, 8, x.shape[1]), axis=0)
    return sum(x[:, k * 128 : (k + 1) * 128] for k in range(x.shape[1] // 128))


def tile_of(m):
    div, least = (lambda a, b: a // b, min) if isinstance(m, int) else (lax.div, jnp.minimum)
    q = 3 - least(div(m, 7), 1) - least(div(m, 12), 1) - div(m, 15)
    r = m - (16 - (q + 1) * (q + 1))
    down = least(div(r, q + 1), 1)
    return q + down * (r - q - 1 - q), r + down * (q - r)


def main_kernel(
    block, scal, img_own, txt_own, img_x, txt_x, d_img_out, d_txt_out, sums, x_got,
    img, txt, d_img, d_txt, give, taken, sbuf, gbuf,
    ibuf, ihalf, tbuf, thalf,
    ig_s, ig_r, tg_s, tg_r, is_s, is_r, ts_s, ts_r, core_s, core_r, hand_s, hand_r, local, free,
):
    place = Place()
    gi, gt = place.image_group(), place.text_group()
    c = place.c
    partner = place.partner()
    greet(place)

    half_rows = 8 * block
    img_blk, img_half = rows_of(img, block)
    txt_blk, txt_half = rows_of(txt, block, half_rows)
    other_blk, _ = rows_of(txt, block)
    wi, wt, core = Wire(ig_s, ig_r), Wire(tg_s, tg_r), Wire(core_s, core_r)

    own_i = pltpu.make_async_copy(img_own, img_blk((False, 0)), local.at[0])
    own_t = pltpu.make_async_copy(txt_own, txt_blk((False, 0)), local.at[1])
    own_i.start()
    own_t.start()
    own_i.wait()
    own_t.wait()
    sent = iter(range(8))

    def share(key):
        core.go(next(sent), txt_blk(key), other_blk(key), partner)

    a = gather_stages(wi, gi, img_blk((False, 0)), img_blk, img_half, True)
    b = gather_stages(wt, gt, txt_blk((False, 0)), txt_blk, txt_half, True, share)
    a[0]()
    b[0]()
    share((False, 0))
    img_f, txt_f = img_x.shape[1] // 2, txt_x.shape[1] // 2
    core.go(8, img_x.at[:, pl.ds(pl.multiple_of((1 - c) * img_f, img_f), img_f)], x_got.at[:, pl.ds(0, img_f)], partner)
    core.go(9, txt_x.at[:, pl.ds(pl.multiple_of((1 - c) * txt_f, txt_f), txt_f)], x_got.at[:, pl.ds(img_f, txt_f)], partner)
    for ref in (d_img, d_txt, give, sums):
        ref[...] = jnp.zeros_like(ref)
    run_both(a[1:], b[1:])
    for k, key in enumerate(SEEN):
        core.got(k, other_blk(key), partner)
    core.got(8, x_got.at[:, pl.ds(0, img_f)], partner)
    core.got(9, x_got.at[:, pl.ds(img_f, txt_f)], partner)
    for wire in (wi, wt, core):
        wire.drain()

    scale, bias = scal[0], scal[1]
    di_blk, di_half = rows_of(d_img, block)
    dt_blk, dt_half = rows_of(d_txt, block)

    outs = []

    def finish(out, mine, k):
        def done(p, q, r):
            mine[...] += p[...] + (q[...] + r[...])
            copy = pltpu.make_async_copy(mine, out, local.at[k])
            copy.start()
            outs.append(copy)

        return done

    wi, wt = Wire(is_s, is_r), Wire(ts_s, ts_r)
    ri = Scatter(wi, gi, di_blk, di_half, (ibuf, ihalf), finish(d_img_out, di_blk((False, 0)), 0))
    rt = Scatter(wt, gt, dt_blk, dt_half, (tbuf, thalf), finish(d_txt_out, dt_blk((False, 0)), 1))

    def hand(k):
        return pltpu.make_async_remote_copy(
            src_ref=give.at[pl.ds(k * TILE, TILE)], dst_ref=taken.at[k % 2], send_sem=hand_s.at[k], recv_sem=hand_r.at[k], device_id=partner, device_id_type=MESH
        )

    def give_chunk(k):
        if k < 2:
            pl.semaphore_wait(free, 1)
        hand(k).start()

    def take_chunk(k):
        hand(k).wait_recv()
        v = d_txt.at[pl.ds(k * TILE, TILE)]
        v[...] += taken[k % 2]
        if k >= 2:
            pl.semaphore_signal(free, inc=1, device_id=partner, device_id_type=MESH)

    def rows(chunk, first=0):
        at = first + chunk * TILE
        return pl.ds(at if isinstance(at, int) else pl.multiple_of(at, TILE), TILE)

    def txt_rows(cc, chunk):
        return rows(chunk, cc * half_rows)

    def score(m, cc):
        i, j = tile_of(m)
        sbuf[cc] = lax.dot_general(img[rows(i), :], txt[txt_rows(cc, j), :], (((1,), (1,)), ((), ())), preferred_element_type=F32)

    def point(cc, diag=None):
        sim = sbuf[cc]
        loss, g = score_terms(sim, scale, bias, diag)
        sums[0] += fold(loss)
        sums[1] += fold(g * sim)
        sums[2] += fold(g)
        gbuf[cc] = g.astype(BF16)

    def products(m, cc):
        i, j = tile_of(m)
        gb = gbuf[cc]
        d_img[rows(i), :] += jnp.dot(gb, txt[txt_rows(cc, j), :], preferred_element_type=F32)
        ref = d_txt if cc else give
        ref[rows(j), :] += lax.dot_general(gb, img[rows(i), :], (((0,), (0,)), ((), ())), preferred_element_type=F32)

    events = {
        3: [ri.twins],
        6: [lambda: give_chunk(3)],
        7: [lambda: take_chunk(3), rt.twins],
        9: [ri.opposite],
        11: [lambda: give_chunk(2)],
        12: [lambda: take_chunk(2), rt.opposite],
        13: [ri.early],
        14: [lambda: give_chunk(1)],
    }
    score(0, 0)
    score(0, 1)
    point(0)

    def step(m, carry):
        score(m + 1, 0)
        point(1)
        products(m, 0)
        score(m + 1, 1)
        point(0)
        products(m, 1)
        for at, todo in events.items():
            @pl.when(m == at)
            def _(todo=todo):
                for f in todo:
                    f()

        return carry

    lax.fori_loop(0, 15, step, 0)
    row = lax.broadcasted_iota(jnp.int32, (TILE, TILE), 0)
    col = lax.broadcasted_iota(jnp.int32, (TILE, TILE), 1)
    point(1, (row == col) & (row < block))
    products(15, 0)
    give_chunk(0)
    products(15, 1)
    ri.across()
    take_chunk(1)
    rt.early()
    ri.twin()
    take_chunk(0)
    rt.twin()
    rt.across()
    ri.ring()
    rt.ring()
    ri.last()
    rt.last()
    for k in range(4):
        hand(k).wait_send()
    for copy in outs:
        copy.wait()
    wi.drain()
    wt.drain()


def main_call(scal, img_emb, txt_emb, img_x, txt_x):
    block, dim = img_emb.shape
    vmem = pl.BlockSpec(memory_space=pltpu.VMEM)
    hbm = pl.BlockSpec(memory_space=pl.ANY)
    sem = pltpu.SemaphoreType.DMA
    f = lambda *s: pltpu.VMEM(s, F32)
    return pl.pallas_call(
        functools.partial(main_kernel, block),
        in_specs=[pl.BlockSpec(memory_space=pltpu.SMEM), hbm, hbm, hbm, hbm],
        out_specs=[hbm, hbm, vmem, hbm],
        out_shape=[
            jax.ShapeDtypeStruct((block, dim), F32),
            jax.ShapeDtypeStruct((block, dim), F32),
            jax.ShapeDtypeStruct((3, 8, 128), F32),
            jax.ShapeDtypeStruct((block, (img_x.shape[1] + txt_x.shape[1]) // 2), BF16),
        ],
        scratch_shapes=[
            pltpu.VMEM((8 * block, dim), BF16),
            pltpu.VMEM((16 * block, dim), BF16),
            f(8 * block, dim),
            f(8 * block, dim),
            f(8 * block, dim),
            f(2, TILE, dim),
            f(2, TILE, TILE),
            pltpu.VMEM((2, TILE, TILE), BF16),
            f(6, block, dim),
            f(2, block // 2, dim),
            f(6, block, dim),
            f(2, block // 2, dim),
            sem((GATHER_COPIES,)), sem((GATHER_COPIES,)), sem((GATHER_COPIES,)), sem((GATHER_COPIES,)),
            sem((SCATTER_COPIES,)), sem((SCATTER_COPIES,)), sem((SCATTER_COPIES,)), sem((SCATTER_COPIES,)),
            sem((10,)), sem((10,)), sem((4,)), sem((4,)), sem((2,)), pltpu.SemaphoreType.REGULAR,
        ],
        compiler_params=pltpu.CompilerParams(collective_id=0, has_side_effects=True, vmem_limit_bytes=VMEM_LIMIT),
        name="scores",
    )(scal, img_emb, txt_emb, img_x, txt_x)


def sum_kernel(
    img_x, txt_x, x_got, du_own, sums_in, d_w_img, d_w_txt, sums,
    w, w2, du, abuf, ahalf, bbuf, bhalf, abuf2, ahalf2, bbuf2, bhalf2, small,
    du_s, du_r, a1s, a1r, b1s, b1r, a2s, a2r, b2s, b2r, a3s, a3r, b3s, b3r, a4s, a4r, b4s, b4r, d_s, d_r, q_s, q_r, local,
):
    place = Place()
    gi, gt = place.image_group(), place.text_group()
    c = place.c
    partner = place.partner()
    greet(place)
    img_f, txt_f = img_x.shape[1] // 2, txt_x.shape[1] // 2
    ni, nt = img_f // 16, txt_f // 16
    rows, lanes = ni + nt, w.shape[1] // 8
    pre = Wire(du_s, du_r)
    pre.go(0, du_own, du, partner)

    def outer(lhs, rhs):
        return lax.dot_general(lhs, rhs, (((0,), (0,)), ((), ())), preferred_element_type=F32)

    def weights(own, part):
        rhs = du_own if own else du
        for k in range(img_f // 128):
            cols = pl.ds(pl.multiple_of(c * img_f + k * 128, 128), 128)
            lhs = img_x[:, cols] if own else x_got[:, k * 128 : (k + 1) * 128]
            put(part, k * 128, 128, ni, 0, outer(lhs, rhs[0]), own)
        for k in range(txt_f // 128):
            cols = pl.ds(pl.multiple_of(c * txt_f + k * 128, 128), 128)
            lhs = txt_x[:, cols] if own else x_got[:, img_f + k * 128 : img_f + (k + 1) * 128]
            put(part, k * 128, 128, nt, ni, outer(lhs, rhs[1]), own)

    def put(ref, first, count, size, shift, val, fresh):
        for b in range(count // size):
            at = ((first + b * size) // size) * rows + shift
            piece = val[b * size : (b + 1) * size]
            if fresh:
                ref[at : at + size] = piece
            else:
                ref[at : at + size] += piece

    weights(True, w)
    pre.got(0, du, partner)
    weights(False, w)
    pre.drain()

    small_wire = Wire(q_s, q_r)
    hops = [
        place.at(x=place.near(place.x)), place.at(x=place.far(place.x)), place.at(y=place.near(place.y)), place.at(y=place.far(place.y)),
        place.at(z=place.near(place.z)), place.at(z=place.far(place.z)), partner,
    ]
    small[0] = sums_in[...]

    def small_send(k):
        small_wire.go(k, small.at[2 * k], small.at[2 * k + 1], hops[k])

    def small_take(k):
        small_wire.got(k, small.at[2 * k + 1], hops[k])
        small[2 * k + 2] = small[2 * k] + small[2 * k + 1]

    dwire = Pieces(d_s, d_r)
    copies = []

    def colour(n, g1, g2, s1, s2, s3, s4, buf1, half1, buf2, half2):
        base = n * 8 * rows
        mine = base + g1.slot((False, 0)) * rows

        def sl(first, count):
            return pl.ds(pl.multiple_of(first, count), count)

        def w_blk(key):
            return w.at[sl(base + g1.slot(key) * rows, rows)]

        def w_half(key, h):
            return w.at[sl(base + g1.slot(key) * rows + h * (rows // 2), rows // 2)]

        def strip(ref, first):
            def blk(key):
                return ref.at[sl(first, rows), sl(g2.slot(key) * lanes, lanes)]

            def half(key, h):
                return ref.at[sl(first + h * (rows // 2), rows // 2), sl(g2.slot(key) * lanes, lanes)]

            return blk, half

        def o_half(key, h):
            i0 = c * img_f + (n * 8 + g1.slot(key)) * ni
            t0 = c * txt_f + (n * 8 + g1.slot(key)) * nt
            return d_w_img.at[sl(i0 + h * (ni // 2), ni // 2)], d_w_txt.at[sl(t0 + h * (nt // 2), nt // 2)]

        def o_blk(key, core=c):
            i0 = core * img_f + (n * 8 + g1.slot(key)) * ni
            t0 = core * txt_f + (n * 8 + g1.slot(key)) * nt
            return d_w_img.at[sl(i0, ni)], d_w_txt.at[sl(t0, nt)]

        w1, wire2, w3 = Wire(*s1), Wire(*s2), Wire(*s3)
        w4 = Pieces(*s4)
        ws_blk, ws_half = strip(w, mine)
        os_blk, os_half = strip(w2, n * rows)
        home = (False, 0)

        def done1(p, q, r):
            v = w_blk(home)
            v[...] += p[...] + q[...] + r[...]

        def done2(p, q, r):
            v = os_blk(home)
            v[...] = ws_blk(home)[...] + p[...] + q[...] + r[...]

        count = [n * 8]
        whole = w2.at[n * rows : n * rows + ni], w2.at[n * rows + ni : (n + 1) * rows]

        def share(key, src=None):
            dwire.go(count[0], o_blk(key) if src is None else src, o_blk(key), partner)
            count[0] += 1

        def share_own():
            share(home, whole)
            for p, (src, dst) in enumerate(zip(whole, o_blk(home))):
                copy = pltpu.make_async_copy(src, dst, local.at[2 * n + p])
                copy.start()
                copies.append(copy)

        def got_shares():
            for k, key in enumerate(SEEN):
                dwire.got(n * 8 + k, o_blk(key, 1 - c), partner)

        stages = Scatter(w1, g1, w_blk, w_half, (buf1, half1), done1).stages()
        stages += Scatter(wire2, g2, ws_blk, ws_half, (buf2, half2), done2).stages()
        stages += gather_stages(w3, g2, os_blk(home), os_blk, os_half, False)
        tail = gather_stages(w4, g1, whole, o_blk, o_half, False, share)
        stages += [tail[0], share_own] + tail[1:] + [got_shares]
        return stages, [w1, wire2, w3, w4]

    sa, wa = colour(0, gi, gt, (a1s, a1r), (a2s, a2r), (a3s, a3r), (a4s, a4r), abuf, ahalf, abuf2, ahalf2)
    sb, wb = colour(1, gt, gi, (b1s, b1r), (b2s, b2r), (b3s, b3r), (b4s, b4r), bbuf, bhalf, bbuf2, bhalf2)
    for n, (fa, fb) in enumerate(zip(sa, sb)):
        fa()
        fb()
        if 0 < n < 8:
            small_take(n - 1)
        if n < 7:
            small_send(n)
    sums[...] = small[14]
    for copy in copies:
        copy.wait()
    for wire in wa + wb + [dwire, small_wire]:
        wire.drain()


def sum_call(img_x, txt_x, x_got, du, sums):
    block = img_x.shape[0]
    feats = x_got.shape[1]
    dim = du.shape[2]
    vmem = pl.BlockSpec(memory_space=pltpu.VMEM)
    hbm = pl.BlockSpec(memory_space=pl.ANY)
    sem = pltpu.SemaphoreType.DMA
    f = lambda *s: pltpu.VMEM(s, F32)
    rows, lanes = feats // 16, dim // 8
    sc, ga, ga2 = sem((SCATTER_COPIES,)), sem((GATHER_COPIES,)), sem((2 * GATHER_COPIES,))
    return pl.pallas_call(
        sum_kernel,
        in_specs=[vmem] * 5,
        out_specs=[hbm, hbm, vmem],
        out_shape=[
            jax.ShapeDtypeStruct((img_x.shape[1], dim), F32),
            jax.ShapeDtypeStruct((txt_x.shape[1], dim), F32),
            jax.ShapeDtypeStruct(sums.shape, F32),
        ],
        scratch_shapes=[
            f(feats, dim),
            f(2 * rows, dim),
            pltpu.VMEM(du.shape, BF16),
            f(6, rows, dim), f(2, rows // 2, dim), f(6, rows, dim), f(2, rows // 2, dim),
            f(6, rows, lanes), f(2, rows // 2, lanes), f(6, rows, lanes), f(2, rows // 2, lanes),
            f(15, *sums.shape),
            sem((1,)), sem((1,)),
            sc, sc, sc, sc, sc, sc, sc, sc,
            ga, ga, ga, ga, ga2, ga2, ga2, ga2,
            sem((32,)), sem((32,)), sem((7,)), sem((7,)), sem((4,)),
        ],
        compiler_params=pltpu.CompilerParams(collective_id=1, has_side_effects=True, vmem_limit_bytes=28 * 2**20),
        name="weights",
    )(img_x, txt_x, x_got, du, sums)


def solution(mesh):
    dev_count = mesh.shape["replica"] * mesh.shape["data"]
    batch_axes = ("replica", "data")

    def local_fn(img_x, txt_x, w_img, w_txt, log_temp, logit_bias):
        block = img_x.shape[0]
        total_rows = block * dev_count
        txt_emb, txt_pull = embed_rows(txt_x, w_txt)
        img_emb, img_pull = embed_rows(img_x, w_img)
        temp_scale = jnp.exp(log_temp[0])
        scal = jnp.stack([temp_scale, logit_bias[0]])
        d_img, d_txt, sums, x_got = main_call(scal, img_emb, txt_emb, img_x, txt_x)
        post = temp_scale / total_rows
        d_img_raw = img_pull(post * d_img)[0].astype(BF16)
        d_txt_raw = txt_pull(post * d_txt)[0].astype(BF16)
        d_w_img, d_w_txt, sums = sum_call(img_x, txt_x, x_got, jnp.stack([d_img_raw, d_txt_raw]), sums)
        parts = jnp.sum(sums, axis=(1, 2)) / total_rows
        return parts[0:1], temp_scale * parts[1:2], parts[2:3], d_w_img, d_w_txt

    batch_spec = P(batch_axes, None)
    return jax.shard_map(local_fn, mesh=mesh, in_specs=(batch_spec, batch_spec, P(), P(), P(), P()), out_specs=(P(), P(), P(), P(), P()), check_vma=False)
```

```python
import functools

import jax
import jax.numpy as jnp
from jax import lax
from jax.experimental import pallas as pl
from jax.experimental.pallas import tpu as pltpu
from jax.sharding import PartitionSpec as P

F32 = jnp.float32
BF16 = jnp.bfloat16
TILE = 512
MESH = pl.DeviceIdType.MESH
VMEM_LIMIT = 67043328


def embed_rows(feat_x, w_proj):
    raw = jnp.dot(feat_x, w_proj, preferred_element_type=F32)
    return raw, (raw * lax.rsqrt(jnp.sum(raw * raw, axis=-1, keepdims=True))).astype(BF16)


class Place:
    def __init__(self):
        rep, dat = lax.axis_index("replica"), lax.axis_index("data")
        self.z, self.y = lax.div(rep, 4), lax.rem(rep, 4)
        self.x, self.c = lax.div(dat, 2), lax.rem(dat, 2)

    def at(self, x=None, y=None, z=None, c=None):
        x = self.x if x is None else lax.rem(x + 8, 4)
        y = self.y if y is None else lax.rem(y + 8, 4)
        z = self.z if z is None else lax.rem(z + 8, 4)
        c = self.c if c is None else c
        return (z * 4 + y, x * 2 + c)

    def partner(self):
        return self.at(c=1 - self.c)

    def near(self, v):
        return v + 1 - 2 * lax.rem(v, 2)

    def far(self, v):
        return v - 1 + 2 * lax.rem(v, 2)

    def image_group(self):
        return Group(self.x, lax.rem(lax.div(self.y + 1, 2), 2), self.at(x=self.x + 1), self.at(x=self.x - 1), self.at(y=self.near(self.y)))

    def text_group(self):
        return Group(self.z, lax.div(self.y, 2), self.at(z=self.z + 1), self.at(z=self.z - 1), self.at(y=self.far(self.y)))

    def peers(self):
        out = [self.partner()]
        for g in (self.image_group(), self.text_group()):
            out += [g.right, g.left, g.pair]
        return out


class Group:
    def __init__(self, pos, side, right, left, pair):
        self.pos, self.side, self.right, self.left, self.pair = pos, side, right, left, pair

    def slot(self, key):
        side = 1 - self.side if key[0] else self.side
        return side * 4 + lax.rem(self.pos + key[1] + 4, 4)


def greet(place):
    barrier = pltpu.get_barrier_semaphore()
    peers = place.peers()
    for dev in peers:
        pl.semaphore_signal(barrier, inc=1, device_id=dev, device_id_type=MESH)
    pl.semaphore_wait(barrier, len(peers))


class Wire:
    def __init__(self, send, recv, first=0):
        self.send, self.recv, self.first, self.open = send, recv, first, []

    def copy(self, k, src, dst, dev):
        k += self.first
        return pltpu.make_async_remote_copy(src_ref=src, dst_ref=dst, send_sem=self.send.at[k], recv_sem=self.recv.at[k], device_id=dev, device_id_type=MESH)

    def go(self, *what):
        self.copy(*what).start()
        self.open.append(what)

    def got(self, k, dst, dev):
        self.copy(k, dst, dst, dev).wait_recv()

    def drain(self):
        for what in self.open:
            self.copy(*what).wait_send()
        self.open = []


class Pieces:
    def __init__(self, *where):
        self.wire = Wire(*where)

    def go(self, k, src, dst, dev):
        for p in range(2):
            self.wire.go(2 * k + p, src[p], dst[p], dev)

    def got(self, k, dst, dev):
        for p in range(2):
            self.wire.got(2 * k + p, dst[p], dev)

    def drain(self):
        self.wire.drain()


GATHER_COPIES = 8
SCATTER_COPIES = 10
OWN, RIGHT, LEFT, FAR = ((0, step) for step in (0, 1, -1, 2))
TWIN, TWIN_RIGHT, TWIN_LEFT, TWIN_FAR = ((1, step) for step in (0, 1, -1, 2))


def gather_stages(wire, g, own, blk, half, relative, seen=None):
    seen = seen or (lambda key: None)

    def moved(key, way):
        twin, step = key
        if not relative:
            return key
        twin, step = {"right": (twin, step - 1), "left": (twin, step + 1), "pair": (1 - twin, step)}[way]
        return twin, (step + 1) % 4 - 1

    def send(k, key, way, h=None):
        dev = getattr(g, way)
        view = blk if h is None else functools.partial(half, h=h)
        wire.go(k, view(key), view(moved(key, way)), dev)

    def start():
        for k, way in enumerate(("right", "left", "pair")):
            wire.go(k, own, blk(moved(OWN, way)), getattr(g, way))

    def ring():
        wire.got(0, blk(LEFT), g.left)
        send(3, LEFT, "right", 0)
        wire.got(1, blk(RIGHT), g.right)
        send(4, RIGHT, "left", 1)
        seen(LEFT)
        seen(RIGHT)

    def twin():
        wire.got(2, blk(TWIN), g.pair)
        send(5, TWIN, "right")
        send(6, TWIN, "left")
        seen(TWIN)

    def across():
        wire.got(3, half(FAR, 0), g.left)
        wire.got(4, half(FAR, 1), g.right)
        send(7, FAR, "pair")
        seen(FAR)

    def last():
        wire.got(5, blk(TWIN_LEFT), g.left)
        wire.got(6, blk(TWIN_RIGHT), g.right)
        seen(TWIN_LEFT)
        seen(TWIN_RIGHT)
        wire.got(7, blk(TWIN_FAR), g.pair)
        seen(TWIN_FAR)

    return [start, ring, twin, across, last]


SEEN = [OWN, LEFT, RIGHT, TWIN, FAR, TWIN_LEFT, TWIN_RIGHT, TWIN_FAR]


class Scatter:
    def __init__(self, wire, g, blk, half, bufs, finish):
        self.wire, self.g, self.blk, self.half, self.finish = wire, g, blk, half, finish
        whole, part = bufs
        self.rp, self.rr0, self.rr1, self.rf0, self.rf1, self.rf2 = (whole.at[k] for k in range(6))
        rows, cut = whole.shape[1], part.shape[1]
        self.lo, self.hi = pl.ds(0, cut), pl.ds(cut, rows - cut)
        self.rh0, self.rh1 = part.at[0], part.at[1, pl.ds(0, rows - cut)]

    def twins(self):
        self.wire.go(1, self.blk(TWIN_RIGHT), self.rr0, self.g.right)
        self.wire.go(2, self.blk(TWIN_LEFT), self.rr1, self.g.left)

    def opposite(self):
        self.wire.go(0, self.blk(TWIN_FAR), self.rp, self.g.pair)

    def early(self):
        self.wire.go(3, self.half(RIGHT, 1), self.rf0.at[self.hi], self.g.right)
        self.wire.go(4, self.half(LEFT, 0), self.rf1.at[self.lo], self.g.left)

    def across(self):
        self.wire.got(0, self.rp, self.g.pair)
        for h, sl in ((0, self.lo), (1, self.hi)):
            v = self.half(FAR, h)
            v[...] += self.rp[sl]
        self.wire.go(5, self.half(FAR, 0), self.rh0, self.g.right)
        self.wire.go(6, self.half(FAR, 1), self.rh1, self.g.left)

    def twin(self):
        self.wire.got(1, self.rr0, self.g.left)
        self.wire.got(2, self.rr1, self.g.right)
        v = self.blk(TWIN)
        v[...] += self.rr0[...] + self.rr1[...]
        self.wire.go(7, v, self.rf2, self.g.pair)

    def ring(self):
        self.wire.got(5, self.rh0, self.g.left)
        v = self.half(RIGHT, 0)
        v[...] += self.rh0[...]
        self.wire.go(8, v, self.rf0.at[self.lo], self.g.right)
        self.wire.got(6, self.rh1, self.g.right)
        v = self.half(LEFT, 1)
        v[...] += self.rh1[...]
        self.wire.go(9, v, self.rf1.at[self.hi], self.g.left)

    def last(self):
        self.wire.got(3, self.rf0.at[self.hi], self.g.left)
        self.wire.got(4, self.rf1.at[self.lo], self.g.right)
        self.wire.got(7, self.rf2, self.g.pair)
        self.wire.got(8, self.rf0.at[self.lo], self.g.left)
        self.wire.got(9, self.rf1.at[self.hi], self.g.right)
        self.finish(self.rf0, self.rf1, self.rf2)

    def stages(self):
        def start():
            self.opposite()
            self.twins()
            self.early()

        return [start, self.across, self.twin, self.ring, self.last]


def run_both(a, b):
    for fa, fb in zip(a, b):
        fa()
        fb()


PLACE = {key: k for k, key in enumerate((OWN, TWIN, RIGHT, LEFT, TWIN_FAR, FAR, TWIN_RIGHT, TWIN_LEFT))}


def rows_of(ref, size, base=0):
    def at(key):
        return base + PLACE[key] * size

    def blk(key):
        return ref.at[pl.ds(at(key), size)]

    def half(key, h):
        return ref.at[pl.ds(at(key) + h * (size // 2), size // 2)]

    return blk, half


def score_terms(sim, scale, bias, diag):
    z = scale * sim + bias
    if diag is not None:
        z = jnp.where(diag, -z, z)
    e = jnp.exp(-jnp.abs(z))
    r = 1.0 / (1.0 + e)
    g = jnp.where(z >= 0.0, r, e * r)
    loss = jnp.maximum(z, 0.0) + jnp.log1p(e)
    if diag is not None:
        g = jnp.where(diag, -g, g)
    return loss, g


def fold(x):
    x = jnp.sum(x.reshape(x.shape[0] // 8, 8, x.shape[1]), axis=0)
    return sum(x[:, k * 128 : (k + 1) * 128] for k in range(x.shape[1] // 128))


def tile_of(m):
    div, least = (lambda a, b: a // b, min) if isinstance(m, int) else (lax.div, jnp.minimum)
    q = 3 - least(div(m, 7), 1) - least(div(m, 12), 1) - div(m, 15)
    r = m - (16 - (q + 1) * (q + 1))
    down = least(div(r, q + 1), 1)
    return q + down * (r - q - 1 - q), r + down * (q - r)


def main_kernel(
    block, scal, img_own, txt_own, img_x, txt_x, d_img_out, d_txt_out, sums, x_got,
    img, txt, d_img, d_txt, give, taken, sbuf, gbuf,
    ibuf, ihalf, tbuf, thalf,
    ig_s, ig_r, tg_s, tg_r, is_s, is_r, ts_s, ts_r, core_s, core_r, hand_s, hand_r, local, free,
):
    place = Place()
    gi, gt = place.image_group(), place.text_group()
    c = place.c
    partner = place.partner()
    greet(place)

    half_rows = 8 * block
    img_blk, img_half = rows_of(img, block)
    txt_blk, txt_half = rows_of(txt, block, half_rows)
    other_blk, _ = rows_of(txt, block)
    wi, wt, core = Wire(ig_s, ig_r), Wire(tg_s, tg_r), Wire(core_s, core_r)

    own_i = pltpu.make_async_copy(img_own, img_blk(OWN), local.at[0])
    own_t = pltpu.make_async_copy(txt_own, txt_blk(OWN), local.at[1])
    own_i.start()
    own_t.start()
    own_i.wait()
    own_t.wait()
    sent = iter(range(8))

    def share(key):
        core.go(next(sent), txt_blk(key), other_blk(key), partner)

    a = gather_stages(wi, gi, img_blk(OWN), img_blk, img_half, True)
    b = gather_stages(wt, gt, txt_blk(OWN), txt_blk, txt_half, True, share)
    a[0]()
    b[0]()
    share(OWN)
    img_f, txt_f = img_x.shape[1] // 2, txt_x.shape[1] // 2
    core.go(8, img_x.at[:, pl.ds(pl.multiple_of((1 - c) * img_f, img_f), img_f)], x_got.at[:, pl.ds(0, img_f)], partner)
    core.go(9, txt_x.at[:, pl.ds(pl.multiple_of((1 - c) * txt_f, txt_f), txt_f)], x_got.at[:, pl.ds(img_f, txt_f)], partner)
    for ref in (d_img, d_txt, give, sums):
        ref[...] = jnp.zeros_like(ref)
    run_both(a[1:], b[1:])
    for k, key in enumerate(SEEN):
        core.got(k, other_blk(key), partner)
    core.got(8, x_got.at[:, pl.ds(0, img_f)], partner)
    core.got(9, x_got.at[:, pl.ds(img_f, txt_f)], partner)
    for wire in (wi, wt, core):
        wire.drain()

    scale, bias = scal[0], scal[1]
    di_blk, di_half = rows_of(d_img, block)
    dt_blk, dt_half = rows_of(d_txt, block)

    outs = []

    def finish(out, mine, k):
        def done(p, q, r):
            mine[...] += p[...] + (q[...] + r[...])
            copy = pltpu.make_async_copy(mine, out, local.at[k])
            copy.start()
            outs.append(copy)

        return done

    wi, wt = Wire(is_s, is_r), Wire(ts_s, ts_r)
    ri = Scatter(wi, gi, di_blk, di_half, (ibuf, ihalf), finish(d_img_out, di_blk(OWN), 0))
    rt = Scatter(wt, gt, dt_blk, dt_half, (tbuf, thalf), finish(d_txt_out, dt_blk(OWN), 1))

    def hand(k):
        return pltpu.make_async_remote_copy(
            src_ref=give.at[pl.ds(k * TILE, TILE)], dst_ref=taken.at[k % 2], send_sem=hand_s.at[k], recv_sem=hand_r.at[k], device_id=partner, device_id_type=MESH
        )

    def give_chunk(k):
        if k < 2:
            pl.semaphore_wait(free, 1)
        hand(k).start()

    def take_chunk(k):
        hand(k).wait_recv()
        v = d_txt.at[pl.ds(k * TILE, TILE)]
        v[...] += taken[k % 2]
        if k >= 2:
            pl.semaphore_signal(free, inc=1, device_id=partner, device_id_type=MESH)

    def rows(chunk, first=0):
        at = first + chunk * TILE
        return pl.ds(at if isinstance(at, int) else pl.multiple_of(at, TILE), TILE)

    def txt_rows(cc, chunk):
        return rows(chunk, cc * half_rows)

    def score(m, cc):
        i, j = tile_of(m)
        sbuf[cc] = lax.dot_general(img[rows(i), :], txt[txt_rows(cc, j), :], (((1,), (1,)), ((), ())), preferred_element_type=F32)

    def point(cc, diag=None):
        sim = sbuf[cc]
        loss, g = score_terms(sim, scale, bias, diag)
        sums[0] += fold(loss)
        sums[1] += fold(g * sim)
        sums[2] += fold(g)
        gbuf[cc] = g.astype(BF16)

    def products(m, cc):
        i, j = tile_of(m)
        gb = gbuf[cc]
        d_img[rows(i), :] += jnp.dot(gb, txt[txt_rows(cc, j), :], preferred_element_type=F32)
        ref = d_txt if cc else give
        ref[rows(j), :] += lax.dot_general(gb, img[rows(i), :], (((0,), (0,)), ((), ())), preferred_element_type=F32)

    events = {
        3: [ri.twins],
        6: [lambda: give_chunk(3)],
        7: [lambda: take_chunk(3), rt.twins],
        9: [ri.opposite],
        11: [lambda: give_chunk(2)],
        12: [lambda: take_chunk(2), rt.opposite],
        13: [ri.early],
        14: [lambda: give_chunk(1)],
    }
    score(0, 0)
    score(0, 1)
    point(0)

    def step(m, carry):
        score(m + 1, 0)
        point(1)
        products(m, 0)
        score(m + 1, 1)
        point(0)
        products(m, 1)
        for at, todo in events.items():
            @pl.when(m == at)
            def _(todo=todo):
                for f in todo:
                    f()

        return carry

    lax.fori_loop(0, 15, step, 0)
    row = lax.broadcasted_iota(jnp.int32, (TILE, TILE), 0)
    col = lax.broadcasted_iota(jnp.int32, (TILE, TILE), 1)
    point(1, (row == col) & (row < block))
    products(15, 0)
    give_chunk(0)
    products(15, 1)
    ri.across()
    take_chunk(1)
    rt.early()
    ri.twin()
    take_chunk(0)
    rt.twin()
    rt.across()
    ri.ring()
    rt.ring()
    ri.last()
    rt.last()
    for k in range(4):
        hand(k).wait_send()
    for copy in outs:
        copy.wait()
    wi.drain()
    wt.drain()


def main_call(scal, img_emb, txt_emb, img_x, txt_x):
    block, dim = img_emb.shape
    vmem = pl.BlockSpec(memory_space=pltpu.VMEM)
    hbm = pl.BlockSpec(memory_space=pl.ANY)
    sem = pltpu.SemaphoreType.DMA
    f = lambda *s: pltpu.VMEM(s, F32)
    return pl.pallas_call(
        functools.partial(main_kernel, block),
        in_specs=[pl.BlockSpec(memory_space=pltpu.SMEM), hbm, hbm, hbm, hbm],
        out_specs=[hbm, hbm, vmem, hbm],
        out_shape=[
            jax.ShapeDtypeStruct((block, dim), F32),
            jax.ShapeDtypeStruct((block, dim), F32),
            jax.ShapeDtypeStruct((3, 8, 128), F32),
            jax.ShapeDtypeStruct((block, (img_x.shape[1] + txt_x.shape[1]) // 2), BF16),
        ],
        scratch_shapes=[
            pltpu.VMEM((8 * block, dim), BF16),
            pltpu.VMEM((16 * block, dim), BF16),
            f(8 * block, dim),
            f(8 * block, dim),
            f(8 * block, dim),
            f(2, TILE, dim),
            f(2, TILE, TILE),
            pltpu.VMEM((2, TILE, TILE), BF16),
            f(6, block, dim),
            f(2, block // 2, dim),
            f(6, block, dim),
            f(2, block // 2, dim),
            sem((GATHER_COPIES,)), sem((GATHER_COPIES,)), sem((GATHER_COPIES,)), sem((GATHER_COPIES,)),
            sem((SCATTER_COPIES,)), sem((SCATTER_COPIES,)), sem((SCATTER_COPIES,)), sem((SCATTER_COPIES,)),
            sem((10,)), sem((10,)), sem((4,)), sem((4,)), sem((2,)), pltpu.SemaphoreType.REGULAR,
        ],
        compiler_params=pltpu.CompilerParams(collective_id=0, has_side_effects=True, vmem_limit_bytes=VMEM_LIMIT),
        name="scores",
    )(scal, img_emb, txt_emb, img_x, txt_x)


def pull_back(raw, cot):
    inv = lax.rsqrt(jnp.sum(raw * raw, axis=-1, keepdims=True))
    along = jnp.sum(cot * raw, axis=-1, keepdims=True) * (inv * inv)
    return (inv * (cot - raw * along)).astype(BF16)


COLOURS = 4


def sum_kernel(
    scal, img_x, txt_x, x_got, img_raw, txt_raw, d_img, d_txt, sums_in, d_w_img, d_w_txt, sums,
    w, w2, du_own, du, buf1, half1, buf2, half2, small,
    du_s, du_r, sc_s, sc_r, ga_s, ga_r, out_s, out_r, core_s, core_r, small_s, small_r, local,
):
    place = Place()
    c, partner = place.c, place.partner()
    du_own[0] = pull_back(img_raw[...], scal[2] * d_img[...])
    du_own[1] = pull_back(txt_raw[...], scal[2] * d_txt[...])
    greet(place)
    pre = Wire(du_s, du_r)
    pre.go(0, du_own, du, partner)
    img_f, txt_f = img_x.shape[1] // 2, txt_x.shape[1] // 2
    ni, nt = img_f // 16, txt_f // 16
    rows, wide = ni + nt, w.shape[1] // 2
    tall, lanes, cut = rows // 2, wide // 4, half2.shape[2]

    def outer(lhs, rhs):
        return lax.dot_general(lhs, rhs, (((0,), (0,)), ((), ())), preferred_element_type=F32)

    def put(first, size, shift, val, fresh):
        for b in range(val.shape[0] // size):
            at = (first // size + b) * rows + shift
            piece = val[b * size : (b + 1) * size]
            if fresh:
                w[at : at + size] = piece
            else:
                w[at : at + size] += piece

    def weights(own):
        rhs = du_own if own else du
        lane = 128
        for k in range(0, img_f, lane):
            cols = pl.ds(pl.multiple_of(c * img_f + k, lane), lane)
            put(k, ni, 0, outer(img_x[:, cols] if own else x_got[:, k : k + lane], rhs[0]), own)
        for k in range(0, txt_f, lane):
            cols = pl.ds(pl.multiple_of(c * txt_f + k, lane), lane)
            put(k, nt, ni, outer(txt_x[:, cols] if own else x_got[:, img_f + k : img_f + k + lane], rhs[1]), own)

    weights(True)
    pre.got(0, du, partner)
    weights(False)
    pre.drain()

    small_wire = Wire(small_s, small_r)
    hops = []
    for name in "xyz":
        v = getattr(place, name)
        hops += [place.at(**{name: place.near(v)}), place.at(**{name: place.far(v)})]
    hops.append(partner)
    small[0] = sums_in[...]

    def small_step(n):
        if 0 < n <= len(hops):
            k = n - 1
            small_wire.got(k, small.at[2 * k + 1], hops[k])
            small[2 * n] = small[2 * k] + small[2 * k + 1]
        if n < len(hops):
            small_wire.go(n, small.at[2 * n], small.at[2 * n + 1], hops[n])

    dwire = Pieces(core_s, core_r)
    copies = []

    def sl(first, count):
        return pl.ds(pl.multiple_of(first, count), count)

    def rows_at(first, count):
        return pl.ds(pl.multiple_of(first, 8), count)

    def colour(n):
        order = (place.image_group(), place.text_group())
        g1, g2 = order if n % 2 == 0 else order[::-1]
        group = n % 2 * 8
        base = group * rows
        across = pl.ds(n // 2 * wide, wide)
        mine = base + g1.slot(OWN) * rows
        keep = n % 2 * rows

        def w_blk(key):
            return w.at[sl(base + g1.slot(key) * rows, rows), across]

        def w_half(key, h):
            return w.at[sl(base + g1.slot(key) * rows + h * tall, tall), across]

        def strip(ref, first):
            def at(key):
                slot = g2.slot(key)
                return first + lax.div(slot, 4) * tall, sl(n // 2 * wide + lax.rem(slot, 4) * lanes, lanes)

            def blk(key):
                top, cols = at(key)
                return ref.at[rows_at(top, tall), cols]

            def half(key, h):
                top, cols = at(key)
                return ref.at[rows_at(top + h * cut, tall - cut if h else cut), cols]

            return blk, half

        def outs(key, core, h, parts):
            at = group + g1.slot(key)
            a, b = ni // parts, nt // parts
            return (
                d_w_img.at[sl(core * img_f + at * ni + h * a, a), across],
                d_w_txt.at[sl(core * txt_f + at * nt + h * b, b), across],
            )

        def o_blk(key, core=c):
            return outs(key, core, 0, 1)

        def o_half(key, h):
            return outs(key, c, h, 2)

        ws_blk, ws_half = strip(w, mine)
        os_blk, os_half = strip(w2, keep)

        def done1(p, q, r):
            v = w_blk(OWN)
            v[...] += p[...] + q[...] + r[...]

        def done2(p, q, r):
            v = os_blk(OWN)
            v[...] = ws_blk(OWN)[...] + p[...] + q[...] + r[...]

        whole = w2.at[pl.ds(keep, ni), across], w2.at[pl.ds(keep + ni, nt), across]
        turn = iter(range(n * 8, n * 8 + 8))

        def share(key, src=None):
            dwire.go(next(turn), o_blk(key) if src is None else src, o_blk(key), partner)

        def share_own():
            share(OWN, whole)
            for p, (src, dst) in enumerate(zip(whole, o_blk(OWN))):
                copy = pltpu.make_async_copy(src, dst, local.at[2 * n + p])
                copy.start()
                copies.append(copy)

        def got_shares():
            for k, key in enumerate(SEEN):
                dwire.got(n * 8 + k, o_blk(key, 1 - c), partner)

        w1, w2_, w3 = (Wire(*args) for args in ((sc_s, sc_r, n * SCATTER_COPIES), (sc_s, sc_r, (COLOURS + n) * SCATTER_COPIES), (ga_s, ga_r, n * GATHER_COPIES)))
        w4 = Pieces(out_s, out_r, 2 * n * GATHER_COPIES)
        stages = Scatter(w1, g1, w_blk, w_half, (buf1.at[n], half1.at[n]), done1).stages()
        stages += Scatter(w2_, g2, ws_blk, ws_half, (buf2.at[n], half2.at[n]), done2).stages()
        stages += gather_stages(w3, g2, os_blk(OWN), os_blk, os_half, False)
        tail = gather_stages(w4, g1, whole, o_blk, o_half, False, share)
        stages += [tail[0], share_own] + tail[1:] + [got_shares]
        return stages, [w1, w2_, w3, w4]

    colours = [colour(n) for n in range(COLOURS)]
    for n in range(len(colours[0][0]) + 1):
        for k, (stages, _) in enumerate(colours):
            at = n - k // 2
            if 0 <= at < len(stages):
                stages[at]()
        small_step(n)
    sums[...] = small[2 * len(hops)]
    for copy in copies:
        copy.wait()
    for _, wires in colours:
        for wire in wires:
            wire.drain()
    dwire.drain()
    small_wire.drain()


def sum_call(scal, img_x, txt_x, x_got, img_raw, txt_raw, d_img, d_txt, sums):
    block, feats = x_got.shape
    dim = d_img.shape[1]
    vmem = pl.BlockSpec(memory_space=pltpu.VMEM)
    hbm = pl.BlockSpec(memory_space=pl.ANY)
    sem = lambda n: [pltpu.SemaphoreType.DMA((n,))] * 2
    f = lambda *s: pltpu.VMEM(s, F32)
    rows, wide = feats // 16, dim // 2
    tall, lanes, cut = rows // 2, wide // 4, 24
    return pl.pallas_call(
        sum_kernel,
        in_specs=[pl.BlockSpec(memory_space=pltpu.SMEM)] + [vmem] * 8,
        out_specs=[hbm, hbm, vmem],
        out_shape=[
            jax.ShapeDtypeStruct((img_x.shape[1], dim), F32),
            jax.ShapeDtypeStruct((txt_x.shape[1], dim), F32),
            jax.ShapeDtypeStruct(sums.shape, F32),
        ],
        scratch_shapes=[
            f(feats, dim),
            f(2 * rows, dim),
            pltpu.VMEM((2, block, dim), BF16),
            pltpu.VMEM((2, block, dim), BF16),
            f(COLOURS, 6, rows, wide), f(COLOURS, 2, tall, wide),
            f(COLOURS, 6, tall, lanes), f(COLOURS, 2, cut, lanes),
            f(15, *sums.shape),
            *sem(1), *sem(2 * COLOURS * SCATTER_COPIES), *sem(COLOURS * GATHER_COPIES), *sem(2 * COLOURS * GATHER_COPIES),
            *sem(2 * COLOURS * 8), *sem(7), pltpu.SemaphoreType.DMA((2 * COLOURS,)),
        ],
        compiler_params=pltpu.CompilerParams(collective_id=1, has_side_effects=True, vmem_limit_bytes=32 * 2**20),
        name="weights",
    )(scal, img_x, txt_x, x_got, img_raw, txt_raw, d_img, d_txt, sums)


def store_kernel(total_rows, scal, sums, src_a, src_b, loss, d_temp, d_bias, dst_a, dst_b, sems):
    copies = [pltpu.make_async_copy(src_a, dst_a, sems.at[0]), pltpu.make_async_copy(src_b, dst_b, sems.at[1])]
    for copy in copies:
        copy.start()
    loss[0] = jnp.sum(sums[0]) / total_rows
    d_temp[0] = scal[0] * (jnp.sum(sums[1]) / total_rows)
    d_bias[0] = jnp.sum(sums[2]) / total_rows
    for copy in copies:
        copy.wait()


def store_call(total_rows, scal, sums, *arrays):
    hbm = pl.BlockSpec(memory_space=pl.ANY)
    smem = pl.BlockSpec(memory_space=pltpu.SMEM)
    one = jax.ShapeDtypeStruct((1,), F32)
    return pl.pallas_call(
        functools.partial(store_kernel, total_rows),
        in_specs=[smem, pl.BlockSpec(memory_space=pltpu.VMEM), hbm, hbm],
        out_specs=[smem] * 3 + [pl.BlockSpec(memory_space=pltpu.HBM)] * 2,
        out_shape=[one] * 3 + [jax.ShapeDtypeStruct(a.shape, a.dtype) for a in arrays],
        scratch_shapes=[pltpu.SemaphoreType.DMA((2,))],
        compiler_params=pltpu.CompilerParams(vmem_limit_bytes=2**20),
        name="store",
    )(scal, sums, *arrays)


def solution(mesh):
    dev_count = mesh.shape["replica"] * mesh.shape["data"]
    batch_axes = ("replica", "data")

    def local_fn(img_x, txt_x, w_img, w_txt, log_temp, logit_bias):
        block = img_x.shape[0]
        total_rows = block * dev_count
        txt_raw, txt_emb = embed_rows(txt_x, w_txt)
        img_raw, img_emb = embed_rows(img_x, w_img)
        temp_scale = jnp.exp(log_temp[0])
        scal = jnp.stack([temp_scale, logit_bias[0], temp_scale / total_rows])
        d_img, d_txt, sums, x_got = main_call(scal, img_emb, txt_emb, img_x, txt_x)
        d_w_img, d_w_txt, sums = sum_call(scal, img_x, txt_x, x_got, img_raw, txt_raw, d_img, d_txt, sums)
        return tuple(store_call(total_rows, scal, sums, d_w_img, d_w_txt))

    batch_spec = P(batch_axes, None)
    return jax.shard_map(local_fn, mesh=mesh, in_specs=(batch_spec, batch_spec, P(), P(), P(), P()), out_specs=(P(), P(), P(), P(), P()), check_vma=False)
```

```python
import functools

import jax
import jax.numpy as jnp
from jax import lax
from jax.experimental import pallas as pl
from jax.experimental.pallas import tpu as pltpu
from jax.sharding import PartitionSpec as P

F32 = jnp.float32
BF16 = jnp.bfloat16
TILE = 512
MESH = pl.DeviceIdType.MESH
VMEM_LIMIT = 67043328


def embed_rows(feat_x, w_proj):
    raw = jnp.dot(feat_x, w_proj, preferred_element_type=F32)
    return raw, (raw * lax.rsqrt(jnp.sum(raw * raw, axis=-1, keepdims=True))).astype(BF16)


class Place:
    def __init__(self):
        rep, dat = lax.axis_index("replica"), lax.axis_index("data")
        self.z, self.y = lax.div(rep, 4), lax.rem(rep, 4)
        self.x, self.c = lax.div(dat, 2), lax.rem(dat, 2)

    def at(self, x=None, y=None, z=None, c=None):
        x = self.x if x is None else lax.rem(x + 8, 4)
        y = self.y if y is None else lax.rem(y + 8, 4)
        z = self.z if z is None else lax.rem(z + 8, 4)
        c = self.c if c is None else c
        return (z * 4 + y, x * 2 + c)

    def partner(self):
        return self.at(c=1 - self.c)

    def near(self, v):
        return v + 1 - 2 * lax.rem(v, 2)

    def far(self, v):
        return v - 1 + 2 * lax.rem(v, 2)

    def image_group(self):
        return Group(self.x, lax.rem(lax.div(self.y + 1, 2), 2), self.at(x=self.x + 1), self.at(x=self.x - 1), self.at(y=self.near(self.y)))

    def text_group(self):
        return Group(self.z, lax.div(self.y, 2), self.at(z=self.z + 1), self.at(z=self.z - 1), self.at(y=self.far(self.y)))

    def peers(self):
        out = [self.partner()]
        for g in (self.image_group(), self.text_group()):
            out += [g.right, g.left, g.pair]
        return out


class Group:
    def __init__(self, pos, side, right, left, pair):
        self.pos, self.side, self.right, self.left, self.pair = pos, side, right, left, pair

    def slot(self, key):
        side = 1 - self.side if key[0] else self.side
        return side * 4 + lax.rem(self.pos + key[1] + 4, 4)


def greet(place):
    barrier = pltpu.get_barrier_semaphore()
    peers = place.peers()
    for dev in peers:
        pl.semaphore_signal(barrier, inc=1, device_id=dev, device_id_type=MESH)
    pl.semaphore_wait(barrier, len(peers))


class Wire:
    def __init__(self, send, recv, first=0):
        self.send, self.recv, self.first, self.open = send, recv, first, []

    def copy(self, k, src, dst, dev):
        k += self.first
        return pltpu.make_async_remote_copy(src_ref=src, dst_ref=dst, send_sem=self.send.at[k], recv_sem=self.recv.at[k], device_id=dev, device_id_type=MESH)

    def go(self, *what):
        self.copy(*what).start()
        self.open.append(what)

    def got(self, k, dst, dev):
        self.copy(k, dst, dst, dev).wait_recv()

    def drain(self):
        for what in self.open:
            self.copy(*what).wait_send()
        self.open = []


class Pieces:
    def __init__(self, *where):
        self.wire = Wire(*where)

    def go(self, k, src, dst, dev):
        for p in range(2):
            self.wire.go(2 * k + p, src[p], dst[p], dev)

    def got(self, k, dst, dev):
        for p in range(2):
            self.wire.got(2 * k + p, dst[p], dev)

    def drain(self):
        self.wire.drain()


GATHER_COPIES = 8
SCATTER_COPIES = 10
OWN, RIGHT, LEFT, FAR = ((0, step) for step in (0, 1, -1, 2))
TWIN, TWIN_RIGHT, TWIN_LEFT, TWIN_FAR = ((1, step) for step in (0, 1, -1, 2))


def gather_stages(wire, g, own, blk, half, relative, seen=None):
    seen = seen or (lambda key: None)

    def moved(key, way):
        twin, step = key
        if not relative:
            return key
        twin, step = {"right": (twin, step - 1), "left": (twin, step + 1), "pair": (1 - twin, step)}[way]
        return twin, (step + 1) % 4 - 1

    def send(k, key, way, h=None):
        dev = getattr(g, way)
        view = blk if h is None else functools.partial(half, h=h)
        wire.go(k, view(key), view(moved(key, way)), dev)

    def start():
        for k, way in enumerate(("right", "left", "pair")):
            wire.go(k, own, blk(moved(OWN, way)), getattr(g, way))

    def ring():
        wire.got(0, blk(LEFT), g.left)
        send(3, LEFT, "right", 0)
        wire.got(1, blk(RIGHT), g.right)
        send(4, RIGHT, "left", 1)
        seen(LEFT)
        seen(RIGHT)

    def twin():
        wire.got(2, blk(TWIN), g.pair)
        send(5, TWIN, "right")
        send(6, TWIN, "left")
        seen(TWIN)

    def across():
        wire.got(3, half(FAR, 0), g.left)
        wire.got(4, half(FAR, 1), g.right)
        send(7, FAR, "pair")
        seen(FAR)

    def last():
        wire.got(5, blk(TWIN_LEFT), g.left)
        wire.got(6, blk(TWIN_RIGHT), g.right)
        seen(TWIN_LEFT)
        seen(TWIN_RIGHT)
        wire.got(7, blk(TWIN_FAR), g.pair)
        seen(TWIN_FAR)

    return [start, ring, twin, across, last]


SEEN = [OWN, LEFT, RIGHT, TWIN, FAR, TWIN_LEFT, TWIN_RIGHT, TWIN_FAR]


class Scatter:
    def __init__(self, wire, g, blk, half, bufs, finish):
        self.wire, self.g, self.blk, self.half, self.finish = wire, g, blk, half, finish
        whole, part = bufs
        self.rp, self.rr0, self.rr1, self.rf0, self.rf1, self.rf2 = (whole.at[k] for k in range(6))
        rows, cut = whole.shape[1], part.shape[1]
        self.lo, self.hi = pl.ds(0, cut), pl.ds(cut, rows - cut)
        self.rh0, self.rh1 = part.at[0], part.at[1, pl.ds(0, rows - cut)]

    def twins(self):
        self.wire.go(1, self.blk(TWIN_RIGHT), self.rr0, self.g.right)
        self.wire.go(2, self.blk(TWIN_LEFT), self.rr1, self.g.left)

    def opposite(self):
        self.wire.go(0, self.blk(TWIN_FAR), self.rp, self.g.pair)

    def early(self):
        self.wire.go(3, self.half(RIGHT, 1), self.rf0.at[self.hi], self.g.right)
        self.wire.go(4, self.half(LEFT, 0), self.rf1.at[self.lo], self.g.left)

    def across(self):
        self.wire.got(0, self.rp, self.g.pair)
        for h, sl in ((0, self.lo), (1, self.hi)):
            v = self.half(FAR, h)
            v[...] += self.rp[sl]
        self.wire.go(5, self.half(FAR, 0), self.rh0, self.g.right)
        self.wire.go(6, self.half(FAR, 1), self.rh1, self.g.left)

    def twin(self):
        self.wire.got(1, self.rr0, self.g.left)
        self.wire.got(2, self.rr1, self.g.right)
        v = self.blk(TWIN)
        v[...] += self.rr0[...] + self.rr1[...]
        self.wire.go(7, v, self.rf2, self.g.pair)

    def ring(self):
        self.wire.got(5, self.rh0, self.g.left)
        v = self.half(RIGHT, 0)
        v[...] += self.rh0[...]
        self.wire.go(8, v, self.rf0.at[self.lo], self.g.right)
        self.wire.got(6, self.rh1, self.g.right)
        v = self.half(LEFT, 1)
        v[...] += self.rh1[...]
        self.wire.go(9, v, self.rf1.at[self.hi], self.g.left)

    def last(self):
        self.wire.got(3, self.rf0.at[self.hi], self.g.left)
        self.wire.got(4, self.rf1.at[self.lo], self.g.right)
        self.wire.got(7, self.rf2, self.g.pair)
        self.wire.got(8, self.rf0.at[self.lo], self.g.left)
        self.wire.got(9, self.rf1.at[self.hi], self.g.right)
        self.finish(self.rf0, self.rf1, self.rf2)

    def stages(self):
        def start():
            self.opposite()
            self.twins()
            self.early()

        return [start, self.across, self.twin, self.ring, self.last]


def run_both(a, b):
    for fa, fb in zip(a, b):
        fa()
        fb()


PLACE = {key: k for k, key in enumerate((OWN, TWIN, RIGHT, LEFT, TWIN_FAR, FAR, TWIN_RIGHT, TWIN_LEFT))}


def rows_of(ref, size, base=0):
    def at(key):
        return base + PLACE[key] * size

    def blk(key):
        return ref.at[pl.ds(at(key), size)]

    def half(key, h):
        return ref.at[pl.ds(at(key) + h * (size // 2), size // 2)]

    return blk, half


def score_terms(sim, scale, bias, diag):
    z = scale * sim + bias
    if diag is not None:
        z = jnp.where(diag, -z, z)
    e = jnp.exp(-jnp.abs(z))
    r = 1.0 / (1.0 + e)
    g = jnp.where(z >= 0.0, r, e * r)
    loss = jnp.maximum(z, 0.0) + jnp.log1p(e)
    if diag is not None:
        g = jnp.where(diag, -g, g)
    return loss, g


def fold(x):
    x = jnp.sum(x.reshape(x.shape[0] // 8, 8, x.shape[1]), axis=0)
    return sum(x[:, k * 128 : (k + 1) * 128] for k in range(x.shape[1] // 128))


def tile_of(m):
    div, least = (lambda a, b: a // b, min) if isinstance(m, int) else (lax.div, jnp.minimum)
    q = 3 - least(div(m, 7), 1) - least(div(m, 12), 1) - div(m, 15)
    r = m - (16 - (q + 1) * (q + 1))
    down = least(div(r, q + 1), 1)
    return r + down * (q - r), q + down * (r - q - 1 - q)


def main_kernel(
    block, scal, img_own, txt_own, img_x, txt_x, img_raw, txt_raw, sums, pack,
    img, txt, d_img, d_txt, give, taken, sbuf, gbuf,
    ibuf, ihalf, tbuf, thalf,
    ig_s, ig_r, tg_s, tg_r, is_s, is_r, ts_s, ts_r, core_s, core_r, hand_s, hand_r, local, free,
):
    place = Place()
    gi, gt = place.image_group(), place.text_group()
    c = place.c
    partner = place.partner()
    greet(place)

    half_rows = 8 * block
    img_blk, img_half = rows_of(img, block)
    txt_blk, txt_half = rows_of(txt, block, half_rows)
    other_blk, _ = rows_of(txt, block)
    wi, wt, core = Wire(ig_s, ig_r), Wire(tg_s, tg_r), Wire(core_s, core_r)

    own_i = pltpu.make_async_copy(img_own, img_blk(OWN), local.at[0])
    own_t = pltpu.make_async_copy(txt_own, txt_blk(OWN), local.at[1])
    own_i.start()
    own_t.start()
    own_i.wait()
    own_t.wait()
    sent = iter(range(8))

    def share(key):
        core.go(next(sent), txt_blk(key), other_blk(key), partner)

    a = gather_stages(wi, gi, img_blk(OWN), img_blk, img_half, True)
    b = gather_stages(wt, gt, txt_blk(OWN), txt_blk, txt_half, True, share)
    a[0]()
    b[0]()
    share(OWN)
    img_f, txt_f = img_x.shape[1] // 2, txt_x.shape[1] // 2
    feats = img_f + txt_f

    def half_of(which, count):
        return pl.ds(pl.multiple_of(which * count, count), count)

    core.go(8, img_x.at[:, half_of(1 - c, img_f)], pack.at[:, pl.ds(feats, img_f)], partner)
    core.go(9, txt_x.at[:, half_of(1 - c, txt_f)], pack.at[:, pl.ds(feats + img_f, txt_f)], partner)
    for ref in (d_img, d_txt, give, sums):
        ref[...] = jnp.zeros_like(ref)
    run_both(a[1:], b[1:])
    for k, key in enumerate(SEEN):
        core.got(k, other_blk(key), partner)
    wi.drain()
    wt.drain()

    scale, bias = scal[0], scal[1]
    di_blk, di_half = rows_of(d_img, block)
    dt_blk, dt_half = rows_of(d_txt, block)

    outs = []

    def put(src, first, count, k):
        copy = pltpu.make_async_copy(src, pack.at[:, pl.ds(first, count)], local.at[4 + k])
        copy.start()
        outs.append(copy)

    def du_view(which, k):
        return pack.at[:, pl.ds(2 * feats + (2 * which + k) * img.shape[1], img.shape[1])]

    def finish(mine, raw, k):
        first = k * block
        step = 64

        def done(p, q, r):
            def rows_of_du(n, carry):
                at = pl.ds(pl.multiple_of(n * step, step), step)
                total = mine[at, :] + p[at, :] + (q[at, :] + r[at, :])
                img[pl.ds(pl.multiple_of(first + n * step, step), step), :] = pull_back(raw[at, :], scal[2] * total)
                return carry

            lax.fori_loop(0, block // step, rows_of_du, 0)
            core.go(10 + k, img.at[pl.ds(first, block)], du_view(1, k), partner)
            put(img.at[pl.ds(first, block)], 2 * feats + k * img.shape[1], img.shape[1], k)

        return done

    wi, wt = Wire(is_s, is_r), Wire(ts_s, ts_r)
    ri = Scatter(wi, gi, di_blk, di_half, (ibuf, ihalf), finish(di_blk(OWN), ibuf.at[0], 0))
    rt = Scatter(wt, gt, dt_blk, dt_half, (tbuf, thalf), finish(dt_blk(OWN), tbuf.at[0], 1))

    def hand(k):
        return pltpu.make_async_remote_copy(
            src_ref=give.at[pl.ds(k * TILE, TILE)], dst_ref=taken.at[k % 2], send_sem=hand_s.at[k], recv_sem=hand_r.at[k], device_id=partner, device_id_type=MESH
        )

    def give_chunk(k):
        if k < 2:
            pl.semaphore_wait(free, 1)
        hand(k).start()

    def take_chunk(k):
        hand(k).wait_recv()
        v = d_txt.at[pl.ds(k * TILE, TILE)]
        v[...] += taken[k % 2]
        if k >= 2:
            pl.semaphore_signal(free, inc=1, device_id=partner, device_id_type=MESH)

    def rows(chunk, first=0):
        at = first + chunk * TILE
        return pl.ds(at if isinstance(at, int) else pl.multiple_of(at, TILE), TILE)

    def txt_rows(cc, chunk):
        return rows(chunk, cc * half_rows)

    def score(m, cc):
        i, j = tile_of(m)
        sbuf[cc] = lax.dot_general(img[rows(i), :], txt[txt_rows(cc, j), :], (((1,), (1,)), ((), ())), preferred_element_type=F32)

    def point(cc, diag=None):
        sim = sbuf[cc]
        loss, g = score_terms(sim, scale, bias, diag)
        sums[0] += fold(loss)
        sums[1] += fold(g * sim)
        sums[2] += fold(g)
        gbuf[cc] = g.astype(BF16)

    def products(m, cc):
        i, j = tile_of(m)
        gb = gbuf[cc]
        d_img[rows(i), :] += jnp.dot(gb, txt[txt_rows(cc, j), :], preferred_element_type=F32)
        ref = d_txt if cc else give
        ref[rows(j), :] += lax.dot_general(gb, img[rows(i), :], (((0,), (0,)), ((), ())), preferred_element_type=F32)

    events = {
        3: [lambda: give_chunk(3)],
        4: [lambda: take_chunk(3), rt.twins],
        6: [ri.twins],
        9: [lambda: give_chunk(2)],
        10: [lambda: take_chunk(2), rt.opposite],
        11: [ri.opposite],
        13: [lambda: give_chunk(1)],
        14: [lambda: take_chunk(1), rt.early, ri.early],
    }
    score(0, 0)
    score(0, 1)
    point(0)

    def step(m, carry):
        score(m + 1, 0)
        point(1)
        products(m, 0)
        score(m + 1, 1)
        point(0)
        products(m, 1)
        for at, todo in events.items():
            @pl.when(m == at)
            def _(todo=todo):
                for f in todo:
                    f()

        return carry

    lax.fori_loop(0, 15, step, 0)
    row = lax.broadcasted_iota(jnp.int32, (TILE, TILE), 0)
    col = lax.broadcasted_iota(jnp.int32, (TILE, TILE), 1)
    point(1, (row == col) & (row < block))
    products(15, 0)
    give_chunk(0)
    products(15, 1)
    rt.across()
    ri.twin()
    ri.across()
    keep = [pltpu.make_async_copy(x.at[:, half_of(c, n)], img.at[pl.ds((2 + k) * block, block), pl.ds(0, n)], local.at[2 + k]) for k, (x, n) in enumerate(((img_x, img_f), (txt_x, txt_f)))]
    keep += [pltpu.make_async_copy(img_raw, ibuf.at[0], local.at[0]), pltpu.make_async_copy(txt_raw, tbuf.at[0], local.at[1])]
    for copy in keep:
        copy.start()
    take_chunk(0)
    rt.twin()
    for copy in keep:
        copy.wait()
    put(img.at[pl.ds(2 * block, block)], 0, img_f, 2)
    put(img.at[pl.ds(3 * block, block), pl.ds(0, txt_f)], img_f, txt_f, 3)
    rt.ring()
    ri.ring()
    rt.last()
    ri.last()
    for k, first in enumerate((feats, feats + img_f)):
        core.got(8 + k, pack.at[:, pl.ds(first, (img_f, txt_f)[k])], partner)
        core.got(10 + k, du_view(1, k), partner)
    for k in range(4):
        hand(k).wait_send()
    for copy in outs:
        copy.wait()
    for wire in (wi, wt, core):
        wire.drain()


def main_call(scal, img_emb, txt_emb, img_x, txt_x, img_raw, txt_raw):
    block, dim = img_emb.shape
    vmem = pl.BlockSpec(memory_space=pltpu.VMEM)
    hbm = pl.BlockSpec(memory_space=pl.ANY)
    sem = pltpu.SemaphoreType.DMA
    f = lambda *s: pltpu.VMEM(s, F32)
    return pl.pallas_call(
        functools.partial(main_kernel, block),
        in_specs=[pl.BlockSpec(memory_space=pltpu.SMEM)] + [hbm] * 6,
        out_specs=[vmem, hbm],
        out_shape=[
            jax.ShapeDtypeStruct((3, 8, 128), F32),
            jax.ShapeDtypeStruct((block, img_x.shape[1] + txt_x.shape[1] + 4 * dim), BF16),
        ],
        scratch_shapes=[
            pltpu.VMEM((8 * block, dim), BF16),
            pltpu.VMEM((16 * block, dim), BF16),
            f(8 * block, dim),
            f(8 * block, dim),
            f(8 * block, dim),
            f(2, TILE, dim),
            f(2, TILE, TILE),
            pltpu.VMEM((2, TILE, TILE), BF16),
            f(6, block, dim),
            f(2, block // 2, dim),
            f(6, block, dim),
            f(2, block // 2, dim),
            sem((GATHER_COPIES,)), sem((GATHER_COPIES,)), sem((GATHER_COPIES,)), sem((GATHER_COPIES,)),
            sem((SCATTER_COPIES,)), sem((SCATTER_COPIES,)), sem((SCATTER_COPIES,)), sem((SCATTER_COPIES,)),
            sem((12,)), sem((12,)), sem((4,)), sem((4,)), sem((8,)), pltpu.SemaphoreType.REGULAR,
        ],
        compiler_params=pltpu.CompilerParams(collective_id=0, has_side_effects=True, vmem_limit_bytes=VMEM_LIMIT),
        name="scores",
    )(scal, img_emb, txt_emb, img_x, txt_x, img_raw, txt_raw)


def pull_back(raw, cot):
    inv = lax.rsqrt(jnp.sum(raw * raw, axis=-1, keepdims=True))
    along = jnp.sum(cot * raw, axis=-1, keepdims=True) * (inv * inv)
    return (inv * (cot - raw * along)).astype(BF16)


COLOURS = 4


def sum_kernel(
    pack, sums_in, d_w_img, d_w_txt, sums,
    w, w2, buf1, half1, buf2, half2, small,
    sc_s, sc_r, ga_s, ga_r, out_s, out_r, core_s, core_r, small_s, small_r, local,
):
    place = Place()
    c, partner = place.c, place.partner()
    greet(place)
    img_f, txt_f, feats = d_w_img.shape[0] // 2, d_w_txt.shape[0] // 2, w.shape[0]
    ni, nt = img_f // 16, txt_f // 16
    rows, wide = ni + nt, w.shape[1] // 2
    tall, lanes, cut = rows // 2, wide // 4, half2.shape[2]

    def outer(lhs, rhs):
        return lax.dot_general(lhs, rhs, (((0,), (0,)), ((), ())), preferred_element_type=F32)

    def weights(first, count, size, shift, k):
        lane, dim = 128, w.shape[1]
        for at in range(0, count, lane):
            val = sum(
                outer(pack[:, side * feats + first + at : side * feats + first + at + lane], pack[:, 2 * feats + (2 * side + k) * dim : 2 * feats + (2 * side + k + 1) * dim])
                for side in range(2)
            )
            for b in range(lane // size):
                to = (at // size + b) * rows + shift
                w[to : to + size] = val[b * size : (b + 1) * size]

    weights(0, img_f, ni, 0, 0)
    weights(img_f, txt_f, nt, ni, 1)

    small_wire = Wire(small_s, small_r)
    hops = []
    for name in "xyz":
        v = getattr(place, name)
        hops += [place.at(**{name: place.near(v)}), place.at(**{name: place.far(v)})]
    hops.append(partner)
    small[0] = sums_in[...]

    def small_step(n):
        if 0 < n <= len(hops):
            k = n - 1
            small_wire.got(k, small.at[2 * k + 1], hops[k])
            small[2 * n] = small[2 * k] + small[2 * k + 1]
        if n < len(hops):
            small_wire.go(n, small.at[2 * n], small.at[2 * n + 1], hops[n])

    dwire = Pieces(core_s, core_r)
    copies = []

    def sl(first, count):
        return pl.ds(pl.multiple_of(first, count), count)

    def rows_at(first, count):
        return pl.ds(pl.multiple_of(first, 8), count)

    def colour(n):
        order = (place.image_group(), place.text_group())
        g1, g2 = order if n % 2 == 0 else order[::-1]
        group = n % 2 * 8
        base = group * rows
        across = pl.ds(n // 2 * wide, wide)
        mine = base + g1.slot(OWN) * rows
        keep = n % 2 * rows

        def w_blk(key):
            return w.at[sl(base + g1.slot(key) * rows, rows), across]

        def w_half(key, h):
            return w.at[sl(base + g1.slot(key) * rows + h * tall, tall), across]

        def strip(ref, first):
            def at(key):
                slot = g2.slot(key)
                return first + lax.div(slot, 4) * tall, sl(n // 2 * wide + lax.rem(slot, 4) * lanes, lanes)

            def blk(key):
                top, cols = at(key)
                return ref.at[rows_at(top, tall), cols]

            def half(key, h):
                top, cols = at(key)
                return ref.at[rows_at(top + h * cut, tall - cut if h else cut), cols]

            return blk, half

        def outs(key, core, h, parts):
            at = group + g1.slot(key)
            a, b = ni // parts, nt // parts
            return (
                d_w_img.at[sl(core * img_f + at * ni + h * a, a), across],
                d_w_txt.at[sl(core * txt_f + at * nt + h * b, b), across],
            )

        def o_blk(key, core=c):
            return outs(key, core, 0, 1)

        def o_half(key, h):
            return outs(key, c, h, 2)

        ws_blk, ws_half = strip(w, mine)
        os_blk, os_half = strip(w2, keep)

        def done1(p, q, r):
            v = w_blk(OWN)
            v[...] += p[...] + q[...] + r[...]

        def done2(p, q, r):
            v = os_blk(OWN)
            v[...] = ws_blk(OWN)[...] + p[...] + q[...] + r[...]

        whole = w2.at[pl.ds(keep, ni), across], w2.at[pl.ds(keep + ni, nt), across]
        turn = iter(range(n * 8, n * 8 + 8))

        def share(key, src=None):
            dwire.go(next(turn), o_blk(key) if src is None else src, o_blk(key), partner)

        def share_own():
            share(OWN, whole)
            for p, (src, dst) in enumerate(zip(whole, o_blk(OWN))):
                copy = pltpu.make_async_copy(src, dst, local.at[2 * n + p])
                copy.start()
                copies.append(copy)

        def got_shares():
            for k, key in enumerate(SEEN):
                dwire.got(n * 8 + k, o_blk(key, 1 - c), partner)

        w1, w2_, w3 = (Wire(*args) for args in ((sc_s, sc_r, n * SCATTER_COPIES), (sc_s, sc_r, (COLOURS + n) * SCATTER_COPIES), (ga_s, ga_r, n * GATHER_COPIES)))
        w4 = Pieces(out_s, out_r, 2 * n * GATHER_COPIES)
        stages = Scatter(w1, g1, w_blk, w_half, (buf1.at[n], half1.at[n]), done1).stages()
        stages += Scatter(w2_, g2, ws_blk, ws_half, (buf2.at[n], half2.at[n]), done2).stages()
        stages += gather_stages(w3, g2, os_blk(OWN), os_blk, os_half, False)
        tail = gather_stages(w4, g1, whole, o_blk, o_half, False, share)
        stages += [tail[0], share_own] + tail[1:] + [got_shares]
        return stages, [w1, w2_, w3, w4]

    colours = [colour(n) for n in range(COLOURS)]
    for n in range(len(colours[0][0]) + 1):
        for k, (stages, _) in enumerate(colours):
            at = n - k // 2
            if 0 <= at < len(stages):
                stages[at]()
        small_step(n)
    sums[...] = small[2 * len(hops)]
    for copy in copies:
        copy.wait()
    for _, wires in colours:
        for wire in wires:
            wire.drain()
    dwire.drain()
    small_wire.drain()


def sum_call(pack, sums, img_x, txt_x, dim):
    feats = (img_x.shape[1] + txt_x.shape[1]) // 2
    vmem = pl.BlockSpec(memory_space=pltpu.VMEM)
    hbm = pl.BlockSpec(memory_space=pl.ANY)
    sem = lambda n: [pltpu.SemaphoreType.DMA((n,))] * 2
    f = lambda *s: pltpu.VMEM(s, F32)
    rows, wide = feats // 16, dim // 2
    tall, lanes, cut = rows // 2, wide // 4, 24
    return pl.pallas_call(
        sum_kernel,
        in_specs=[vmem, vmem],
        out_specs=[hbm, hbm, vmem],
        out_shape=[
            jax.ShapeDtypeStruct((img_x.shape[1], dim), F32),
            jax.ShapeDtypeStruct((txt_x.shape[1], dim), F32),
            jax.ShapeDtypeStruct(sums.shape, F32),
        ],
        scratch_shapes=[
            f(feats, dim),
            f(2 * rows, dim),
            f(COLOURS, 6, rows, wide), f(COLOURS, 2, tall, wide),
            f(COLOURS, 6, tall, lanes), f(COLOURS, 2, cut, lanes),
            f(15, *sums.shape),
            *sem(2 * COLOURS * SCATTER_COPIES), *sem(COLOURS * GATHER_COPIES), *sem(2 * COLOURS * GATHER_COPIES),
            *sem(2 * COLOURS * 8), *sem(7), pltpu.SemaphoreType.DMA((2 * COLOURS,)),
        ],
        compiler_params=pltpu.CompilerParams(collective_id=1, has_side_effects=True, vmem_limit_bytes=32 * 2**20),
        name="weights",
    )(pack, sums)


def store_kernel(total_rows, scal, sums, src_a, src_b, loss, d_temp, d_bias, dst_a, dst_b, sems):
    copies = [pltpu.make_async_copy(src_a, dst_a, sems.at[0]), pltpu.make_async_copy(src_b, dst_b, sems.at[1])]
    for copy in copies:
        copy.start()
    loss[0] = jnp.sum(sums[0]) / total_rows
    d_temp[0] = scal[0] * (jnp.sum(sums[1]) / total_rows)
    d_bias[0] = jnp.sum(sums[2]) / total_rows
    for copy in copies:
        copy.wait()


def store_call(total_rows, scal, sums, *arrays):
    hbm = pl.BlockSpec(memory_space=pl.ANY)
    smem = pl.BlockSpec(memory_space=pltpu.SMEM)
    one = jax.ShapeDtypeStruct((1,), F32)
    return pl.pallas_call(
        functools.partial(store_kernel, total_rows),
        in_specs=[smem, pl.BlockSpec(memory_space=pltpu.VMEM), hbm, hbm],
        out_specs=[smem] * 3 + [pl.BlockSpec(memory_space=pltpu.HBM)] * 2,
        out_shape=[one] * 3 + [jax.ShapeDtypeStruct(a.shape, a.dtype) for a in arrays],
        scratch_shapes=[pltpu.SemaphoreType.DMA((2,))],
        compiler_params=pltpu.CompilerParams(vmem_limit_bytes=2**20),
        name="store",
    )(scal, sums, *arrays)


def solution(mesh):
    dev_count = mesh.shape["replica"] * mesh.shape["data"]
    batch_axes = ("replica", "data")

    def local_fn(img_x, txt_x, w_img, w_txt, log_temp, logit_bias):
        block = img_x.shape[0]
        total_rows = block * dev_count
        txt_raw, txt_emb = embed_rows(txt_x, w_txt)
        img_raw, img_emb = embed_rows(img_x, w_img)
        temp_scale = jnp.exp(log_temp[0])
        scal = jnp.stack([temp_scale, logit_bias[0], temp_scale / total_rows])
        sums, pack = main_call(scal, img_emb, txt_emb, img_x, txt_x, img_raw, txt_raw)
        d_w_img, d_w_txt, sums = sum_call(pack, sums, img_x, txt_x, w_img.shape[1])
        return tuple(store_call(total_rows, scal, sums, d_w_img, d_w_txt))

    batch_spec = P(batch_axes, None)
    return jax.shard_map(local_fn, mesh=mesh, in_specs=(batch_spec, batch_spec, P(), P(), P(), P()), out_specs=(P(), P(), P(), P(), P()), check_vma=False)
```

```python
import functools

import jax
import jax.numpy as jnp
from jax import lax
from jax.experimental import pallas as pl
from jax.experimental.pallas import tpu as pltpu
from jax.sharding import PartitionSpec as P

F32 = jnp.float32
BF16 = jnp.bfloat16
TILE = 512
MESH = pl.DeviceIdType.MESH
VMEM_LIMIT = 67043328


def embed_rows(feat_x, w_proj):
    raw = jnp.dot(feat_x, w_proj, preferred_element_type=F32)
    return raw, (raw * lax.rsqrt(jnp.sum(raw * raw, axis=-1, keepdims=True))).astype(BF16)


OWN, RIGHT, LEFT, FAR = ((0, step) for step in (0, 1, -1, 2))
TWIN, TWIN_RIGHT, TWIN_LEFT, TWIN_FAR = ((1, step) for step in (0, 1, -1, 2))
SEEN = [OWN, LEFT, RIGHT, TWIN, FAR, TWIN_LEFT, TWIN_RIGHT, TWIN_FAR]


class Place:
    def __init__(self):
        rep, dat = lax.axis_index("replica"), lax.axis_index("data")
        self.z, self.y = lax.div(rep, 4), lax.rem(rep, 4)
        self.x, self.c = lax.div(dat, 2), lax.rem(dat, 2)

    def at(self, x=None, y=None, z=None, c=None):
        x = self.x if x is None else lax.rem(x + 8, 4)
        y = self.y if y is None else lax.rem(y + 8, 4)
        z = self.z if z is None else lax.rem(z + 8, 4)
        c = self.c if c is None else c
        return (z * 4 + y, x * 2 + c)

    def partner(self):
        return self.at(c=1 - self.c)

    def near(self, v):
        return v + 1 - 2 * lax.rem(v, 2)

    def far(self, v):
        return v - 1 + 2 * lax.rem(v, 2)

    def image_group(self):
        return Group(self.x, lax.rem(lax.div(self.y + 1, 2), 2), lambda key: self.at(x=self.x + key[1], y=self.near(self.y) if key[0] else None))

    def text_group(self):
        return Group(self.z, lax.div(self.y, 2), lambda key: self.at(z=self.z + key[1], y=self.far(self.y) if key[0] else None))

    def peers(self, keys):
        return [self.partner()] + [g.dev(key) for g in (self.image_group(), self.text_group()) for key in keys]


class Group:
    def __init__(self, pos, side, dev):
        self.pos, self.side, self.dev = pos, side, dev
        self.right, self.left, self.pair = (dev(key) for key in (RIGHT, LEFT, TWIN))

    def slot(self, key):
        side = 1 - self.side if key[0] else self.side
        return side * 4 + lax.rem(self.pos + key[1] + 4, 4)


def greet(place, keys):
    barrier = pltpu.get_barrier_semaphore()
    peers = place.peers(keys)
    for dev in peers:
        pl.semaphore_signal(barrier, inc=1, device_id=dev, device_id_type=MESH)
    pl.semaphore_wait(barrier, len(peers))


class Wire:
    def __init__(self, send, recv, first=0):
        self.send, self.recv, self.first, self.open = send, recv, first, []

    def copy(self, k, src, dst, dev):
        k += self.first
        return pltpu.make_async_remote_copy(src_ref=src, dst_ref=dst, send_sem=self.send.at[k], recv_sem=self.recv.at[k], device_id=dev, device_id_type=MESH)

    def go(self, *what):
        self.copy(*what).start()
        self.open.append(what)

    def got(self, k, dst, dev):
        self.copy(k, dst, dst, dev).wait_recv()

    def drain(self):
        for what in self.open:
            self.copy(*what).wait_send()
        self.open = []


class Pieces:
    def __init__(self, *where):
        self.wire = Wire(*where)

    def go(self, k, src, dst, dev):
        for p in range(2):
            self.wire.go(2 * k + p, src[p], dst[p], dev)

    def got(self, k, dst, dev):
        for p in range(2):
            self.wire.got(2 * k + p, dst[p], dev)

    def drain(self):
        self.wire.drain()


GATHER_COPIES = 8
SCATTER_COPIES = 10


def gather_stages(wire, g, own, blk, half, relative, seen=None):
    seen = seen or (lambda key: None)

    def moved(key, way):
        twin, step = key
        if not relative:
            return key
        twin, step = {"right": (twin, step - 1), "left": (twin, step + 1), "pair": (1 - twin, step)}[way]
        return twin, (step + 1) % 4 - 1

    def send(k, key, way, h=None):
        dev = getattr(g, way)
        view = blk if h is None else functools.partial(half, h=h)
        wire.go(k, view(key), view(moved(key, way)), dev)

    def start():
        for k, way in enumerate(("right", "left", "pair")):
            wire.go(k, own, blk(moved(OWN, way)), getattr(g, way))

    def ring():
        wire.got(0, blk(LEFT), g.left)
        send(3, LEFT, "right", 0)
        wire.got(1, blk(RIGHT), g.right)
        send(4, RIGHT, "left", 1)
        seen(LEFT)
        seen(RIGHT)

    def twin():
        wire.got(2, blk(TWIN), g.pair)
        send(5, TWIN, "right")
        send(6, TWIN, "left")
        seen(TWIN)

    def across():
        wire.got(3, half(FAR, 0), g.left)
        wire.got(4, half(FAR, 1), g.right)
        send(7, FAR, "pair")
        seen(FAR)

    def last():
        wire.got(5, blk(TWIN_LEFT), g.left)
        wire.got(6, blk(TWIN_RIGHT), g.right)
        seen(TWIN_LEFT)
        seen(TWIN_RIGHT)
        wire.got(7, blk(TWIN_FAR), g.pair)
        seen(TWIN_FAR)

    return [start, ring, twin, across, last]


def direct_stages(wire, g, blk):
    def send():
        for k, key in enumerate(SEEN[1:]):
            wire.go(k, blk(OWN), blk(OWN), g.dev(key))

    def take():
        for k, (twin, step) in enumerate(SEEN[1:]):
            back = (twin, step if step == 2 else -step)
            wire.got(k, blk(back), g.dev(back))

    return [send, take]


def direct_scatter_stages(wire, g, blk, bufs, done):
    def send():
        for k, key in enumerate(SEEN[1:]):
            wire.go(k, blk(key), bufs.at[k], g.dev(key))

    def take():
        for k, (twin, step) in enumerate(SEEN[1:]):
            wire.got(k, bufs.at[k], g.dev((twin, step if step == 2 else -step)))
        done([bufs[k] for k in range(7)])

    return [send, take]


class Scatter:
    def __init__(self, wire, g, blk, half, bufs, finish):
        self.wire, self.g, self.blk, self.half, self.finish = wire, g, blk, half, finish
        whole, part = bufs
        self.rp, self.rr0, self.rr1, self.rf0, self.rf1, self.rf2 = (whole.at[k] for k in range(6))
        rows, cut = whole.shape[1], part.shape[1]
        self.lo, self.hi = pl.ds(0, cut), pl.ds(cut, rows - cut)
        self.rh0, self.rh1 = part.at[0], part.at[1, pl.ds(0, rows - cut)]

    def twins(self):
        self.wire.go(1, self.blk(TWIN_RIGHT), self.rr0, self.g.right)
        self.wire.go(2, self.blk(TWIN_LEFT), self.rr1, self.g.left)

    def opposite(self):
        self.wire.go(0, self.blk(TWIN_FAR), self.rp, self.g.pair)

    def early(self):
        self.wire.go(3, self.half(RIGHT, 1), self.rf0.at[self.hi], self.g.right)
        self.wire.go(4, self.half(LEFT, 0), self.rf1.at[self.lo], self.g.left)

    def across(self):
        self.wire.got(0, self.rp, self.g.pair)
        for h, sl in ((0, self.lo), (1, self.hi)):
            v = self.half(FAR, h)
            v[...] += self.rp[sl]
        self.wire.go(5, self.half(FAR, 0), self.rh0, self.g.right)
        self.wire.go(6, self.half(FAR, 1), self.rh1, self.g.left)

    def twin(self):
        self.wire.got(1, self.rr0, self.g.left)
        self.wire.got(2, self.rr1, self.g.right)
        v = self.blk(TWIN)
        v[...] += self.rr0[...] + self.rr1[...]
        self.wire.go(7, v, self.rf2, self.g.pair)

    def ring(self):
        self.wire.got(5, self.rh0, self.g.left)
        v = self.half(RIGHT, 0)
        v[...] += self.rh0[...]
        self.wire.go(8, v, self.rf0.at[self.lo], self.g.right)
        self.wire.got(6, self.rh1, self.g.right)
        v = self.half(LEFT, 1)
        v[...] += self.rh1[...]
        self.wire.go(9, v, self.rf1.at[self.hi], self.g.left)

    def last(self):
        self.wire.got(3, self.rf0.at[self.hi], self.g.left)
        self.wire.got(4, self.rf1.at[self.lo], self.g.right)
        self.wire.got(7, self.rf2, self.g.pair)
        self.wire.got(8, self.rf0.at[self.lo], self.g.left)
        self.wire.got(9, self.rf1.at[self.hi], self.g.right)
        self.finish(self.rf0, self.rf1, self.rf2)

    def stages(self):
        def start():
            self.opposite()
            self.twins()
            self.early()

        return [start, self.across, self.twin, self.ring, self.last]


def run_both(a, b):
    for fa, fb in zip(a, b):
        fa()
        fb()


PLACE = {key: k for k, key in enumerate((OWN, TWIN, RIGHT, LEFT, TWIN_FAR, FAR, TWIN_RIGHT, TWIN_LEFT))}


def rows_of(ref, size, base=0):
    def at(key):
        return base + PLACE[key] * size

    def blk(key):
        return ref.at[pl.ds(at(key), size)]

    def half(key, h):
        return ref.at[pl.ds(at(key) + h * (size // 2), size // 2)]

    return blk, half


def score_terms(sim, scale, bias, diag):
    z = scale * sim + bias
    if diag is not None:
        z = jnp.where(diag, -z, z)
    e = jnp.exp(-jnp.abs(z))
    r = 1.0 / (1.0 + e)
    g = jnp.where(z >= 0.0, r, e * r)
    loss = jnp.maximum(z, 0.0) + jnp.log1p(e)
    if diag is not None:
        g = jnp.where(diag, -g, g)
    return loss, g


def fold(x):
    x = jnp.sum(x.reshape(x.shape[0] // 8, 8, x.shape[1]), axis=0)
    return sum(x[:, k * 128 : (k + 1) * 128] for k in range(x.shape[1] // 128))


def tile_of(m):
    div, least = (lambda a, b: a // b, min) if isinstance(m, int) else (lax.div, jnp.minimum)
    q = 3 - least(div(m, 7), 1) - least(div(m, 12), 1) - div(m, 15)
    r = m - (16 - (q + 1) * (q + 1))
    down = least(div(r, q + 1), 1)
    return r + down * (q - r), q + down * (r - q - 1 - q)


def main_kernel(
    block, scal, img_own, txt_own, img_x, txt_x, img_raw, txt_raw, sums, pack,
    img, txt, d_img, d_txt, give, taken, sbuf, gbuf,
    ibuf, ihalf, tbuf, thalf,
    ig_s, ig_r, tg_s, tg_r, is_s, is_r, ts_s, ts_r, core_s, core_r, hand_s, hand_r, local, free,
):
    place = Place()
    gi, gt = place.image_group(), place.text_group()
    c = place.c
    partner = place.partner()
    greet(place, (RIGHT, LEFT, TWIN))

    half_rows = 8 * block
    img_blk, img_half = rows_of(img, block)
    txt_blk, txt_half = rows_of(txt, block, half_rows)
    other_blk, _ = rows_of(txt, block)
    wi, wt, core = Wire(ig_s, ig_r), Wire(tg_s, tg_r), Wire(core_s, core_r)

    own_i = pltpu.make_async_copy(img_own, img_blk(OWN), local.at[0])
    own_t = pltpu.make_async_copy(txt_own, txt_blk(OWN), local.at[1])
    own_i.start()
    own_t.start()
    own_i.wait()
    own_t.wait()
    sent = iter(range(8))

    def share(key):
        core.go(next(sent), txt_blk(key), other_blk(key), partner)

    a = gather_stages(wi, gi, img_blk(OWN), img_blk, img_half, True)
    b = gather_stages(wt, gt, txt_blk(OWN), txt_blk, txt_half, True, share)
    a[0]()
    b[0]()
    share(OWN)
    img_f, txt_f = img_x.shape[1] // 2, txt_x.shape[1] // 2
    feats = img_f + txt_f

    def half_of(which, count):
        return pl.ds(pl.multiple_of(which * count, count), count)

    core.go(8, img_x.at[:, half_of(1 - c, img_f)], pack.at[:, pl.ds(feats, img_f)], partner)
    core.go(9, txt_x.at[:, half_of(1 - c, txt_f)], pack.at[:, pl.ds(feats + img_f, txt_f)], partner)
    for ref in (d_img, d_txt, give, sums):
        ref[...] = jnp.zeros_like(ref)
    run_both(a[1:], b[1:])
    for k, key in enumerate(SEEN):
        core.got(k, other_blk(key), partner)
    wi.drain()
    wt.drain()

    scale, bias = scal[0], scal[1]
    di_blk, di_half = rows_of(d_img, block)
    dt_blk, dt_half = rows_of(d_txt, block)

    outs = []

    def put(src, first, count, k):
        copy = pltpu.make_async_copy(src, pack.at[:, pl.ds(first, count)], local.at[4 + k])
        copy.start()
        outs.append(copy)

    def du_view(which, k):
        return pack.at[:, pl.ds(2 * feats + (2 * which + k) * img.shape[1], img.shape[1])]

    def finish(mine, raw, k):
        first = k * block
        step = 64

        def done(p, q, r):
            def rows_of_du(n, carry):
                at = pl.ds(pl.multiple_of(n * step, step), step)
                total = mine[at, :] + p[at, :] + (q[at, :] + r[at, :])
                img[pl.ds(pl.multiple_of(first + n * step, step), step), :] = pull_back(raw[at, :], scal[2] * total)
                return carry

            lax.fori_loop(0, block // step, rows_of_du, 0)
            core.go(10 + k, img.at[pl.ds(first, block)], du_view(1, k), partner)
            put(img.at[pl.ds(first, block)], 2 * feats + k * img.shape[1], img.shape[1], k)

        return done

    wi, wt = Wire(is_s, is_r), Wire(ts_s, ts_r)
    ri = Scatter(wi, gi, di_blk, di_half, (ibuf, ihalf), finish(di_blk(OWN), ibuf.at[0], 0))
    rt = Scatter(wt, gt, dt_blk, dt_half, (tbuf, thalf), finish(dt_blk(OWN), tbuf.at[0], 1))

    def hand(k):
        return pltpu.make_async_remote_copy(
            src_ref=give.at[pl.ds(k * TILE, TILE)], dst_ref=taken.at[k % 2], send_sem=hand_s.at[k], recv_sem=hand_r.at[k], device_id=partner, device_id_type=MESH
        )

    def give_chunk(k):
        if k < 2:
            pl.semaphore_wait(free, 1)
        hand(k).start()

    def take_chunk(k):
        hand(k).wait_recv()
        v = d_txt.at[pl.ds(k * TILE, TILE)]
        v[...] += taken[k % 2]
        if k >= 2:
            pl.semaphore_signal(free, inc=1, device_id=partner, device_id_type=MESH)

    def rows(chunk, first=0):
        at = first + chunk * TILE
        return pl.ds(at if isinstance(at, int) else pl.multiple_of(at, TILE), TILE)

    def txt_rows(cc, chunk):
        return rows(chunk, cc * half_rows)

    def score(m, cc):
        i, j = tile_of(m)
        sbuf[cc] = lax.dot_general(img[rows(i), :], txt[txt_rows(cc, j), :], (((1,), (1,)), ((), ())), preferred_element_type=F32)

    def point(cc, diag=None):
        sim = sbuf[cc]
        loss, g = score_terms(sim, scale, bias, diag)
        sums[0] += fold(loss)
        sums[1] += fold(g * sim)
        sums[2] += fold(g)
        gbuf[cc] = g.astype(BF16)

    def products(m, cc):
        i, j = tile_of(m)
        gb = gbuf[cc]
        d_img[rows(i), :] += jnp.dot(gb, txt[txt_rows(cc, j), :], preferred_element_type=F32)
        ref = d_txt if cc else give
        ref[rows(j), :] += lax.dot_general(gb, img[rows(i), :], (((0,), (0,)), ((), ())), preferred_element_type=F32)

    events = {
        3: [lambda: give_chunk(3)],
        4: [lambda: take_chunk(3), rt.twins],
        6: [ri.twins],
        9: [lambda: give_chunk(2)],
        10: [lambda: take_chunk(2), rt.opposite],
        11: [ri.opposite],
        13: [lambda: give_chunk(1)],
        14: [lambda: take_chunk(1), rt.early, ri.early],
    }
    score(0, 0)
    score(0, 1)
    point(0)

    def step(m, carry):
        score(m + 1, 0)
        point(1)
        products(m, 0)
        score(m + 1, 1)
        point(0)
        products(m, 1)
        for at, todo in events.items():
            @pl.when(m == at)
            def _(todo=todo):
                for f in todo:
                    f()

        return carry

    lax.fori_loop(0, 15, step, 0)
    row = lax.broadcasted_iota(jnp.int32, (TILE, TILE), 0)
    col = lax.broadcasted_iota(jnp.int32, (TILE, TILE), 1)
    point(1, (row == col) & (row < block))
    products(15, 0)
    give_chunk(0)
    products(15, 1)
    rt.across()
    ri.twin()
    ri.across()
    keep = [pltpu.make_async_copy(x.at[:, half_of(c, n)], img.at[pl.ds((2 + k) * block, block), pl.ds(0, n)], local.at[2 + k]) for k, (x, n) in enumerate(((img_x, img_f), (txt_x, txt_f)))]
    keep += [pltpu.make_async_copy(img_raw, ibuf.at[0], local.at[0]), pltpu.make_async_copy(txt_raw, tbuf.at[0], local.at[1])]
    for copy in keep:
        copy.start()
    take_chunk(0)
    rt.twin()
    for copy in keep:
        copy.wait()
    put(img.at[pl.ds(2 * block, block)], 0, img_f, 2)
    put(img.at[pl.ds(3 * block, block), pl.ds(0, txt_f)], img_f, txt_f, 3)
    rt.ring()
    ri.ring()
    rt.last()
    ri.last()
    for k, first in enumerate((feats, feats + img_f)):
        core.got(8 + k, pack.at[:, pl.ds(first, (img_f, txt_f)[k])], partner)
        core.got(10 + k, du_view(1, k), partner)
    for k in range(4):
        hand(k).wait_send()
    for copy in outs:
        copy.wait()
    for wire in (wi, wt, core):
        wire.drain()


def main_call(scal, img_emb, txt_emb, img_x, txt_x, img_raw, txt_raw):
    block, dim = img_emb.shape
    vmem = pl.BlockSpec(memory_space=pltpu.VMEM)
    hbm = pl.BlockSpec(memory_space=pl.ANY)
    sem = pltpu.SemaphoreType.DMA
    f = lambda *s: pltpu.VMEM(s, F32)
    return pl.pallas_call(
        functools.partial(main_kernel, block),
        in_specs=[pl.BlockSpec(memory_space=pltpu.SMEM)] + [hbm] * 6,
        out_specs=[vmem, hbm],
        out_shape=[
            jax.ShapeDtypeStruct((3, 8, 128), F32),
            jax.ShapeDtypeStruct((block, img_x.shape[1] + txt_x.shape[1] + 4 * dim), BF16),
        ],
        scratch_shapes=[
            pltpu.VMEM((8 * block, dim), BF16),
            pltpu.VMEM((16 * block, dim), BF16),
            f(8 * block, dim),
            f(8 * block, dim),
            f(8 * block, dim),
            f(2, TILE, dim),
            f(2, TILE, TILE),
            pltpu.VMEM((2, TILE, TILE), BF16),
            f(6, block, dim),
            f(2, block // 2, dim),
            f(6, block, dim),
            f(2, block // 2, dim),
            sem((GATHER_COPIES,)), sem((GATHER_COPIES,)), sem((GATHER_COPIES,)), sem((GATHER_COPIES,)),
            sem((SCATTER_COPIES,)), sem((SCATTER_COPIES,)), sem((SCATTER_COPIES,)), sem((SCATTER_COPIES,)),
            sem((12,)), sem((12,)), sem((4,)), sem((4,)), sem((8,)), pltpu.SemaphoreType.REGULAR,
        ],
        compiler_params=pltpu.CompilerParams(collective_id=0, has_side_effects=True, vmem_limit_bytes=VMEM_LIMIT),
        name="scores",
    )(scal, img_emb, txt_emb, img_x, txt_x, img_raw, txt_raw)


def pull_back(raw, cot):
    inv = lax.rsqrt(jnp.sum(raw * raw, axis=-1, keepdims=True))
    along = jnp.sum(cot * raw, axis=-1, keepdims=True) * (inv * inv)
    return (inv * (cot - raw * along)).astype(BF16)


COLOURS = 4


def sum_kernel(
    pack, sums_in, d_w_img, d_w_txt, sums,
    w, w2, buf1, half1, buf2, small,
    sc_s, sc_r, ga_s, ga_r, out_s, out_r, core_s, core_r, small_s, small_r, local,
):
    place = Place()
    c, partner = place.c, place.partner()
    greet(place, SEEN[1:])
    img_f, txt_f, feats = d_w_img.shape[0] // 2, d_w_txt.shape[0] // 2, w.shape[0]
    ni, nt = img_f // 16, txt_f // 16
    rows, wide = ni + nt, w.shape[1] // 2
    tall, lanes = rows // 2, wide // 4

    def outer(lhs, rhs):
        return lax.dot_general(lhs, rhs, (((0,), (0,)), ((), ())), preferred_element_type=F32)

    def weights(to, first, count, size, shift, k):
        lane, dim = 128, w.shape[1]
        for at in range(0, count, lane):
            val = sum(
                outer(pack[:, side * feats + first + at : side * feats + first + at + lane], pack[:, pl.ds(2 * feats + (2 * side + k) * dim + to * wide, wide)])
                for side in range(2)
            )
            for b in range(lane // size):
                top = (at // size + b) * rows + shift
                w[top : top + size, pl.ds(to * wide, wide)] = val[b * size : (b + 1) * size]

    def lane_half(to):
        weights(to, 0, img_f, ni, 0, 0)
        weights(to, img_f, txt_f, nt, ni, 1)

    lane_half(0)

    small_wire = Wire(small_s, small_r)
    hops = []
    for name in "xyz":
        v = getattr(place, name)
        hops += [place.at(**{name: place.near(v)}), place.at(**{name: place.far(v)})]
    hops.append(partner)
    small[0] = sums_in[...]

    def small_step(n):
        if 0 < n <= len(hops):
            k = n - 1
            small_wire.got(k, small.at[2 * k + 1], hops[k])
            small[2 * n] = small[2 * k] + small[2 * k + 1]
        if n < len(hops):
            small_wire.go(n, small.at[2 * n], small.at[2 * n + 1], hops[n])

    dwire = Pieces(core_s, core_r)
    copies = []

    def sl(first, count):
        return pl.ds(pl.multiple_of(first, count), count)

    def rows_at(first, count):
        return pl.ds(pl.multiple_of(first, 8), count)

    def colour(n):
        order = (place.image_group(), place.text_group())
        g1, g2 = order if n % 2 == 0 else order[::-1]
        group = n % 2 * 8
        base = group * rows
        across = pl.ds(n // 2 * wide, wide)
        mine = base + g1.slot(OWN) * rows
        keep = n % 2 * rows

        def w_blk(key):
            return w.at[sl(base + g1.slot(key) * rows, rows), across]

        def w_half(key, h):
            return w.at[sl(base + g1.slot(key) * rows + h * tall, tall), across]

        def strip(ref, first):
            def at(key):
                slot = g2.slot(key)
                return first + lax.div(slot, 4) * tall, sl(n // 2 * wide + lax.rem(slot, 4) * lanes, lanes)

            def blk(key):
                top, cols = at(key)
                return ref.at[rows_at(top, tall), cols]

            return blk

        def outs(key, core, h, parts):
            at = group + g1.slot(key)
            a, b = ni // parts, nt // parts
            return (
                d_w_img.at[sl(core * img_f + at * ni + h * a, a), across],
                d_w_txt.at[sl(core * txt_f + at * nt + h * b, b), across],
            )

        def o_blk(key, core=c):
            return outs(key, core, 0, 1)

        def o_half(key, h):
            return outs(key, c, h, 2)

        ws_blk = strip(w, mine)
        os_blk = strip(w2, keep)

        def done1(p, q, r):
            v = w_blk(OWN)
            v[...] += p[...] + q[...] + r[...]

        def done2(terms):
            v = os_blk(OWN)
            v[...] = ws_blk(OWN)[...] + sum(terms)

        whole = w2.at[pl.ds(keep, ni), across], w2.at[pl.ds(keep + ni, nt), across]
        turn = iter(range(n * 8, n * 8 + 8))

        def share(key, src=None):
            dwire.go(next(turn), o_blk(key) if src is None else src, o_blk(key), partner)

        def share_own():
            share(OWN, whole)
            for p, (src, dst) in enumerate(zip(whole, o_blk(OWN))):
                copy = pltpu.make_async_copy(src, dst, local.at[2 * n + p])
                copy.start()
                copies.append(copy)

        def got_shares():
            for k, key in enumerate(SEEN):
                dwire.got(n * 8 + k, o_blk(key, 1 - c), partner)

        w1, w2_, w3 = (Wire(*args) for args in ((sc_s, sc_r, n * SCATTER_COPIES), (sc_s, sc_r, (COLOURS + n) * SCATTER_COPIES), (ga_s, ga_r, n * GATHER_COPIES)))
        w4 = Pieces(out_s, out_r, 2 * n * GATHER_COPIES)
        stages = Scatter(w1, g1, w_blk, w_half, (buf1.at[n], half1.at[n]), done1).stages()
        stages += direct_scatter_stages(w2_, g2, ws_blk, buf2.at[n], done2)
        stages += direct_stages(w3, g2, os_blk)
        tail = gather_stages(w4, g1, whole, o_blk, o_half, False, share)
        stages += [tail[0], share_own] + tail[1:] + [got_shares]
        return stages, [w1, w2_, w3, w4]

    colours = [colour(n) for n in range(COLOURS)]
    for n in range(len(colours[0][0]) + 1):
        for k, (stages, _) in enumerate(colours):
            at = n - k // 2 * 1
            if 0 <= at < len(stages):
                stages[at]()
        if n == 0:
            lane_half(1)
        small_step(n)
    sums[...] = small[2 * len(hops)]
    for copy in copies:
        copy.wait()
    for _, wires in colours:
        for wire in wires:
            wire.drain()
    dwire.drain()
    small_wire.drain()


def sum_call(pack, sums, img_x, txt_x, dim):
    feats = (img_x.shape[1] + txt_x.shape[1]) // 2
    vmem = pl.BlockSpec(memory_space=pltpu.VMEM)
    hbm = pl.BlockSpec(memory_space=pl.ANY)
    sem = lambda n: [pltpu.SemaphoreType.DMA((n,))] * 2
    f = lambda *s: pltpu.VMEM(s, F32)
    rows, wide = feats // 16, dim // 2
    tall, lanes = rows // 2, wide // 4
    return pl.pallas_call(
        sum_kernel,
        in_specs=[vmem, vmem],
        out_specs=[hbm, hbm, vmem],
        out_shape=[
            jax.ShapeDtypeStruct((img_x.shape[1], dim), F32),
            jax.ShapeDtypeStruct((txt_x.shape[1], dim), F32),
            jax.ShapeDtypeStruct(sums.shape, F32),
        ],
        scratch_shapes=[
            f(feats, dim),
            f(2 * rows, dim),
            f(COLOURS, 6, rows, wide), f(COLOURS, 2, tall, wide),
            f(COLOURS, 7, tall, lanes),
            f(15, *sums.shape),
            *sem(2 * COLOURS * SCATTER_COPIES), *sem(COLOURS * GATHER_COPIES), *sem(2 * COLOURS * GATHER_COPIES),
            *sem(2 * COLOURS * 8), *sem(7), pltpu.SemaphoreType.DMA((2 * COLOURS,)),
        ],
        compiler_params=pltpu.CompilerParams(collective_id=1, has_side_effects=True, vmem_limit_bytes=32 * 2**20),
        name="weights",
    )(pack, sums)


def store_kernel(total_rows, scal, sums, src_a, src_b, loss, d_temp, d_bias, dst_a, dst_b, sems):
    copies = [pltpu.make_async_copy(src_a, dst_a, sems.at[0]), pltpu.make_async_copy(src_b, dst_b, sems.at[1])]
    for copy in copies:
        copy.start()
    loss[0] = jnp.sum(sums[0]) / total_rows
    d_temp[0] = scal[0] * (jnp.sum(sums[1]) / total_rows)
    d_bias[0] = jnp.sum(sums[2]) / total_rows
    for copy in copies:
        copy.wait()


def store_call(total_rows, scal, sums, *arrays):
    hbm = pl.BlockSpec(memory_space=pl.ANY)
    smem = pl.BlockSpec(memory_space=pltpu.SMEM)
    one = jax.ShapeDtypeStruct((1,), F32)
    return pl.pallas_call(
        functools.partial(store_kernel, total_rows),
        in_specs=[smem, pl.BlockSpec(memory_space=pltpu.VMEM), hbm, hbm],
        out_specs=[smem] * 3 + [pl.BlockSpec(memory_space=pltpu.HBM)] * 2,
        out_shape=[one] * 3 + [jax.ShapeDtypeStruct(a.shape, a.dtype) for a in arrays],
        scratch_shapes=[pltpu.SemaphoreType.DMA((2,))],
        compiler_params=pltpu.CompilerParams(vmem_limit_bytes=2**20),
        name="store",
    )(scal, sums, *arrays)


def solution(mesh):
    dev_count = mesh.shape["replica"] * mesh.shape["data"]
    batch_axes = ("replica", "data")

    def local_fn(img_x, txt_x, w_img, w_txt, log_temp, logit_bias):
        block = img_x.shape[0]
        total_rows = block * dev_count
        txt_raw, txt_emb = embed_rows(txt_x, w_txt)
        img_raw, img_emb = embed_rows(img_x, w_img)
        temp_scale = jnp.exp(log_temp[0])
        scal = jnp.stack([temp_scale, logit_bias[0], temp_scale / total_rows])
        sums, pack = main_call(scal, img_emb, txt_emb, img_x, txt_x, img_raw, txt_raw)
        d_w_img, d_w_txt, sums = sum_call(pack, sums, img_x, txt_x, w_img.shape[1])
        return tuple(store_call(total_rows, scal, sums, d_w_img, d_w_txt))

    batch_spec = P(batch_axes, None)
    return jax.shard_map(local_fn, mesh=mesh, in_specs=(batch_spec, batch_spec, P(), P(), P(), P()), out_specs=(P(), P(), P(), P(), P()), check_vma=False)
```

```python
import functools

import jax
import jax.numpy as jnp
from jax import lax
from jax.experimental import pallas as pl
from jax.experimental.pallas import tpu as pltpu
from jax.sharding import PartitionSpec as P

F32 = jnp.float32
BF16 = jnp.bfloat16
TILE = 512
MESH = pl.DeviceIdType.MESH
VMEM_LIMIT = 67043328


def embed_rows(feat_x, w_proj):
    raw = jnp.dot(feat_x, w_proj, preferred_element_type=F32)
    return raw, (raw * lax.rsqrt(jnp.sum(raw * raw, axis=-1, keepdims=True))).astype(BF16)


OWN, RIGHT, LEFT, FAR = ((0, step) for step in (0, 1, -1, 2))
TWIN, TWIN_RIGHT, TWIN_LEFT, TWIN_FAR = ((1, step) for step in (0, 1, -1, 2))
SEEN = [OWN, LEFT, RIGHT, TWIN, FAR, TWIN_LEFT, TWIN_RIGHT, TWIN_FAR]


class Place:
    def __init__(self):
        rep, dat = lax.axis_index("replica"), lax.axis_index("data")
        self.z, self.y = lax.div(rep, 4), lax.rem(rep, 4)
        self.x, self.c = lax.div(dat, 2), lax.rem(dat, 2)

    def at(self, x=None, y=None, z=None, c=None):
        x = self.x if x is None else lax.rem(x + 8, 4)
        y = self.y if y is None else lax.rem(y + 8, 4)
        z = self.z if z is None else lax.rem(z + 8, 4)
        c = self.c if c is None else c
        return (z * 4 + y, x * 2 + c)

    def partner(self):
        return self.at(c=1 - self.c)

    def near(self, v):
        return v + 1 - 2 * lax.rem(v, 2)

    def far(self, v):
        return v - 1 + 2 * lax.rem(v, 2)

    def image_group(self):
        return Group(self.x, lax.rem(lax.div(self.y + 1, 2), 2), lambda key: self.at(x=self.x + key[1], y=self.near(self.y) if key[0] else None))

    def text_group(self):
        return Group(self.z, lax.div(self.y, 2), lambda key: self.at(z=self.z + key[1], y=self.far(self.y) if key[0] else None))

    def peers(self, keys):
        return [self.partner()] + [g.dev(key) for g in (self.image_group(), self.text_group()) for key in keys]


class Group:
    def __init__(self, pos, side, dev):
        self.pos, self.side, self.dev = pos, side, dev
        self.right, self.left, self.pair = (dev(key) for key in (RIGHT, LEFT, TWIN))

    def slot(self, key):
        side = 1 - self.side if key[0] else self.side
        return side * 4 + lax.rem(self.pos + key[1] + 4, 4)


def greet(place, keys):
    barrier = pltpu.get_barrier_semaphore()
    peers = place.peers(keys)
    for dev in peers:
        pl.semaphore_signal(barrier, inc=1, device_id=dev, device_id_type=MESH)
    pl.semaphore_wait(barrier, len(peers))


class Wire:
    def __init__(self, send, recv, first=0):
        self.send, self.recv, self.first, self.open = send, recv, first, []

    def copy(self, k, src, dst, dev):
        k += self.first
        return pltpu.make_async_remote_copy(src_ref=src, dst_ref=dst, send_sem=self.send.at[k], recv_sem=self.recv.at[k], device_id=dev, device_id_type=MESH)

    def go(self, *what):
        self.copy(*what).start()
        self.open.append(what)

    def got(self, k, dst, dev):
        self.copy(k, dst, dst, dev).wait_recv()

    def drain(self):
        for what in self.open:
            self.copy(*what).wait_send()
        self.open = []


class Pieces:
    def __init__(self, *where):
        self.wire = Wire(*where)

    def go(self, k, src, dst, dev):
        for p in range(2):
            self.wire.go(2 * k + p, src[p], dst[p], dev)

    def got(self, k, dst, dev):
        for p in range(2):
            self.wire.got(2 * k + p, dst[p], dev)

    def drain(self):
        self.wire.drain()


GATHER_COPIES = 8
SCATTER_COPIES = 10


def gather_stages(wire, g, own, blk, half, relative, seen=None):
    seen = seen or (lambda key: None)

    def moved(key, way):
        twin, step = key
        if not relative:
            return key
        twin, step = {"right": (twin, step - 1), "left": (twin, step + 1), "pair": (1 - twin, step)}[way]
        return twin, (step + 1) % 4 - 1

    def send(k, key, way, h=None):
        dev = getattr(g, way)
        view = blk if h is None else functools.partial(half, h=h)
        wire.go(k, view(key), view(moved(key, way)), dev)

    def start():
        for k, way in enumerate(("right", "left", "pair")):
            wire.go(k, own, blk(moved(OWN, way)), getattr(g, way))

    def ring():
        wire.got(0, blk(LEFT), g.left)
        send(3, LEFT, "right", 0)
        wire.got(1, blk(RIGHT), g.right)
        send(4, RIGHT, "left", 1)
        seen(LEFT)
        seen(RIGHT)

    def twin():
        wire.got(2, blk(TWIN), g.pair)
        send(5, TWIN, "right")
        send(6, TWIN, "left")
        seen(TWIN)

    def across():
        wire.got(3, half(FAR, 0), g.left)
        wire.got(4, half(FAR, 1), g.right)
        send(7, FAR, "pair")
        seen(FAR)

    def last():
        wire.got(5, blk(TWIN_LEFT), g.left)
        wire.got(6, blk(TWIN_RIGHT), g.right)
        seen(TWIN_LEFT)
        seen(TWIN_RIGHT)

    def far():
        wire.got(7, blk(TWIN_FAR), g.pair)
        seen(TWIN_FAR)

    return [start, ring, twin, across, last, far]


def direct_stages(wire, g, blk):
    def send():
        for k, key in enumerate(SEEN[1:]):
            wire.go(k, blk(OWN), blk(OWN), g.dev(key))

    def take():
        for k, (twin, step) in enumerate(SEEN[1:]):
            back = (twin, step if step == 2 else -step)
            wire.got(k, blk(back), g.dev(back))

    return [send, take]


def direct_scatter_stages(wire, g, blk, bufs, done):
    def send():
        for k, key in enumerate(SEEN[1:]):
            wire.go(k, blk(key), bufs.at[k], g.dev(key))

    def take():
        for k, (twin, step) in enumerate(SEEN[1:]):
            wire.got(k, bufs.at[k], g.dev((twin, step if step == 2 else -step)))
        done([bufs[k] for k in range(7)])

    return [send, take]


class Scatter:
    def __init__(self, wire, g, blk, half, bufs, finish):
        self.wire, self.g, self.blk, self.half, self.finish = wire, g, blk, half, finish
        whole, part = bufs
        self.rp, self.rr0, self.rr1, self.rf0, self.rf1, self.rf2 = (whole.at[k] for k in range(6))
        rows, cut = whole.shape[1], part.shape[1]
        self.lo, self.hi = pl.ds(0, cut), pl.ds(cut, rows - cut)
        self.rh0, self.rh1 = part.at[0], part.at[1, pl.ds(0, rows - cut)]

    def twins(self):
        self.wire.go(1, self.blk(TWIN_RIGHT), self.rr0, self.g.right)
        self.wire.go(2, self.blk(TWIN_LEFT), self.rr1, self.g.left)

    def opposite(self):
        self.wire.go(0, self.blk(TWIN_FAR), self.rp, self.g.pair)

    def early(self):
        self.wire.go(3, self.half(RIGHT, 1), self.rf0.at[self.hi], self.g.right)
        self.wire.go(4, self.half(LEFT, 0), self.rf1.at[self.lo], self.g.left)

    def across(self):
        self.wire.got(0, self.rp, self.g.pair)
        for h, sl in ((0, self.lo), (1, self.hi)):
            v = self.half(FAR, h)
            v[...] += self.rp[sl]
        self.wire.go(5, self.half(FAR, 0), self.rh0, self.g.right)
        self.wire.go(6, self.half(FAR, 1), self.rh1, self.g.left)

    def twin(self):
        self.wire.got(1, self.rr0, self.g.left)
        self.wire.got(2, self.rr1, self.g.right)
        v = self.blk(TWIN)
        v[...] += self.rr0[...] + self.rr1[...]
        self.wire.go(7, v, self.rf2, self.g.pair)

    def ring(self):
        self.wire.got(5, self.rh0, self.g.left)
        v = self.half(RIGHT, 0)
        v[...] += self.rh0[...]
        self.wire.go(8, v, self.rf0.at[self.lo], self.g.right)
        self.wire.got(6, self.rh1, self.g.right)
        v = self.half(LEFT, 1)
        v[...] += self.rh1[...]
        self.wire.go(9, v, self.rf1.at[self.hi], self.g.left)

    def last(self):
        self.wire.got(3, self.rf0.at[self.hi], self.g.left)
        self.wire.got(4, self.rf1.at[self.lo], self.g.right)
        self.wire.got(7, self.rf2, self.g.pair)
        self.wire.got(8, self.rf0.at[self.lo], self.g.left)
        self.wire.got(9, self.rf1.at[self.hi], self.g.right)
        self.finish(self.rf0, self.rf1, self.rf2)

    def stages(self):
        def start():
            self.opposite()
            self.twins()
            self.early()

        return [start, self.across, self.twin, self.ring, self.last]


def run_both(a, b):
    for fa, fb in zip(a, b):
        fa()
        fb()


PLACE = {key: k for k, key in enumerate((OWN, TWIN, RIGHT, LEFT, TWIN_FAR, FAR, TWIN_RIGHT, TWIN_LEFT))}


def rows_of(ref, size, base=0):
    def at(key):
        return base + PLACE[key] * size

    def blk(key):
        return ref.at[pl.ds(at(key), size)]

    def half(key, h):
        return ref.at[pl.ds(at(key) + h * (size // 2), size // 2)]

    return blk, half


def score_terms(sim, scale, bias, diag):
    z = scale * sim + bias
    if diag is not None:
        z = jnp.where(diag, -z, z)
    e = jnp.exp(-jnp.abs(z))
    r = 1.0 / (1.0 + e)
    g = jnp.where(z >= 0.0, r, e * r)
    loss = jnp.maximum(z, 0.0) + jnp.log1p(e)
    if diag is not None:
        g = jnp.where(diag, -g, g)
    return loss, g


def fold(x):
    x = jnp.sum(x.reshape(x.shape[0] // 8, 8, x.shape[1]), axis=0)
    return sum(x[:, k * 128 : (k + 1) * 128] for k in range(x.shape[1] // 128))


def tile_of(m):
    div, least = (lambda a, b: a // b, min) if isinstance(m, int) else (lax.div, jnp.minimum)
    q = 3 - least(div(m, 7), 1) - least(div(m, 12), 1) - div(m, 15)
    r = m - (16 - (q + 1) * (q + 1))
    down = least(div(r, q + 1), 1)
    return r + down * (q - r), q + down * (r - q - 1 - q)


def main_kernel(
    block, scal, img_own, txt_own, img_x, txt_x, img_raw, txt_raw, sums, pack,
    img, txt, d_img, d_txt, give, taken, sbuf, gbuf,
    ibuf, ihalf, tbuf, thalf,
    ig_s, ig_r, tg_s, tg_r, is_s, is_r, ts_s, ts_r, core_s, core_r, hand_s, hand_r, local, free,
):
    place = Place()
    gi, gt = place.image_group(), place.text_group()
    c = place.c
    partner = place.partner()
    greet(place, (RIGHT, LEFT, TWIN))

    half_rows = 8 * block
    img_blk, img_half = rows_of(img, block)
    txt_blk, txt_half = rows_of(txt, block, half_rows)
    other_blk, _ = rows_of(txt, block)
    wi, wt, core = Wire(ig_s, ig_r), Wire(tg_s, tg_r), Wire(core_s, core_r)

    own_i = pltpu.make_async_copy(img_own, img_blk(OWN), local.at[0])
    own_t = pltpu.make_async_copy(txt_own, txt_blk(OWN), local.at[1])
    own_i.start()
    own_t.start()
    own_i.wait()
    own_t.wait()
    sent = iter(range(8))

    def share(key):
        core.go(next(sent), txt_blk(key), other_blk(key), partner)

    a = gather_stages(wi, gi, img_blk(OWN), img_blk, img_half, True)
    b = gather_stages(wt, gt, txt_blk(OWN), txt_blk, txt_half, True, share)
    a[0]()
    b[0]()
    share(OWN)
    img_f, txt_f = img_x.shape[1] // 2, txt_x.shape[1] // 2
    feats = img_f + txt_f

    def half_of(which, count):
        return pl.ds(pl.multiple_of(which * count, count), count)

    core.go(8, img_x.at[:, half_of(1 - c, img_f)], pack.at[:, pl.ds(feats, img_f)], partner)
    core.go(9, txt_x.at[:, half_of(1 - c, txt_f)], pack.at[:, pl.ds(feats + img_f, txt_f)], partner)
    for ref in (d_img, d_txt, give, sums):
        ref[...] = jnp.zeros_like(ref)
    run_both(a[1:4], b[1:4])
    b[4]()

    def take_texts(first, last):
        for k in range(first, last):
            core.got(k, other_blk(SEEN[k]), partner)

    def gather_rest():
        b[5]()
        a[4]()
        a[5]()

    take_texts(0, 7)

    scale, bias = scal[0], scal[1]
    di_blk, di_half = rows_of(d_img, block)
    dt_blk, dt_half = rows_of(d_txt, block)

    outs = []

    def put(src, first, count, k):
        copy = pltpu.make_async_copy(src, pack.at[:, pl.ds(first, count)], local.at[4 + k])
        copy.start()
        outs.append(copy)

    def du_view(which, k):
        return pack.at[:, pl.ds(2 * feats + (2 * which + k) * img.shape[1], img.shape[1])]

    def finish(mine, raw, k):
        first = k * block
        step = 64

        def done(p, q, r):
            def rows_of_du(n, carry):
                at = pl.ds(pl.multiple_of(n * step, step), step)
                total = mine[at, :] + p[at, :] + (q[at, :] + r[at, :])
                img[pl.ds(pl.multiple_of(first + n * step, step), step), :] = pull_back(raw[at, :], scal[2] * total)
                return carry

            lax.fori_loop(0, block // step, rows_of_du, 0)
            core.go(10 + k, img.at[pl.ds(first, block)], du_view(1, k), partner)
            put(img.at[pl.ds(first, block)], 2 * feats + k * img.shape[1], img.shape[1], k)

        return done

    si, st = Wire(is_s, is_r), Wire(ts_s, ts_r)
    ri = Scatter(si, gi, di_blk, di_half, (ibuf, ihalf), finish(di_blk(OWN), ibuf.at[0], 0))
    rt = Scatter(st, gt, dt_blk, dt_half, (tbuf, thalf), finish(dt_blk(OWN), tbuf.at[0], 1))

    def hand(k):
        return pltpu.make_async_remote_copy(
            src_ref=give.at[pl.ds(k * TILE, TILE)], dst_ref=taken.at[k % 2], send_sem=hand_s.at[k], recv_sem=hand_r.at[k], device_id=partner, device_id_type=MESH
        )

    def give_chunk(k):
        if k < 2:
            pl.semaphore_wait(free, 1)
        hand(k).start()

    def take_chunk(k):
        hand(k).wait_recv()
        v = d_txt.at[pl.ds(k * TILE, TILE)]
        v[...] += taken[k % 2]
        if k >= 2:
            pl.semaphore_signal(free, inc=1, device_id=partner, device_id_type=MESH)

    def rows(chunk, first=0):
        at = first + chunk * TILE
        return pl.ds(at if isinstance(at, int) else pl.multiple_of(at, TILE), TILE)

    def txt_rows(cc, chunk):
        return rows(chunk, cc * half_rows)

    def score(m, cc):
        i, j = tile_of(m)
        sbuf[cc] = lax.dot_general(img[rows(i), :], txt[txt_rows(cc, j), :], (((1,), (1,)), ((), ())), preferred_element_type=F32)

    def point(cc, diag=None):
        sim = sbuf[cc]
        loss, g = score_terms(sim, scale, bias, diag)
        sums[0] += fold(loss)
        sums[1] += fold(g * sim)
        sums[2] += fold(g)
        gbuf[cc] = g.astype(BF16)

    def products(m, cc):
        i, j = tile_of(m)
        gb = gbuf[cc]
        d_img[rows(i), :] += jnp.dot(gb, txt[txt_rows(cc, j), :], preferred_element_type=F32)
        ref = d_txt if cc else give
        ref[rows(j), :] += lax.dot_general(gb, img[rows(i), :], (((0,), (0,)), ((), ())), preferred_element_type=F32)

    events = {
        0: [gather_rest],
        2: [lambda: take_texts(7, 8)],
        3: [lambda: give_chunk(3)],
        4: [lambda: take_chunk(3), rt.twins],
        6: [ri.twins],
        9: [lambda: give_chunk(2)],
        10: [lambda: take_chunk(2), rt.opposite],
        11: [ri.opposite],
        13: [lambda: give_chunk(1)],
        14: [lambda: take_chunk(1), rt.early, ri.early],
    }
    score(0, 0)
    score(0, 1)
    point(0)

    def step(m, carry):
        score(m + 1, 0)
        point(1)
        products(m, 0)
        score(m + 1, 1)
        point(0)
        products(m, 1)
        for at, todo in events.items():
            @pl.when(m == at)
            def _(todo=todo):
                for f in todo:
                    f()

        return carry

    lax.fori_loop(0, 15, step, 0)
    row = lax.broadcasted_iota(jnp.int32, (TILE, TILE), 0)
    col = lax.broadcasted_iota(jnp.int32, (TILE, TILE), 1)
    point(1, (row == col) & (row < block))
    products(15, 0)
    give_chunk(0)
    products(15, 1)
    rt.across()
    ri.twin()
    ri.across()
    wi.drain()
    wt.drain()
    keep = [pltpu.make_async_copy(x.at[:, half_of(c, n)], img.at[pl.ds((2 + k) * block, block), pl.ds(0, n)], local.at[2 + k]) for k, (x, n) in enumerate(((img_x, img_f), (txt_x, txt_f)))]
    keep += [pltpu.make_async_copy(img_raw, ibuf.at[0], local.at[0]), pltpu.make_async_copy(txt_raw, tbuf.at[0], local.at[1])]
    for copy in keep:
        copy.start()
    take_chunk(0)
    rt.twin()
    for copy in keep:
        copy.wait()
    put(img.at[pl.ds(2 * block, block)], 0, img_f, 2)
    put(img.at[pl.ds(3 * block, block), pl.ds(0, txt_f)], img_f, txt_f, 3)
    rt.ring()
    ri.ring()
    rt.last()
    ri.last()
    for k, first in enumerate((feats, feats + img_f)):
        core.got(8 + k, pack.at[:, pl.ds(first, (img_f, txt_f)[k])], partner)
        core.got(10 + k, du_view(1, k), partner)
    for k in range(4):
        hand(k).wait_send()
    for copy in outs:
        copy.wait()
    for wire in (si, st, core):
        wire.drain()


def main_call(scal, img_emb, txt_emb, img_x, txt_x, img_raw, txt_raw):
    block, dim = img_emb.shape
    vmem = pl.BlockSpec(memory_space=pltpu.VMEM)
    hbm = pl.BlockSpec(memory_space=pl.ANY)
    sem = pltpu.SemaphoreType.DMA
    f = lambda *s: pltpu.VMEM(s, F32)
    return pl.pallas_call(
        functools.partial(main_kernel, block),
        in_specs=[pl.BlockSpec(memory_space=pltpu.SMEM)] + [hbm] * 6,
        out_specs=[vmem, hbm],
        out_shape=[
            jax.ShapeDtypeStruct((3, 8, 128), F32),
            jax.ShapeDtypeStruct((block, img_x.shape[1] + txt_x.shape[1] + 4 * dim), BF16),
        ],
        scratch_shapes=[
            pltpu.VMEM((8 * block, dim), BF16),
            pltpu.VMEM((16 * block, dim), BF16),
            f(8 * block, dim),
            f(8 * block, dim),
            f(8 * block, dim),
            f(2, TILE, dim),
            f(2, TILE, TILE),
            pltpu.VMEM((2, TILE, TILE), BF16),
            f(6, block, dim),
            f(2, block // 2, dim),
            f(6, block, dim),
            f(2, block // 2, dim),
            sem((GATHER_COPIES,)), sem((GATHER_COPIES,)), sem((GATHER_COPIES,)), sem((GATHER_COPIES,)),
            sem((SCATTER_COPIES,)), sem((SCATTER_COPIES,)), sem((SCATTER_COPIES,)), sem((SCATTER_COPIES,)),
            sem((12,)), sem((12,)), sem((4,)), sem((4,)), sem((8,)), pltpu.SemaphoreType.REGULAR,
        ],
        compiler_params=pltpu.CompilerParams(collective_id=0, has_side_effects=True, vmem_limit_bytes=VMEM_LIMIT),
        name="scores",
    )(scal, img_emb, txt_emb, img_x, txt_x, img_raw, txt_raw)


def pull_back(raw, cot):
    inv = lax.rsqrt(jnp.sum(raw * raw, axis=-1, keepdims=True))
    along = jnp.sum(cot * raw, axis=-1, keepdims=True) * (inv * inv)
    return (inv * (cot - raw * along)).astype(BF16)


COLOURS = 4


def sum_kernel(
    pack, sums_in, d_w_img, d_w_txt, sums,
    w, w2, buf1, half1, buf2, small,
    sc_s, sc_r, ga_s, ga_r, out_s, out_r, core_s, core_r, small_s, small_r, local,
):
    place = Place()
    c, partner = place.c, place.partner()
    greet(place, SEEN[1:])
    img_f, txt_f, feats = d_w_img.shape[0] // 2, d_w_txt.shape[0] // 2, w.shape[0]
    ni, nt = img_f // 16, txt_f // 16
    rows, wide = ni + nt, w.shape[1] // 2
    tall, lanes = rows // 2, wide // 4

    def outer(lhs, rhs):
        return lax.dot_general(lhs, rhs, (((0,), (0,)), ((), ())), preferred_element_type=F32)

    def weights(to, first, count, size, shift, k):
        lane, dim = 128, w.shape[1]
        for at in range(0, count, lane):
            val = sum(
                outer(pack[:, side * feats + first + at : side * feats + first + at + lane], pack[:, pl.ds(2 * feats + (2 * side + k) * dim + to * wide, wide)])
                for side in range(2)
            )
            for b in range(lane // size):
                top = (at // size + b) * rows + shift
                w[top : top + size, pl.ds(to * wide, wide)] = val[b * size : (b + 1) * size]

    def lane_half(to):
        weights(to, 0, img_f, ni, 0, 0)
        weights(to, img_f, txt_f, nt, ni, 1)

    lane_half(0)

    small_wire = Wire(small_s, small_r)
    hops = []
    for name in "xyz":
        v = getattr(place, name)
        hops += [place.at(**{name: place.near(v)}), place.at(**{name: place.far(v)})]
    hops.append(partner)
    small[0] = sums_in[...]

    def small_step(n):
        if 0 < n <= len(hops):
            k = n - 1
            small_wire.got(k, small.at[2 * k + 1], hops[k])
            small[2 * n] = small[2 * k] + small[2 * k + 1]
        if n < len(hops):
            small_wire.go(n, small.at[2 * n], small.at[2 * n + 1], hops[n])

    dwire = Pieces(core_s, core_r)
    copies = []

    def sl(first, count):
        return pl.ds(pl.multiple_of(first, count), count)

    def rows_at(first, count):
        return pl.ds(pl.multiple_of(first, 8), count)

    def colour(n):
        order = (place.image_group(), place.text_group())
        g1, g2 = order if n % 2 == 0 else order[::-1]
        group = n % 2 * 8
        base = group * rows
        across = pl.ds(n // 2 * wide, wide)
        mine = base + g1.slot(OWN) * rows
        keep = n % 2 * rows

        def w_blk(key):
            return w.at[sl(base + g1.slot(key) * rows, rows), across]

        def w_half(key, h):
            return w.at[sl(base + g1.slot(key) * rows + h * tall, tall), across]

        def strip(ref, first):
            def at(key):
                slot = g2.slot(key)
                return first + lax.div(slot, 4) * tall, sl(n // 2 * wide + lax.rem(slot, 4) * lanes, lanes)

            def blk(key):
                top, cols = at(key)
                return ref.at[rows_at(top, tall), cols]

            return blk

        def outs(key, core, h, parts):
            at = group + g1.slot(key)
            a, b = ni // parts, nt // parts
            return (
                d_w_img.at[sl(core * img_f + at * ni + h * a, a), across],
                d_w_txt.at[sl(core * txt_f + at * nt + h * b, b), across],
            )

        def o_blk(key, core=c):
            return outs(key, core, 0, 1)

        def o_half(key, h):
            return outs(key, c, h, 2)

        ws_blk = strip(w, mine)
        os_blk = strip(w2, keep)

        def done1(p, q, r):
            v = w_blk(OWN)
            v[...] += p[...] + q[...] + r[...]

        def done2(terms):
            v = os_blk(OWN)
            v[...] = ws_blk(OWN)[...] + sum(terms)

        whole = w2.at[pl.ds(keep, ni), across], w2.at[pl.ds(keep + ni, nt), across]
        turn = iter(range(n * 8, n * 8 + 8))

        def share(key, src=None):
            dwire.go(next(turn), o_blk(key) if src is None else src, o_blk(key), partner)

        def share_own():
            share(OWN, whole)
            for p, (src, dst) in enumerate(zip(whole, o_blk(OWN))):
                copy = pltpu.make_async_copy(src, dst, local.at[2 * n + p])
                copy.start()
                copies.append(copy)

        def got_shares():
            for k, key in enumerate(SEEN):
                dwire.got(n * 8 + k, o_blk(key, 1 - c), partner)

        w1, w2_, w3 = (Wire(*args) for args in ((sc_s, sc_r, n * SCATTER_COPIES), (sc_s, sc_r, (COLOURS + n) * SCATTER_COPIES), (ga_s, ga_r, n * GATHER_COPIES)))
        w4 = Pieces(out_s, out_r, 2 * n * GATHER_COPIES)
        stages = Scatter(w1, g1, w_blk, w_half, (buf1.at[n], half1.at[n]), done1).stages()
        stages += direct_scatter_stages(w2_, g2, ws_blk, buf2.at[n], done2)
        stages += direct_stages(w3, g2, os_blk)
        tail = gather_stages(w4, g1, whole, o_blk, o_half, False, share)
        stages += [tail[0], share_own] + tail[1:] + [got_shares]
        return stages, [w1, w2_, w3, w4]

    colours = [colour(n) for n in range(COLOURS)]
    for n in range(len(colours[0][0]) + 1):
        for k, (stages, _) in enumerate(colours):
            at = n - k // 2 * 1
            if 0 <= at < len(stages):
                stages[at]()
        if n == 0:
            lane_half(1)
        small_step(n)
    sums[...] = small[2 * len(hops)]
    for copy in copies:
        copy.wait()
    for _, wires in colours:
        for wire in wires:
            wire.drain()
    dwire.drain()
    small_wire.drain()


def sum_call(pack, sums, img_x, txt_x, dim):
    feats = (img_x.shape[1] + txt_x.shape[1]) // 2
    vmem = pl.BlockSpec(memory_space=pltpu.VMEM)
    hbm = pl.BlockSpec(memory_space=pl.ANY)
    sem = lambda n: [pltpu.SemaphoreType.DMA((n,))] * 2
    f = lambda *s: pltpu.VMEM(s, F32)
    rows, wide = feats // 16, dim // 2
    tall, lanes = rows // 2, wide // 4
    return pl.pallas_call(
        sum_kernel,
        in_specs=[vmem, vmem],
        out_specs=[hbm, hbm, vmem],
        out_shape=[
            jax.ShapeDtypeStruct((img_x.shape[1], dim), F32),
            jax.ShapeDtypeStruct((txt_x.shape[1], dim), F32),
            jax.ShapeDtypeStruct(sums.shape, F32),
        ],
        scratch_shapes=[
            f(feats, dim),
            f(2 * rows, dim),
            f(COLOURS, 6, rows, wide), f(COLOURS, 2, tall, wide),
            f(COLOURS, 7, tall, lanes),
            f(15, *sums.shape),
            *sem(2 * COLOURS * SCATTER_COPIES), *sem(COLOURS * GATHER_COPIES), *sem(2 * COLOURS * GATHER_COPIES),
            *sem(2 * COLOURS * 8), *sem(7), pltpu.SemaphoreType.DMA((2 * COLOURS,)),
        ],
        compiler_params=pltpu.CompilerParams(collective_id=1, has_side_effects=True, vmem_limit_bytes=32 * 2**20),
        name="weights",
    )(pack, sums)


def store_kernel(total_rows, scal, sums, src_a, src_b, loss, d_temp, d_bias, dst_a, dst_b, sems):
    copies = [pltpu.make_async_copy(src_a, dst_a, sems.at[0]), pltpu.make_async_copy(src_b, dst_b, sems.at[1])]
    for copy in copies:
        copy.start()
    loss[0] = jnp.sum(sums[0]) / total_rows
    d_temp[0] = scal[0] * (jnp.sum(sums[1]) / total_rows)
    d_bias[0] = jnp.sum(sums[2]) / total_rows
    for copy in copies:
        copy.wait()


def store_call(total_rows, scal, sums, *arrays):
    hbm = pl.BlockSpec(memory_space=pl.ANY)
    smem = pl.BlockSpec(memory_space=pltpu.SMEM)
    one = jax.ShapeDtypeStruct((1,), F32)
    return pl.pallas_call(
        functools.partial(store_kernel, total_rows),
        in_specs=[smem, pl.BlockSpec(memory_space=pltpu.VMEM), hbm, hbm],
        out_specs=[smem] * 3 + [pl.BlockSpec(memory_space=pltpu.HBM)] * 2,
        out_shape=[one] * 3 + [jax.ShapeDtypeStruct(a.shape, a.dtype) for a in arrays],
        scratch_shapes=[pltpu.SemaphoreType.DMA((2,))],
        compiler_params=pltpu.CompilerParams(vmem_limit_bytes=2**20),
        name="store",
    )(scal, sums, *arrays)


def solution(mesh):
    dev_count = mesh.shape["replica"] * mesh.shape["data"]
    batch_axes = ("replica", "data")

    def local_fn(img_x, txt_x, w_img, w_txt, log_temp, logit_bias):
        block = img_x.shape[0]
        total_rows = block * dev_count
        txt_raw, txt_emb = embed_rows(txt_x, w_txt)
        img_raw, img_emb = embed_rows(img_x, w_img)
        temp_scale = jnp.exp(log_temp[0])
        scal = jnp.stack([temp_scale, logit_bias[0], temp_scale / total_rows])
        sums, pack = main_call(scal, img_emb, txt_emb, img_x, txt_x, img_raw, txt_raw)
        d_w_img, d_w_txt, sums = sum_call(pack, sums, img_x, txt_x, w_img.shape[1])
        return tuple(store_call(total_rows, scal, sums, d_w_img, d_w_txt))

    batch_spec = P(batch_axes, None)
    return jax.shard_map(local_fn, mesh=mesh, in_specs=(batch_spec, batch_spec, P(), P(), P(), P()), out_specs=(P(), P(), P(), P(), P()), check_vma=False)
```

```python
import functools

import jax
import jax.numpy as jnp
from jax import lax
from jax.experimental import pallas as pl
from jax.experimental.pallas import tpu as pltpu
from jax.sharding import PartitionSpec as P

F32 = jnp.float32
BF16 = jnp.bfloat16
TILE = 512
MESH = pl.DeviceIdType.MESH
VMEM_LIMIT = 67043328


def embed_rows(feat_x, w_proj):
    raw = jnp.dot(feat_x, w_proj, preferred_element_type=F32)
    return raw, (raw * lax.rsqrt(jnp.sum(raw * raw, axis=-1, keepdims=True))).astype(BF16)


OWN, RIGHT, LEFT, FAR = ((0, step) for step in (0, 1, -1, 2))
TWIN, TWIN_RIGHT, TWIN_LEFT, TWIN_FAR = ((1, step) for step in (0, 1, -1, 2))
SEEN = [OWN, LEFT, RIGHT, TWIN, FAR, TWIN_LEFT, TWIN_RIGHT, TWIN_FAR]


class Place:
    def __init__(self):
        rep, dat = lax.axis_index("replica"), lax.axis_index("data")
        self.z, self.y = lax.div(rep, 4), lax.rem(rep, 4)
        self.x, self.c = lax.div(dat, 2), lax.rem(dat, 2)

    def at(self, x=None, y=None, z=None, c=None):
        x = self.x if x is None else lax.rem(x + 8, 4)
        y = self.y if y is None else lax.rem(y + 8, 4)
        z = self.z if z is None else lax.rem(z + 8, 4)
        c = self.c if c is None else c
        return (z * 4 + y, x * 2 + c)

    def partner(self):
        return self.at(c=1 - self.c)

    def near(self, v):
        return v + 1 - 2 * lax.rem(v, 2)

    def far(self, v):
        return v - 1 + 2 * lax.rem(v, 2)

    def image_group(self):
        return Group(self.x, lax.rem(lax.div(self.y + 1, 2), 2), lambda key: self.at(x=self.x + key[1], y=self.near(self.y) if key[0] else None))

    def text_group(self):
        return Group(self.z, lax.div(self.y, 2), lambda key: self.at(z=self.z + key[1], y=self.far(self.y) if key[0] else None))

    def peers(self, keys):
        return [self.partner()] + [g.dev(key) for g in (self.image_group(), self.text_group()) for key in keys]


class Group:
    def __init__(self, pos, side, dev):
        self.pos, self.side, self.dev = pos, side, dev
        self.right, self.left, self.pair = (dev(key) for key in (RIGHT, LEFT, TWIN))

    def slot(self, key):
        side = 1 - self.side if key[0] else self.side
        return side * 4 + lax.rem(self.pos + key[1] + 4, 4)


def greet(place, keys):
    barrier = pltpu.get_barrier_semaphore()
    peers = place.peers(keys)
    for dev in peers:
        pl.semaphore_signal(barrier, inc=1, device_id=dev, device_id_type=MESH)
    return lambda: pl.semaphore_wait(barrier, len(peers))


class Wire:
    def __init__(self, send, recv, first=0):
        self.send, self.recv, self.first, self.open = send, recv, first, []

    def copy(self, k, src, dst, dev):
        k += self.first
        return pltpu.make_async_remote_copy(src_ref=src, dst_ref=dst, send_sem=self.send.at[k], recv_sem=self.recv.at[k], device_id=dev, device_id_type=MESH)

    def go(self, *what):
        self.copy(*what).start()
        self.open.append(what)

    def got(self, k, dst, dev):
        self.copy(k, dst, dst, dev).wait_recv()

    def drain(self):
        for what in self.open:
            self.copy(*what).wait_send()
        self.open = []


class Pieces:
    def __init__(self, *where):
        self.wire = Wire(*where)

    def go(self, k, src, dst, dev):
        for p in range(2):
            self.wire.go(2 * k + p, src[p], dst[p], dev)

    def got(self, k, dst, dev):
        for p in range(2):
            self.wire.got(2 * k + p, dst[p], dev)

    def drain(self):
        self.wire.drain()


GATHER_COPIES = 8
SCATTER_COPIES = 10


def gather_stages(wire, g, own, blk, half, relative, seen=None):
    seen = seen or (lambda key: None)

    def moved(key, way):
        twin, step = key
        if not relative:
            return key
        twin, step = {"right": (twin, step - 1), "left": (twin, step + 1), "pair": (1 - twin, step)}[way]
        return twin, (step + 1) % 4 - 1

    def send(k, key, way, h=None):
        dev = getattr(g, way)
        view = blk if h is None else functools.partial(half, h=h)
        wire.go(k, view(key), view(moved(key, way)), dev)

    def start():
        for k, way in enumerate(("right", "left", "pair")):
            wire.go(k, own, blk(moved(OWN, way)), getattr(g, way))

    def ring():
        wire.got(0, blk(LEFT), g.left)
        send(3, LEFT, "right", 0)
        wire.got(1, blk(RIGHT), g.right)
        send(4, RIGHT, "left", 1)
        seen(LEFT)
        seen(RIGHT)

    def twin():
        wire.got(2, blk(TWIN), g.pair)
        send(5, TWIN, "right")
        send(6, TWIN, "left")
        seen(TWIN)

    def across():
        wire.got(3, half(FAR, 0), g.left)
        wire.got(4, half(FAR, 1), g.right)
        send(7, FAR, "pair")
        seen(FAR)

    def last():
        wire.got(5, blk(TWIN_LEFT), g.left)
        wire.got(6, blk(TWIN_RIGHT), g.right)
        seen(TWIN_LEFT)
        seen(TWIN_RIGHT)

    def far():
        wire.got(7, blk(TWIN_FAR), g.pair)
        seen(TWIN_FAR)

    return [start, ring, twin, across, last, far]


def direct_stages(wire, g, blk):
    def send():
        for k, key in enumerate(SEEN[1:]):
            wire.go(k, blk(OWN), blk(OWN), g.dev(key))

    def take():
        for k, (twin, step) in enumerate(SEEN[1:]):
            back = (twin, step if step == 2 else -step)
            wire.got(k, blk(back), g.dev(back))

    return [send, take]


def direct_scatter_stages(wire, g, blk, bufs, done):
    def send():
        for k, key in enumerate(SEEN[1:]):
            wire.go(k, blk(key), bufs.at[k], g.dev(key))

    def take():
        for k, (twin, step) in enumerate(SEEN[1:]):
            wire.got(k, bufs.at[k], g.dev((twin, step if step == 2 else -step)))
        done([bufs[k] for k in range(7)])

    return [send, take]


class Scatter:
    def __init__(self, wire, g, blk, half, bufs, finish):
        self.wire, self.g, self.blk, self.half, self.finish = wire, g, blk, half, finish
        whole, part = bufs
        self.rp, self.rr0, self.rr1, self.rf0, self.rf1, self.rf2 = (whole.at[k] for k in range(6))
        rows, cut = whole.shape[1], part.shape[1]
        self.lo, self.hi = pl.ds(0, cut), pl.ds(cut, rows - cut)
        self.rh0, self.rh1 = part.at[0], part.at[1, pl.ds(0, rows - cut)]

    def twins(self):
        self.wire.go(1, self.blk(TWIN_RIGHT), self.rr0, self.g.right)
        self.wire.go(2, self.blk(TWIN_LEFT), self.rr1, self.g.left)

    def opposite(self):
        self.wire.go(0, self.blk(TWIN_FAR), self.rp, self.g.pair)

    def early(self):
        self.wire.go(3, self.half(RIGHT, 1), self.rf0.at[self.hi], self.g.right)
        self.wire.go(4, self.half(LEFT, 0), self.rf1.at[self.lo], self.g.left)

    def across(self):
        self.wire.got(0, self.rp, self.g.pair)
        for h, sl in ((0, self.lo), (1, self.hi)):
            v = self.half(FAR, h)
            v[...] += self.rp[sl]
        self.wire.go(5, self.half(FAR, 0), self.rh0, self.g.right)
        self.wire.go(6, self.half(FAR, 1), self.rh1, self.g.left)

    def twin(self):
        self.wire.got(1, self.rr0, self.g.left)
        self.wire.got(2, self.rr1, self.g.right)
        v = self.blk(TWIN)
        v[...] += self.rr0[...] + self.rr1[...]
        self.wire.go(7, v, self.rf2, self.g.pair)

    def ring(self):
        self.wire.got(5, self.rh0, self.g.left)
        v = self.half(RIGHT, 0)
        v[...] += self.rh0[...]
        self.wire.go(8, v, self.rf0.at[self.lo], self.g.right)
        self.wire.got(6, self.rh1, self.g.right)
        v = self.half(LEFT, 1)
        v[...] += self.rh1[...]
        self.wire.go(9, v, self.rf1.at[self.hi], self.g.left)

    def last(self):
        self.wire.got(3, self.rf0.at[self.hi], self.g.left)
        self.wire.got(4, self.rf1.at[self.lo], self.g.right)
        self.wire.got(7, self.rf2, self.g.pair)
        self.wire.got(8, self.rf0.at[self.lo], self.g.left)
        self.wire.got(9, self.rf1.at[self.hi], self.g.right)
        self.finish(self.rf0, self.rf1, self.rf2)

    def stages(self):
        def start():
            self.opposite()
            self.twins()
            self.early()

        return [start, self.across, self.twin, self.ring, self.last]


def run_both(a, b):
    for fa, fb in zip(a, b):
        fa()
        fb()


PLACE = {key: k for k, key in enumerate((OWN, TWIN, RIGHT, LEFT, TWIN_FAR, FAR, TWIN_RIGHT, TWIN_LEFT))}


def rows_of(ref, size, base=0):
    def at(key):
        return base + PLACE[key] * size

    def blk(key):
        return ref.at[pl.ds(at(key), size)]

    def half(key, h):
        return ref.at[pl.ds(at(key) + h * (size // 2), size // 2)]

    return blk, half


def score_terms(sim, scale, bias, diag):
    z = scale * sim + bias
    if diag is not None:
        z = jnp.where(diag, -z, z)
    e = jnp.exp(-jnp.abs(z))
    w = 1.0 + e
    r = pl.reciprocal(w)
    g = jnp.where(z >= 0.0, r, e * r)
    loss = jnp.maximum(z, 0.0) + jnp.where(e < 1e-4, e * (1.0 - 0.5 * e), jnp.log(w))
    if diag is not None:
        g = jnp.where(diag, -g, g)
    return loss, g


def fold(x):
    x = jnp.sum(x.reshape(x.shape[0] // 8, 8, x.shape[1]), axis=0)
    return sum(x[:, k * 128 : (k + 1) * 128] for k in range(x.shape[1] // 128))


def tile_of(m):
    div, least = (lambda a, b: a // b, min) if isinstance(m, int) else (lax.div, jnp.minimum)
    q = 3 - least(div(m, 7), 1) - least(div(m, 12), 1) - div(m, 15)
    r = m - (16 - (q + 1) * (q + 1))
    down = least(div(r, q + 1), 1)
    return r + down * (q - r), q + down * (r - q - 1 - q)


def main_kernel(
    block, scal, img_own, txt_own, img_x, txt_x, img_raw, txt_raw, sums, pack,
    img, txt, d_img, d_txt, give, taken, sbuf, gbuf,
    ibuf, ihalf, tbuf, thalf,
    ig_s, ig_r, tg_s, tg_r, is_s, is_r, ts_s, ts_r, core_s, core_r, hand_s, hand_r, local, free,
):
    place = Place()
    gi, gt = place.image_group(), place.text_group()
    c = place.c
    partner = place.partner()
    met = greet(place, (RIGHT, LEFT, TWIN))

    half_rows = 8 * block
    img_blk, img_half = rows_of(img, block)
    txt_blk, txt_half = rows_of(txt, block, half_rows)
    other_blk, _ = rows_of(txt, block)
    wi, wt, core = Wire(ig_s, ig_r), Wire(tg_s, tg_r), Wire(core_s, core_r)

    own_i = pltpu.make_async_copy(img_own, img_blk(OWN), local.at[0])
    own_t = pltpu.make_async_copy(txt_own, txt_blk(OWN), local.at[1])
    own_i.start()
    own_t.start()
    own_i.wait()
    own_t.wait()
    met()
    sent = iter(range(8))

    def share(key):
        core.go(next(sent), txt_blk(key), other_blk(key), partner)

    a = gather_stages(wi, gi, img_blk(OWN), img_blk, img_half, True)
    b = gather_stages(wt, gt, txt_blk(OWN), txt_blk, txt_half, True, share)
    a[0]()
    b[0]()
    share(OWN)
    img_f, txt_f = img_x.shape[1] // 2, txt_x.shape[1] // 2
    feats = img_f + txt_f

    def half_of(which, count):
        return pl.ds(pl.multiple_of(which * count, count), count)

    core.go(8, img_x.at[:, half_of(1 - c, img_f)], pack.at[:, pl.ds(feats, img_f)], partner)
    core.go(9, txt_x.at[:, half_of(1 - c, txt_f)], pack.at[:, pl.ds(feats + img_f, txt_f)], partner)
    for ref in (d_img, d_txt, give, sums):
        ref[...] = jnp.zeros_like(ref)
    run_both(a[1:4], b[1:4])
    b[4]()

    def take_texts(first, last):
        for k in range(first, last):
            core.got(k, other_blk(SEEN[k]), partner)

    def gather_rest():
        b[5]()
        a[4]()
        a[5]()

    take_texts(0, 7)

    scale, bias = scal[0], scal[1]
    di_blk, di_half = rows_of(d_img, block)
    dt_blk, dt_half = rows_of(d_txt, block)

    outs = []

    def put(src, first, count, k):
        copy = pltpu.make_async_copy(src, pack.at[:, pl.ds(first, count)], local.at[4 + k])
        copy.start()
        outs.append(copy)

    def du_view(which, k):
        return pack.at[:, pl.ds(2 * feats + (2 * which + k) * img.shape[1], img.shape[1])]

    def finish(mine, raw, k):
        first = k * block
        step = 64

        def done(p, q, r):
            def rows_of_du(n, carry):
                at = pl.ds(pl.multiple_of(n * step, step), step)
                total = mine[at, :] + p[at, :] + (q[at, :] + r[at, :])
                img[pl.ds(pl.multiple_of(first + n * step, step), step), :] = pull_back(raw[at, :], scal[2] * total)
                return carry

            lax.fori_loop(0, block // step, rows_of_du, 0)
            core.go(10 + k, img.at[pl.ds(first, block)], du_view(1, k), partner)
            put(img.at[pl.ds(first, block)], 2 * feats + k * img.shape[1], img.shape[1], k)

        return done

    si, st = Wire(is_s, is_r), Wire(ts_s, ts_r)
    ri = Scatter(si, gi, di_blk, di_half, (ibuf, ihalf), finish(di_blk(OWN), ibuf.at[0], 0))
    rt = Scatter(st, gt, dt_blk, dt_half, (tbuf, thalf), finish(dt_blk(OWN), tbuf.at[0], 1))

    def hand(k):
        return pltpu.make_async_remote_copy(
            src_ref=give.at[pl.ds(k * TILE, TILE)], dst_ref=taken.at[k % 2], send_sem=hand_s.at[k], recv_sem=hand_r.at[k], device_id=partner, device_id_type=MESH
        )

    def give_chunk(k):
        if k < 2:
            pl.semaphore_wait(free, 1)
        hand(k).start()

    def take_chunk(k):
        hand(k).wait_recv()
        v = d_txt.at[pl.ds(k * TILE, TILE)]
        v[...] += taken[k % 2]
        if k >= 2:
            pl.semaphore_signal(free, inc=1, device_id=partner, device_id_type=MESH)

    def rows(chunk, first=0):
        at = first + chunk * TILE
        return pl.ds(at if isinstance(at, int) else pl.multiple_of(at, TILE), TILE)

    def txt_rows(cc, chunk):
        return rows(chunk, cc * half_rows)

    def score(m, cc):
        i, j = tile_of(m)
        sbuf[cc] = lax.dot_general(img[rows(i), :], txt[txt_rows(cc, j), :], (((1,), (1,)), ((), ())), preferred_element_type=F32)

    def part_of_point(cc, at, diag=None):
        sim = sbuf[cc, at]
        loss, g = score_terms(sim, scale, bias, diag)
        sums[0] += fold(loss)
        sums[1] += fold(g * sim)
        sums[2] += fold(g)
        gbuf[cc, at] = g.astype(BF16)

    def point(cc, diag=None):
        if diag is None:
            part_of_point(cc, slice(0, block))
            part_of_point(cc, slice(block, TILE))
        else:
            part_of_point(cc, slice(0, block), diag)
            part_of_point(cc, slice(block, TILE))

    def products(m, cc):
        i, j = tile_of(m)
        gb = gbuf[cc]
        d_img[rows(i), :] += jnp.dot(gb, txt[txt_rows(cc, j), :], preferred_element_type=F32)
        ref = d_txt if cc else give
        ref[rows(j), :] += lax.dot_general(gb, img[rows(i), :], (((0,), (0,)), ((), ())), preferred_element_type=F32)

    events = {
        0: [gather_rest],
        2: [lambda: take_texts(7, 8)],
        3: [lambda: give_chunk(3)],
        4: [lambda: take_chunk(3), rt.twins],
        6: [ri.twins],
        9: [lambda: give_chunk(2)],
        10: [lambda: take_chunk(2), rt.opposite],
        11: [ri.opposite],
        13: [lambda: give_chunk(1)],
        14: [lambda: take_chunk(1), rt.early, ri.early],
    }
    score(0, 0)
    score(0, 1)
    point(0)

    def step(m, carry):
        score(m + 1, 0)
        point(1)
        products(m, 0)
        score(m + 1, 1)
        point(0)
        products(m, 1)
        for at, todo in events.items():
            @pl.when(m == at)
            def _(todo=todo):
                for f in todo:
                    f()

        return carry

    lax.fori_loop(0, 15, step, 0)
    row = lax.broadcasted_iota(jnp.int32, (block, TILE), 0)
    col = lax.broadcasted_iota(jnp.int32, (block, TILE), 1)
    point(1, row == col)
    products(15, 0)
    give_chunk(0)
    products(15, 1)
    rt.across()
    ri.twin()
    ri.across()
    wi.drain()
    wt.drain()
    keep = [pltpu.make_async_copy(x.at[:, half_of(c, n)], img.at[pl.ds((2 + k) * block, block), pl.ds(0, n)], local.at[2 + k]) for k, (x, n) in enumerate(((img_x, img_f), (txt_x, txt_f)))]
    keep += [pltpu.make_async_copy(img_raw, ibuf.at[0], local.at[0]), pltpu.make_async_copy(txt_raw, tbuf.at[0], local.at[1])]
    for copy in keep:
        copy.start()
    take_chunk(0)
    rt.twin()
    for copy in keep:
        copy.wait()
    put(img.at[pl.ds(2 * block, block)], 0, img_f, 2)
    put(img.at[pl.ds(3 * block, block), pl.ds(0, txt_f)], img_f, txt_f, 3)
    rt.ring()
    ri.ring()
    rt.last()
    ri.last()
    for k, first in enumerate((feats, feats + img_f)):
        core.got(8 + k, pack.at[:, pl.ds(first, (img_f, txt_f)[k])], partner)
        core.got(10 + k, du_view(1, k), partner)
    for k in range(4):
        hand(k).wait_send()
    for copy in outs:
        copy.wait()
    for wire in (si, st, core):
        wire.drain()


def main_call(scal, img_emb, txt_emb, img_x, txt_x, img_raw, txt_raw):
    block, dim = img_emb.shape
    vmem = pl.BlockSpec(memory_space=pltpu.VMEM)
    hbm = pl.BlockSpec(memory_space=pl.ANY)
    sem = pltpu.SemaphoreType.DMA
    f = lambda *s: pltpu.VMEM(s, F32)
    return pl.pallas_call(
        functools.partial(main_kernel, block),
        in_specs=[pl.BlockSpec(memory_space=pltpu.SMEM)] + [hbm] * 6,
        out_specs=[vmem, hbm],
        out_shape=[
            jax.ShapeDtypeStruct((3, 8, 128), F32),
            jax.ShapeDtypeStruct((block, img_x.shape[1] + txt_x.shape[1] + 4 * dim), BF16),
        ],
        scratch_shapes=[
            pltpu.VMEM((8 * block, dim), BF16),
            pltpu.VMEM((16 * block, dim), BF16),
            f(8 * block, dim),
            f(8 * block, dim),
            f(8 * block, dim),
            f(2, TILE, dim),
            f(2, TILE, TILE),
            pltpu.VMEM((2, TILE, TILE), BF16),
            f(6, block, dim),
            f(2, block // 2, dim),
            f(6, block, dim),
            f(2, block // 2, dim),
            sem((GATHER_COPIES,)), sem((GATHER_COPIES,)), sem((GATHER_COPIES,)), sem((GATHER_COPIES,)),
            sem((SCATTER_COPIES,)), sem((SCATTER_COPIES,)), sem((SCATTER_COPIES,)), sem((SCATTER_COPIES,)),
            sem((12,)), sem((12,)), sem((4,)), sem((4,)), sem((8,)), pltpu.SemaphoreType.REGULAR,
        ],
        compiler_params=pltpu.CompilerParams(collective_id=0, has_side_effects=True, vmem_limit_bytes=VMEM_LIMIT),
        name="scores",
    )(scal, img_emb, txt_emb, img_x, txt_x, img_raw, txt_raw)


def pull_back(raw, cot):
    inv = lax.rsqrt(jnp.sum(raw * raw, axis=-1, keepdims=True))
    along = jnp.sum(cot * raw, axis=-1, keepdims=True) * (inv * inv)
    return (inv * (cot - raw * along)).astype(BF16)


COLOURS = 4


def sum_kernel(
    pack, sums_in, d_w_img, d_w_txt, sums,
    w, w2, buf1, half1, buf2, small,
    sc_s, sc_r, ga_s, ga_r, out_s, out_r, core_s, core_r, small_s, small_r, local,
):
    place = Place()
    c, partner = place.c, place.partner()
    met = greet(place, SEEN[1:])
    img_f, txt_f, feats = d_w_img.shape[0] // 2, d_w_txt.shape[0] // 2, w.shape[0]
    ni, nt = img_f // 16, txt_f // 16
    rows, wide = ni + nt, w.shape[1] // 2
    tall, lanes = rows // 2, wide // 4

    def outer(lhs, rhs):
        return lax.dot_general(lhs, rhs, (((0,), (0,)), ((), ())), preferred_element_type=F32)

    def weights(to, first, count, size, shift, k):
        lane, dim = 128, w.shape[1]
        for at in range(0, count, lane):
            val = sum(
                outer(pack[:, side * feats + first + at : side * feats + first + at + lane], pack[:, pl.ds(2 * feats + (2 * side + k) * dim + to * wide, wide)])
                for side in range(2)
            )
            for b in range(lane // size):
                top = (at // size + b) * rows + shift
                w[top : top + size, pl.ds(to * wide, wide)] = val[b * size : (b + 1) * size]

    def lane_half(to):
        weights(to, 0, img_f, ni, 0, 0)
        weights(to, img_f, txt_f, nt, ni, 1)

    lane_half(0)
    met()

    small_wire = Wire(small_s, small_r)
    hops = []
    for name in "xyz":
        v = getattr(place, name)
        hops += [place.at(**{name: place.near(v)}), place.at(**{name: place.far(v)})]
    hops.append(partner)
    small[0] = sums_in[...]

    def small_step(n):
        if 0 < n <= len(hops):
            k = n - 1
            small_wire.got(k, small.at[2 * k + 1], hops[k])
            small[2 * n] = small[2 * k] + small[2 * k + 1]
        if n < len(hops):
            small_wire.go(n, small.at[2 * n], small.at[2 * n + 1], hops[n])

    dwire = Pieces(core_s, core_r)
    copies = []

    def sl(first, count):
        return pl.ds(pl.multiple_of(first, count), count)

    def rows_at(first, count):
        return pl.ds(pl.multiple_of(first, 8), count)

    def colour(n):
        order = (place.image_group(), place.text_group())
        g1, g2 = order if n % 2 == 0 else order[::-1]
        group = n % 2 * 8
        base = group * rows
        across = pl.ds(n // 2 * wide, wide)
        mine = base + g1.slot(OWN) * rows
        keep = n % 2 * rows

        def w_blk(key):
            return w.at[sl(base + g1.slot(key) * rows, rows), across]

        def w_half(key, h):
            return w.at[sl(base + g1.slot(key) * rows + h * tall, tall), across]

        def strip(ref, first):
            def at(key):
                slot = g2.slot(key)
                return first + lax.div(slot, 4) * tall, sl(n // 2 * wide + lax.rem(slot, 4) * lanes, lanes)

            def blk(key):
                top, cols = at(key)
                return ref.at[rows_at(top, tall), cols]

            return blk

        def outs(key, core, h, parts):
            at = group + g1.slot(key)
            a, b = ni // parts, nt // parts
            return (
                d_w_img.at[sl(core * img_f + at * ni + h * a, a), across],
                d_w_txt.at[sl(core * txt_f + at * nt + h * b, b), across],
            )

        def o_blk(key, core=c):
            return outs(key, core, 0, 1)

        def o_half(key, h):
            return outs(key, c, h, 2)

        ws_blk = strip(w, mine)
        os_blk = strip(w2, keep)

        def done1(p, q, r):
            v = w_blk(OWN)
            v[...] += p[...] + q[...] + r[...]

        def done2(terms):
            v = os_blk(OWN)
            v[...] = ws_blk(OWN)[...] + sum(terms)

        whole = w2.at[pl.ds(keep, ni), across], w2.at[pl.ds(keep + ni, nt), across]
        turn = iter(range(n * 8, n * 8 + 8))

        def share(key, src=None):
            dwire.go(next(turn), o_blk(key) if src is None else src, o_blk(key), partner)

        def share_own():
            share(OWN, whole)
            for p, (src, dst) in enumerate(zip(whole, o_blk(OWN))):
                copy = pltpu.make_async_copy(src, dst, local.at[2 * n + p])
                copy.start()
                copies.append(copy)

        def got_shares():
            for k, key in enumerate(SEEN):
                dwire.got(n * 8 + k, o_blk(key, 1 - c), partner)

        w1, w2_, w3 = (Wire(*args) for args in ((sc_s, sc_r, n * SCATTER_COPIES), (sc_s, sc_r, (COLOURS + n) * SCATTER_COPIES), (ga_s, ga_r, n * GATHER_COPIES)))
        w4 = Pieces(out_s, out_r, 2 * n * GATHER_COPIES)
        stages = Scatter(w1, g1, w_blk, w_half, (buf1.at[n], half1.at[n]), done1).stages()
        stages += direct_scatter_stages(w2_, g2, ws_blk, buf2.at[n], done2)
        stages += direct_stages(w3, g2, os_blk)
        tail = gather_stages(w4, g1, whole, o_blk, o_half, False, share)
        stages += [tail[0], share_own] + tail[1:] + [got_shares]
        return stages, [w1, w2_, w3, w4]

    colours = [colour(n) for n in range(COLOURS)]
    for n in range(len(colours[0][0]) + 1):
        for k, (stages, _) in enumerate(colours):
            at = n - k // 2 * 1
            if 0 <= at < len(stages):
                stages[at]()
        if n == 0:
            lane_half(1)
        small_step(n)
    sums[...] = small[2 * len(hops)]
    for copy in copies:
        copy.wait()
    for _, wires in colours:
        for wire in wires:
            wire.drain()
    dwire.drain()
    small_wire.drain()


def sum_call(pack, sums, img_x, txt_x, dim):
    feats = (img_x.shape[1] + txt_x.shape[1]) // 2
    vmem = pl.BlockSpec(memory_space=pltpu.VMEM)
    hbm = pl.BlockSpec(memory_space=pl.ANY)
    sem = lambda n: [pltpu.SemaphoreType.DMA((n,))] * 2
    f = lambda *s: pltpu.VMEM(s, F32)
    rows, wide = feats // 16, dim // 2
    tall, lanes = rows // 2, wide // 4
    return pl.pallas_call(
        sum_kernel,
        in_specs=[vmem, vmem],
        out_specs=[hbm, hbm, vmem],
        out_shape=[
            jax.ShapeDtypeStruct((img_x.shape[1], dim), F32),
            jax.ShapeDtypeStruct((txt_x.shape[1], dim), F32),
            jax.ShapeDtypeStruct(sums.shape, F32),
        ],
        scratch_shapes=[
            f(feats, dim),
            f(2 * rows, dim),
            f(COLOURS, 6, rows, wide), f(COLOURS, 2, tall, wide),
            f(COLOURS, 7, tall, lanes),
            f(15, *sums.shape),
            *sem(2 * COLOURS * SCATTER_COPIES), *sem(COLOURS * GATHER_COPIES), *sem(2 * COLOURS * GATHER_COPIES),
            *sem(2 * COLOURS * 8), *sem(7), pltpu.SemaphoreType.DMA((2 * COLOURS,)),
        ],
        compiler_params=pltpu.CompilerParams(collective_id=1, has_side_effects=True, vmem_limit_bytes=32 * 2**20),
        name="weights",
    )(pack, sums)


def store_kernel(total_rows, scal, sums, src_a, src_b, loss, d_temp, d_bias, dst_a, dst_b, sems):
    copies = [pltpu.make_async_copy(src_a, dst_a, sems.at[0]), pltpu.make_async_copy(src_b, dst_b, sems.at[1])]
    for copy in copies:
        copy.start()
    loss[0] = jnp.sum(sums[0]) / total_rows
    d_temp[0] = scal[0] * (jnp.sum(sums[1]) / total_rows)
    d_bias[0] = jnp.sum(sums[2]) / total_rows
    for copy in copies:
        copy.wait()


def store_call(total_rows, scal, sums, *arrays):
    hbm = pl.BlockSpec(memory_space=pl.ANY)
    smem = pl.BlockSpec(memory_space=pltpu.SMEM)
    one = jax.ShapeDtypeStruct((1,), F32)
    return pl.pallas_call(
        functools.partial(store_kernel, total_rows),
        in_specs=[smem, pl.BlockSpec(memory_space=pltpu.VMEM), hbm, hbm],
        out_specs=[smem] * 3 + [pl.BlockSpec(memory_space=pltpu.HBM)] * 2,
        out_shape=[one] * 3 + [jax.ShapeDtypeStruct(a.shape, a.dtype) for a in arrays],
        scratch_shapes=[pltpu.SemaphoreType.DMA((2,))],
        compiler_params=pltpu.CompilerParams(vmem_limit_bytes=2**20),
        name="store",
    )(scal, sums, *arrays)


def solution(mesh):
    dev_count = mesh.shape["replica"] * mesh.shape["data"]
    batch_axes = ("replica", "data")

    def local_fn(img_x, txt_x, w_img, w_txt, log_temp, logit_bias):
        block = img_x.shape[0]
        total_rows = block * dev_count
        txt_raw, txt_emb = embed_rows(txt_x, w_txt)
        img_raw, img_emb = embed_rows(img_x, w_img)
        temp_scale = jnp.exp(log_temp[0])
        scal = jnp.stack([temp_scale, logit_bias[0], temp_scale / total_rows])
        sums, pack = main_call(scal, img_emb, txt_emb, img_x, txt_x, img_raw, txt_raw)
        d_w_img, d_w_txt, sums = sum_call(pack, sums, img_x, txt_x, w_img.shape[1])
        return tuple(store_call(total_rows, scal, sums, d_w_img, d_w_txt))

    batch_spec = P(batch_axes, None)
    return jax.shard_map(local_fn, mesh=mesh, in_specs=(batch_spec, batch_spec, P(), P(), P(), P()), out_specs=(P(), P(), P(), P(), P()), check_vma=False)
```

```python
import functools

import jax
import jax.numpy as jnp
from jax import lax
from jax.experimental import pallas as pl
from jax.experimental.pallas import tpu as pltpu
from jax.sharding import PartitionSpec as P

F32 = jnp.float32
BF16 = jnp.bfloat16
TILE = 512
MESH = pl.DeviceIdType.MESH
VMEM_LIMIT = 67043328


def embed_rows(feat_x, w_proj):
    raw = jnp.dot(feat_x, w_proj, preferred_element_type=F32)
    return raw, (raw * lax.rsqrt(jnp.sum(raw * raw, axis=-1, keepdims=True))).astype(BF16)


OWN, RIGHT, LEFT, FAR = ((0, step) for step in (0, 1, -1, 2))
TWIN, TWIN_RIGHT, TWIN_LEFT, TWIN_FAR = ((1, step) for step in (0, 1, -1, 2))
SEEN = [OWN, LEFT, RIGHT, TWIN, FAR, TWIN_LEFT, TWIN_RIGHT, TWIN_FAR]


class Place:
    def __init__(self):
        rep, dat = lax.axis_index("replica"), lax.axis_index("data")
        self.z, self.y = lax.div(rep, 4), lax.rem(rep, 4)
        self.x, self.c = lax.div(dat, 2), lax.rem(dat, 2)

    def at(self, x=None, y=None, z=None, c=None):
        x = self.x if x is None else lax.rem(x + 8, 4)
        y = self.y if y is None else lax.rem(y + 8, 4)
        z = self.z if z is None else lax.rem(z + 8, 4)
        c = self.c if c is None else c
        return (z * 4 + y, x * 2 + c)

    def partner(self):
        return self.at(c=1 - self.c)

    def near(self, v):
        return v + 1 - 2 * lax.rem(v, 2)

    def far(self, v):
        return v - 1 + 2 * lax.rem(v, 2)

    def image_group(self):
        return Group(self.x, lax.rem(lax.div(self.y + 1, 2), 2), lambda key: self.at(x=self.x + key[1], y=self.near(self.y) if key[0] else None))

    def text_group(self):
        return Group(self.z, lax.div(self.y, 2), lambda key: self.at(z=self.z + key[1], y=self.far(self.y) if key[0] else None))

    def peers(self, keys):
        return [self.partner()] + [g.dev(key) for g in (self.image_group(), self.text_group()) for key in keys]


class Group:
    def __init__(self, pos, side, dev):
        self.pos, self.side, self.dev = pos, side, dev
        self.right, self.left, self.pair = (dev(key) for key in (RIGHT, LEFT, TWIN))

    def slot(self, key):
        side = 1 - self.side if key[0] else self.side
        return side * 4 + lax.rem(self.pos + key[1] + 4, 4)


def greet(place, keys):
    barrier = pltpu.get_barrier_semaphore()
    peers = place.peers(keys)
    for dev in peers:
        pl.semaphore_signal(barrier, inc=1, device_id=dev, device_id_type=MESH)
    return lambda: pl.semaphore_wait(barrier, len(peers))


class Wire:
    def __init__(self, send, recv, first=0):
        self.send, self.recv, self.first, self.open = send, recv, first, []

    def copy(self, k, src, dst, dev):
        k += self.first
        return pltpu.make_async_remote_copy(src_ref=src, dst_ref=dst, send_sem=self.send.at[k], recv_sem=self.recv.at[k], device_id=dev, device_id_type=MESH)

    def go(self, *what):
        self.copy(*what).start()
        self.open.append(what)

    def got(self, k, dst, dev):
        self.copy(k, dst, dst, dev).wait_recv()

    def drain(self):
        for what in self.open:
            self.copy(*what).wait_send()
        self.open = []


class Pieces:
    def __init__(self, *where):
        self.wire = Wire(*where)

    def go(self, k, src, dst, dev):
        for p in range(2):
            self.wire.go(2 * k + p, src[p], dst[p], dev)

    def got(self, k, dst, dev):
        for p in range(2):
            self.wire.got(2 * k + p, dst[p], dev)

    def drain(self):
        self.wire.drain()


GATHER_COPIES = 8
SCATTER_COPIES = 10


def gather_stages(wire, g, own, blk, half, relative, seen=None):
    seen = seen or (lambda key: None)

    def moved(key, way):
        twin, step = key
        if not relative:
            return key
        twin, step = {"right": (twin, step - 1), "left": (twin, step + 1), "pair": (1 - twin, step)}[way]
        return twin, (step + 1) % 4 - 1

    def send(k, key, way, h=None):
        dev = getattr(g, way)
        view = blk if h is None else functools.partial(half, h=h)
        wire.go(k, view(key), view(moved(key, way)), dev)

    def start():
        for k, way in enumerate(("right", "left", "pair")):
            wire.go(k, own, blk(moved(OWN, way)), getattr(g, way))

    def ring():
        wire.got(0, blk(LEFT), g.left)
        send(3, LEFT, "right", 0)
        wire.got(1, blk(RIGHT), g.right)
        send(4, RIGHT, "left", 1)
        seen(LEFT)
        seen(RIGHT)

    def twin():
        wire.got(2, blk(TWIN), g.pair)
        send(5, TWIN, "right")
        send(6, TWIN, "left")
        seen(TWIN)

    def across():
        wire.got(3, half(FAR, 0), g.left)
        wire.got(4, half(FAR, 1), g.right)
        send(7, FAR, "pair")
        seen(FAR)

    def last():
        wire.got(5, blk(TWIN_LEFT), g.left)
        wire.got(6, blk(TWIN_RIGHT), g.right)
        seen(TWIN_LEFT)
        seen(TWIN_RIGHT)

    def far():
        wire.got(7, blk(TWIN_FAR), g.pair)
        seen(TWIN_FAR)

    return [start, ring, twin, across, last, far]


def direct_stages(wire, g, blk):
    def send():
        for k, key in enumerate(SEEN[1:]):
            wire.go(k, blk(OWN), blk(OWN), g.dev(key))

    def take():
        for k, (twin, step) in enumerate(SEEN[1:]):
            back = (twin, step if step == 2 else -step)
            wire.got(k, blk(back), g.dev(back))

    return [send, take]


def direct_scatter_stages(wire, g, blk, bufs, done):
    def send():
        for k, key in enumerate(SEEN[1:]):
            wire.go(k, blk(key), bufs.at[k], g.dev(key))

    def take():
        for k, (twin, step) in enumerate(SEEN[1:]):
            wire.got(k, bufs.at[k], g.dev((twin, step if step == 2 else -step)))
        done([bufs[k] for k in range(7)])

    return [send, take]


class Scatter:
    def __init__(self, wire, g, blk, half, bufs, finish):
        self.wire, self.g, self.blk, self.half, self.finish = wire, g, blk, half, finish
        whole, part = bufs
        self.rp, self.rr0, self.rr1, self.rf0, self.rf1, self.rf2 = (whole.at[k] for k in range(6))
        rows, cut = whole.shape[1], part.shape[1]
        self.lo, self.hi = pl.ds(0, cut), pl.ds(cut, rows - cut)
        self.rh0, self.rh1 = part.at[0], part.at[1, pl.ds(0, rows - cut)]

    def twins(self):
        self.wire.go(1, self.blk(TWIN_RIGHT), self.rr0, self.g.right)
        self.wire.go(2, self.blk(TWIN_LEFT), self.rr1, self.g.left)

    def opposite(self):
        self.wire.go(0, self.blk(TWIN_FAR), self.rp, self.g.pair)

    def early(self):
        self.wire.go(3, self.half(RIGHT, 1), self.rf0.at[self.hi], self.g.right)
        self.wire.go(4, self.half(LEFT, 0), self.rf1.at[self.lo], self.g.left)

    def across(self):
        self.wire.got(0, self.rp, self.g.pair)
        for h, sl in ((0, self.lo), (1, self.hi)):
            v = self.half(FAR, h)
            v[...] += self.rp[sl]
        self.wire.go(5, self.half(FAR, 0), self.rh0, self.g.right)
        self.wire.go(6, self.half(FAR, 1), self.rh1, self.g.left)

    def twin(self):
        self.wire.got(1, self.rr0, self.g.left)
        self.wire.got(2, self.rr1, self.g.right)
        v = self.blk(TWIN)
        v[...] += self.rr0[...] + self.rr1[...]
        self.wire.go(7, v, self.rf2, self.g.pair)

    def ring(self):
        self.wire.got(5, self.rh0, self.g.left)
        v = self.half(RIGHT, 0)
        v[...] += self.rh0[...]
        self.wire.go(8, v, self.rf0.at[self.lo], self.g.right)
        self.wire.got(6, self.rh1, self.g.right)
        v = self.half(LEFT, 1)
        v[...] += self.rh1[...]
        self.wire.go(9, v, self.rf1.at[self.hi], self.g.left)

    def last(self):
        self.wire.got(3, self.rf0.at[self.hi], self.g.left)
        self.wire.got(4, self.rf1.at[self.lo], self.g.right)
        self.wire.got(7, self.rf2, self.g.pair)
        self.wire.got(8, self.rf0.at[self.lo], self.g.left)
        self.wire.got(9, self.rf1.at[self.hi], self.g.right)
        self.finish(self.rf0, self.rf1, self.rf2)

    def stages(self):
        def start():
            self.opposite()
            self.twins()
            self.early()

        return [start, self.across, self.twin, self.ring, self.last]


def run_both(a, b):
    for fa, fb in zip(a, b):
        fa()
        fb()


PLACE = {key: k for k, key in enumerate((OWN, TWIN, RIGHT, LEFT, TWIN_FAR, FAR, TWIN_RIGHT, TWIN_LEFT))}


def rows_of(ref, size, base=0):
    def at(key):
        return base + PLACE[key] * size

    def blk(key):
        return ref.at[pl.ds(at(key), size)]

    def half(key, h):
        return ref.at[pl.ds(at(key) + h * (size // 2), size // 2)]

    return blk, half


def score_terms(sim, scale, bias, diag):
    z = scale * sim + bias
    if diag is not None:
        z = jnp.where(diag, -z, z)
    e = jnp.exp(-jnp.abs(z))
    w = 1.0 + e
    r = pl.reciprocal(w)
    g = jnp.where(z >= 0.0, r, e * r)
    loss = jnp.maximum(z, 0.0) + jnp.where(e < 1e-4, e * (1.0 - 0.5 * e), jnp.log(w))
    if diag is not None:
        g = jnp.where(diag, -g, g)
    return loss, g


def fold(x):
    x = jnp.sum(x.reshape(x.shape[0] // 8, 8, x.shape[1]), axis=0)
    return sum(x[:, k * 128 : (k + 1) * 128] for k in range(x.shape[1] // 128))


def tile_of(m):
    div, least = (lambda a, b: a // b, min) if isinstance(m, int) else (lax.div, jnp.minimum)
    q = 3 - least(div(m, 7), 1) - least(div(m, 12), 1) - div(m, 15)
    r = m - (16 - (q + 1) * (q + 1))
    down = least(div(r, q + 1), 1)
    return r + down * (q - r), q + down * (r - q - 1 - q)


def main_kernel(
    block, scal, img_own, txt_own, img_x, txt_x, img_raw, txt_raw, sums, pack,
    img, txt, d_img, d_txt, give, taken, sbuf, gbuf,
    ibuf, ihalf, tbuf, thalf,
    ig_s, ig_r, tg_s, tg_r, is_s, is_r, ts_s, ts_r, core_s, core_r, hand_s, hand_r, local, free,
):
    place = Place()
    gi, gt = place.image_group(), place.text_group()
    c = place.c
    partner = place.partner()
    met = greet(place, (RIGHT, LEFT, TWIN))

    half_rows = 8 * block
    img_blk, img_half = rows_of(img, block)
    txt_blk, txt_half = rows_of(txt, block, half_rows)
    other_blk, _ = rows_of(txt, block)
    wi, wt, core = Wire(ig_s, ig_r), Wire(tg_s, tg_r), Wire(core_s, core_r)

    own_i = pltpu.make_async_copy(img_own, img_blk(OWN), local.at[0])
    own_t = pltpu.make_async_copy(txt_own, txt_blk(OWN), local.at[1])
    own_i.start()
    own_t.start()
    own_i.wait()
    own_t.wait()
    met()
    sent = iter(range(8))

    def share(key):
        core.go(next(sent), txt_blk(key), other_blk(key), partner)

    a = gather_stages(wi, gi, img_blk(OWN), img_blk, img_half, True)
    b = gather_stages(wt, gt, txt_blk(OWN), txt_blk, txt_half, True, share)
    a[0]()
    b[0]()
    share(OWN)
    img_f, txt_f = img_x.shape[1] // 2, txt_x.shape[1] // 2
    feats = img_f + txt_f

    def half_of(which, count):
        return pl.ds(pl.multiple_of(which * count, count), count)

    core.go(8, img_x.at[:, half_of(1 - c, img_f)], pack.at[:, pl.ds(feats, img_f)], partner)
    core.go(9, txt_x.at[:, half_of(1 - c, txt_f)], pack.at[:, pl.ds(feats + img_f, txt_f)], partner)
    for ref in (d_img, d_txt, give, sums):
        ref[...] = jnp.zeros_like(ref)
    run_both(a[1:4], b[1:4])
    b[4]()

    def take_texts(first, last):
        for k in range(first, last):
            core.got(k, other_blk(SEEN[k]), partner)

    def gather_rest():
        b[5]()
        a[4]()
        a[5]()

    take_texts(0, 7)

    scale, bias = scal[0], scal[1]
    di_blk, di_half = rows_of(d_img, block)
    dt_blk, dt_half = rows_of(d_txt, block)

    outs = []

    def put(src, first, count, k):
        copy = pltpu.make_async_copy(src, pack.at[:, pl.ds(first, count)], local.at[4 + k])
        copy.start()
        outs.append(copy)

    def du_view(which, k):
        return pack.at[:, pl.ds(2 * feats + (2 * which + k) * img.shape[1], img.shape[1])]

    def finish(mine, raw, k):
        first = k * block
        step = 64

        def done(p, q, r):
            def rows_of_du(n, carry):
                at = pl.ds(pl.multiple_of(n * step, step), step)
                total = mine[at, :] + p[at, :] + (q[at, :] + r[at, :])
                img[pl.ds(pl.multiple_of(first + n * step, step), step), :] = pull_back(raw[at, :], scal[2] * total)
                return carry

            lax.fori_loop(0, block // step, rows_of_du, 0)
            core.go(10 + k, img.at[pl.ds(first, block)], du_view(1, k), partner)
            put(img.at[pl.ds(first, block)], 2 * feats + k * img.shape[1], img.shape[1], k)

        return done

    si, st = Wire(is_s, is_r), Wire(ts_s, ts_r)
    ri = Scatter(si, gi, di_blk, di_half, (ibuf, ihalf), finish(di_blk(OWN), ibuf.at[0], 0))
    rt = Scatter(st, gt, dt_blk, dt_half, (tbuf, thalf), finish(dt_blk(OWN), tbuf.at[0], 1))

    def hand(k):
        return pltpu.make_async_remote_copy(
            src_ref=give.at[pl.ds(k * TILE, TILE)], dst_ref=taken.at[k % 2], send_sem=hand_s.at[k], recv_sem=hand_r.at[k], device_id=partner, device_id_type=MESH
        )

    def give_chunk(k):
        if k < 2:
            pl.semaphore_wait(free, 1)
        hand(k).start()

    def take_chunk(k):
        hand(k).wait_recv()
        v = d_txt.at[pl.ds(k * TILE, TILE)]
        v[...] += taken[k % 2]
        if k >= 2:
            pl.semaphore_signal(free, inc=1, device_id=partner, device_id_type=MESH)

    def rows(chunk, first=0):
        at = first + chunk * TILE
        return pl.ds(at if isinstance(at, int) else pl.multiple_of(at, TILE), TILE)

    def txt_rows(cc, chunk):
        return rows(chunk, cc * half_rows)

    def score(m, cc):
        i, j = tile_of(m)
        sbuf[cc] = lax.dot_general(img[rows(i), :], txt[txt_rows(cc, j), :], (((1,), (1,)), ((), ())), preferred_element_type=F32)

    def part_of_point(cc, at, diag=None):
        sim = sbuf[cc, at]
        loss, g = score_terms(sim, scale, bias, diag)
        sums[0] += fold(loss)
        sums[1] += fold(g * sim)
        sums[2] += fold(g)
        gbuf[cc, at] = g.astype(BF16)

    def point(cc, diag=None):
        if diag is None:
            part_of_point(cc, slice(0, block))
            part_of_point(cc, slice(block, TILE))
        else:
            part_of_point(cc, slice(0, block), diag)
            part_of_point(cc, slice(block, TILE))

    def products(m, cc):
        i, j = tile_of(m)
        gb = gbuf[cc]
        d_img[rows(i), :] += jnp.dot(gb, txt[txt_rows(cc, j), :], preferred_element_type=F32)
        ref = d_txt if cc else give
        ref[rows(j), :] += lax.dot_general(gb, img[rows(i), :], (((0,), (0,)), ((), ())), preferred_element_type=F32)

    events = {
        0: [gather_rest],
        2: [lambda: take_texts(7, 8)],
        3: [lambda: give_chunk(3)],
        4: [lambda: take_chunk(3), rt.twins],
        6: [ri.twins],
        9: [lambda: give_chunk(2)],
        10: [lambda: take_chunk(2), rt.opposite],
        11: [ri.opposite],
        13: [lambda: give_chunk(1)],
        14: [ri.early, lambda: take_chunk(1), rt.early],
    }
    score(0, 0)
    score(0, 1)
    point(0)

    def step(m, carry):
        score(m + 1, 0)
        point(1)
        products(m, 0)
        score(m + 1, 1)
        point(0)
        products(m, 1)
        for at, todo in events.items():
            @pl.when(m == at)
            def _(todo=todo):
                for f in todo:
                    f()

        return carry

    lax.fori_loop(0, 15, step, 0)
    row = lax.broadcasted_iota(jnp.int32, (block, TILE), 0)
    col = lax.broadcasted_iota(jnp.int32, (block, TILE), 1)
    point(1, row == col)
    products(15, 0)
    give_chunk(0)
    products(15, 1)
    rt.across()
    ri.twin()
    ri.across()
    wi.drain()
    wt.drain()
    keep = [pltpu.make_async_copy(x.at[:, half_of(c, n)], img.at[pl.ds((2 + k) * block, block), pl.ds(0, n)], local.at[2 + k]) for k, (x, n) in enumerate(((img_x, img_f), (txt_x, txt_f)))]
    keep += [pltpu.make_async_copy(img_raw, ibuf.at[0], local.at[0]), pltpu.make_async_copy(txt_raw, tbuf.at[0], local.at[1])]
    for copy in keep:
        copy.start()
    take_chunk(0)
    rt.twin()
    for copy in keep:
        copy.wait()
    put(img.at[pl.ds(2 * block, block)], 0, img_f, 2)
    put(img.at[pl.ds(3 * block, block), pl.ds(0, txt_f)], img_f, txt_f, 3)
    rt.ring()
    ri.ring()
    rt.last()
    ri.last()
    for k, first in enumerate((feats, feats + img_f)):
        core.got(8 + k, pack.at[:, pl.ds(first, (img_f, txt_f)[k])], partner)
        core.got(10 + k, du_view(1, k), partner)
    for k in range(4):
        hand(k).wait_send()
    for copy in outs:
        copy.wait()
    for wire in (si, st, core):
        wire.drain()


def main_call(scal, img_emb, txt_emb, img_x, txt_x, img_raw, txt_raw):
    block, dim = img_emb.shape
    vmem = pl.BlockSpec(memory_space=pltpu.VMEM)
    hbm = pl.BlockSpec(memory_space=pl.ANY)
    sem = pltpu.SemaphoreType.DMA
    f = lambda *s: pltpu.VMEM(s, F32)
    return pl.pallas_call(
        functools.partial(main_kernel, block),
        in_specs=[pl.BlockSpec(memory_space=pltpu.SMEM)] + [hbm] * 6,
        out_specs=[vmem, hbm],
        out_shape=[
            jax.ShapeDtypeStruct((3, 8, 128), F32),
            jax.ShapeDtypeStruct((block, img_x.shape[1] + txt_x.shape[1] + 4 * dim), BF16),
        ],
        scratch_shapes=[
            pltpu.VMEM((8 * block, dim), BF16),
            pltpu.VMEM((16 * block, dim), BF16),
            f(8 * block, dim),
            f(8 * block, dim),
            f(8 * block, dim),
            f(2, TILE, dim),
            f(2, TILE, TILE),
            pltpu.VMEM((2, TILE, TILE), BF16),
            f(6, block, dim),
            f(2, block // 2, dim),
            f(6, block, dim),
            f(2, block // 2, dim),
            sem((GATHER_COPIES,)), sem((GATHER_COPIES,)), sem((GATHER_COPIES,)), sem((GATHER_COPIES,)),
            sem((SCATTER_COPIES,)), sem((SCATTER_COPIES,)), sem((SCATTER_COPIES,)), sem((SCATTER_COPIES,)),
            sem((12,)), sem((12,)), sem((4,)), sem((4,)), sem((8,)), pltpu.SemaphoreType.REGULAR,
        ],
        compiler_params=pltpu.CompilerParams(collective_id=0, has_side_effects=True, vmem_limit_bytes=VMEM_LIMIT),
        name="scores",
    )(scal, img_emb, txt_emb, img_x, txt_x, img_raw, txt_raw)


def pull_back(raw, cot):
    inv = lax.rsqrt(jnp.sum(raw * raw, axis=-1, keepdims=True))
    along = jnp.sum(cot * raw, axis=-1, keepdims=True) * (inv * inv)
    return (inv * (cot - raw * along)).astype(BF16)


COLOURS = 4


def sum_kernel(
    pack, sums_in, d_w_img, d_w_txt, sums,
    w, w2, buf1, half1, buf2, small,
    sc_s, sc_r, ga_s, ga_r, out_s, out_r, core_s, core_r, small_s, small_r, local,
):
    place = Place()
    c, partner = place.c, place.partner()
    met = greet(place, SEEN[1:])
    img_f, txt_f, feats = d_w_img.shape[0] // 2, d_w_txt.shape[0] // 2, w.shape[0]
    ni, nt = img_f // 16, txt_f // 16
    rows, wide = ni + nt, w.shape[1] // 2
    tall, lanes = rows // 2, wide // 4

    def outer(lhs, rhs):
        return lax.dot_general(lhs, rhs, (((0,), (0,)), ((), ())), preferred_element_type=F32)

    def weights(to, first, count, size, shift, k):
        lane, dim = 128, w.shape[1]
        for at in range(0, count, lane):
            val = sum(
                outer(pack[:, side * feats + first + at : side * feats + first + at + lane], pack[:, pl.ds(2 * feats + (2 * side + k) * dim + to * wide, wide)])
                for side in range(2)
            )
            for b in range(lane // size):
                top = (at // size + b) * rows + shift
                w[top : top + size, pl.ds(to * wide, wide)] = val[b * size : (b + 1) * size]

    def lane_half(to):
        weights(to, 0, img_f, ni, 0, 0)
        weights(to, img_f, txt_f, nt, ni, 1)

    lane_half(0)
    met()

    small_wire = Wire(small_s, small_r)
    hops = []
    for name in "xyz":
        v = getattr(place, name)
        hops += [place.at(**{name: place.near(v)}), place.at(**{name: place.far(v)})]
    hops.append(partner)
    small[0] = sums_in[...]

    def small_step(n):
        if 0 < n <= len(hops):
            k = n - 1
            small_wire.got(k, small.at[2 * k + 1], hops[k])
            small[2 * n] = small[2 * k] + small[2 * k + 1]
        if n < len(hops):
            small_wire.go(n, small.at[2 * n], small.at[2 * n + 1], hops[n])

    dwire = Pieces(core_s, core_r)
    copies = []

    def sl(first, count):
        return pl.ds(pl.multiple_of(first, count), count)

    def rows_at(first, count):
        return pl.ds(pl.multiple_of(first, 8), count)

    def colour(n):
        order = (place.image_group(), place.text_group())
        g1, g2 = order if n % 2 == 0 else order[::-1]
        group = n % 2 * 8
        base = group * rows
        across = pl.ds(n // 2 * wide, wide)
        mine = base + g1.slot(OWN) * rows
        keep = n % 2 * rows

        def w_blk(key):
            return w.at[sl(base + g1.slot(key) * rows, rows), across]

        def w_half(key, h):
            return w.at[sl(base + g1.slot(key) * rows + h * tall, tall), across]

        def strip(ref, first):
            def at(key):
                slot = g2.slot(key)
                return first + lax.div(slot, 4) * tall, sl(n // 2 * wide + lax.rem(slot, 4) * lanes, lanes)

            def blk(key):
                top, cols = at(key)
                return ref.at[rows_at(top, tall), cols]

            return blk

        def outs(key, core, h, parts):
            at = group + g1.slot(key)
            a, b = ni // parts, nt // parts
            return (
                d_w_img.at[sl(core * img_f + at * ni + h * a, a), across],
                d_w_txt.at[sl(core * txt_f + at * nt + h * b, b), across],
            )

        def o_blk(key, core=c):
            return outs(key, core, 0, 1)

        def o_half(key, h):
            return outs(key, c, h, 2)

        ws_blk = strip(w, mine)
        os_blk = strip(w2, keep)

        def done1(p, q, r):
            v = w_blk(OWN)
            v[...] += p[...] + q[...] + r[...]

        def done2(terms):
            v = os_blk(OWN)
            v[...] = ws_blk(OWN)[...] + sum(terms)

        whole = w2.at[pl.ds(keep, ni), across], w2.at[pl.ds(keep + ni, nt), across]
        turn = iter(range(n * 8, n * 8 + 8))

        def share(key, src=None):
            dwire.go(next(turn), o_blk(key) if src is None else src, o_blk(key), partner)

        def share_own():
            share(OWN, whole)
            for p, (src, dst) in enumerate(zip(whole, o_blk(OWN))):
                copy = pltpu.make_async_copy(src, dst, local.at[2 * n + p])
                copy.start()
                copies.append(copy)

        def got_shares():
            for k, key in enumerate(SEEN):
                dwire.got(n * 8 + k, o_blk(key, 1 - c), partner)

        w1, w2_, w3 = (Wire(*args) for args in ((sc_s, sc_r, n * SCATTER_COPIES), (sc_s, sc_r, (COLOURS + n) * SCATTER_COPIES), (ga_s, ga_r, n * GATHER_COPIES)))
        w4 = Pieces(out_s, out_r, 2 * n * GATHER_COPIES)
        stages = Scatter(w1, g1, w_blk, w_half, (buf1.at[n], half1.at[n]), done1).stages()
        stages += direct_scatter_stages(w2_, g2, ws_blk, buf2.at[n], done2)
        stages += direct_stages(w3, g2, os_blk)
        tail = gather_stages(w4, g1, whole, o_blk, o_half, False, share)
        stages += [tail[0], share_own] + tail[1:] + [got_shares]
        return stages, [w1, w2_, w3, w4]

    colours = [colour(n) for n in range(COLOURS)]
    for n in range(len(colours[0][0]) + 1):
        for k, (stages, _) in enumerate(colours):
            at = n - k // 2 * 1
            if 0 <= at < len(stages):
                stages[at]()
        if n == 0:
            lane_half(1)
        small_step(n)
    sums[...] = small[2 * len(hops)]
    for copy in copies:
        copy.wait()
    for _, wires in colours:
        for wire in wires:
            wire.drain()
    dwire.drain()
    small_wire.drain()


def sum_call(pack, sums, img_x, txt_x, dim):
    feats = (img_x.shape[1] + txt_x.shape[1]) // 2
    vmem = pl.BlockSpec(memory_space=pltpu.VMEM)
    hbm = pl.BlockSpec(memory_space=pl.ANY)
    sem = lambda n: [pltpu.SemaphoreType.DMA((n,))] * 2
    f = lambda *s: pltpu.VMEM(s, F32)
    rows, wide = feats // 16, dim // 2
    tall, lanes = rows // 2, wide // 4
    return pl.pallas_call(
        sum_kernel,
        in_specs=[vmem, vmem],
        out_specs=[hbm, hbm, vmem],
        out_shape=[
            jax.ShapeDtypeStruct((img_x.shape[1], dim), F32),
            jax.ShapeDtypeStruct((txt_x.shape[1], dim), F32),
            jax.ShapeDtypeStruct(sums.shape, F32),
        ],
        scratch_shapes=[
            f(feats, dim),
            f(2 * rows, dim),
            f(COLOURS, 6, rows, wide), f(COLOURS, 2, tall, wide),
            f(COLOURS, 7, tall, lanes),
            f(15, *sums.shape),
            *sem(2 * COLOURS * SCATTER_COPIES), *sem(COLOURS * GATHER_COPIES), *sem(2 * COLOURS * GATHER_COPIES),
            *sem(2 * COLOURS * 8), *sem(7), pltpu.SemaphoreType.DMA((2 * COLOURS,)),
        ],
        compiler_params=pltpu.CompilerParams(collective_id=1, has_side_effects=True, vmem_limit_bytes=32 * 2**20),
        name="weights",
    )(pack, sums)


def store_kernel(total_rows, scal, sums, src_a, src_b, loss, d_temp, d_bias, dst_a, dst_b, sems):
    copies = [pltpu.make_async_copy(src_a, dst_a, sems.at[0]), pltpu.make_async_copy(src_b, dst_b, sems.at[1])]
    for copy in copies:
        copy.start()
    loss[0] = jnp.sum(sums[0]) / total_rows
    d_temp[0] = scal[0] * (jnp.sum(sums[1]) / total_rows)
    d_bias[0] = jnp.sum(sums[2]) / total_rows
    for copy in copies:
        copy.wait()


def store_call(total_rows, scal, sums, *arrays):
    hbm = pl.BlockSpec(memory_space=pl.ANY)
    smem = pl.BlockSpec(memory_space=pltpu.SMEM)
    one = jax.ShapeDtypeStruct((1,), F32)
    return pl.pallas_call(
        functools.partial(store_kernel, total_rows),
        in_specs=[smem, pl.BlockSpec(memory_space=pltpu.VMEM), hbm, hbm],
        out_specs=[smem] * 3 + [pl.BlockSpec(memory_space=pltpu.HBM)] * 2,
        out_shape=[one] * 3 + [jax.ShapeDtypeStruct(a.shape, a.dtype) for a in arrays],
        scratch_shapes=[pltpu.SemaphoreType.DMA((2,))],
        compiler_params=pltpu.CompilerParams(vmem_limit_bytes=2**20),
        name="store",
    )(scal, sums, *arrays)


def solution(mesh):
    dev_count = mesh.shape["replica"] * mesh.shape["data"]
    batch_axes = ("replica", "data")

    def local_fn(img_x, txt_x, w_img, w_txt, log_temp, logit_bias):
        block = img_x.shape[0]
        total_rows = block * dev_count
        txt_raw, txt_emb = embed_rows(txt_x, w_txt)
        img_raw, img_emb = embed_rows(img_x, w_img)
        temp_scale = jnp.exp(log_temp[0])
        scal = jnp.stack([temp_scale, logit_bias[0], temp_scale / total_rows])
        sums, pack = main_call(scal, img_emb, txt_emb, img_x, txt_x, img_raw, txt_raw)
        d_w_img, d_w_txt, sums = sum_call(pack, sums, img_x, txt_x, w_img.shape[1])
        return tuple(store_call(total_rows, scal, sums, d_w_img, d_w_txt))

    batch_spec = P(batch_axes, None)
    return jax.shard_map(local_fn, mesh=mesh, in_specs=(batch_spec, batch_spec, P(), P(), P(), P()), out_specs=(P(), P(), P(), P(), P()), check_vma=False)
```
